16 devices in a mesh: data: 16 (over z, y, x, core).
Axes of the slice: x: 2, y: 2, z: 2, core: 2. Of those that a mesh axis runs over, the one named last changes fastest.
Arguments:
- feat_a: bfloat16 [16384, 512], P('data')
- feat_b: bfloat16 [16384, 512], P('data')
- w_in: bfloat16 [512, 2048], replicated
- w_mid: bfloat16 [2048, 2048], replicated
- w_out: bfloat16 [2048, 2048], replicated
- t_in: bfloat16 [512, 2048], replicated
- t_mid: bfloat16 [2048, 2048], replicated
- t_out: bfloat16 [2048, 2048], replicated
- gain_1: float32 [2048], replicated
- bias_1: float32 [2048], replicated
- gain_2: float32 [2048], replicated
- bias_2: float32 [2048], replicated
- off_weight: float32 [], replicated
Outputs:
- output 1: float32 [], replicated
- output 2: float32 [16384, 2048], P('data')
- output 3: float32 [512, 2048], replicated
- output 4: float32 [2048, 2048], replicated
- output 5: float32 [2048, 2048], replicated
- output 6: float32 [2048], replicated
- output 7: float32 [2048], replicated
- output 8: float32 [2048], replicated
- output 9: float32 [2048], replicated
All inputs are finite; a program needn't handle non-finite values.
Results may differ from the reference program's by a relative error of at most 0.00291604.
Values are sent between devices in bfloat16 or wider.
A program may use at most 1 GiB of HBM per device.

```python
import jax
import jax.numpy as jnp
from jax import lax

FEAT_DIM = 512
PROJ_DIM = 2048
ROWS_DEV = 1024
SHARDS = 16
ROWS = ROWS_DEV * SHARDS
NORM_EPS = 1e-5


def setup_inputs(seed: int = 0) -> dict:
    key_list = jax.random.split(jax.random.key(seed), 16)
    row_shape = (SHARDS, ROWS_DEV, FEAT_DIM)
    base_draw = jax.random.normal(key_list[0], row_shape, jnp.float32)
    view_noise = jax.random.normal(key_list[1], row_shape, jnp.float32)
    shard_shift = 0.5 * jax.random.normal(key_list[2], (SHARDS, 1, FEAT_DIM), jnp.float32)
    shard_scale = jax.random.uniform(key_list[3], (SHARDS, 1, FEAT_DIM), jnp.float32, 0.6, 1.4)
    feat_a = (base_draw * shard_scale + shard_shift).reshape(ROWS, FEAT_DIM)
    feat_b = ((0.8 * base_draw + 0.6 * view_noise) * shard_scale + shard_shift).reshape(ROWS, FEAT_DIM)
    in_scale = FEAT_DIM ** -0.5
    hid_scale = PROJ_DIM ** -0.5
    in_shape = (FEAT_DIM, PROJ_DIM)
    hid_shape = (PROJ_DIM, PROJ_DIM)
    w_in = in_scale * jax.random.normal(key_list[4], in_shape, jnp.float32)
    w_mid = hid_scale * jax.random.normal(key_list[5], hid_shape, jnp.float32)
    w_out = hid_scale * jax.random.normal(key_list[6], hid_shape, jnp.float32)
    t_in = 0.8 * w_in + 0.6 * in_scale * jax.random.normal(key_list[7], in_shape, jnp.float32)
    t_mid = 0.8 * w_mid + 0.6 * hid_scale * jax.random.normal(key_list[8], hid_shape, jnp.float32)
    t_out = 0.8 * w_out + 0.6 * hid_scale * jax.random.normal(key_list[9], hid_shape, jnp.float32)
    gain_1 = jax.random.uniform(key_list[10], (PROJ_DIM,), jnp.float32, 0.5, 1.5)
    bias_1 = 0.3 * jax.random.normal(key_list[11], (PROJ_DIM,), jnp.float32)
    gain_2 = jax.random.uniform(key_list[12], (PROJ_DIM,), jnp.float32, 0.5, 1.5)
    bias_2 = 0.3 * jax.random.normal(key_list[13], (PROJ_DIM,), jnp.float32)
    off_weight = (ROWS / PROJ_DIM) * jax.random.uniform(key_list[14], (), jnp.float32, 0.1, 0.3)
    return {
        "feat_a": feat_a.astype(jnp.bfloat16),
        "feat_b": feat_b.astype(jnp.bfloat16),
        "w_in": w_in.astype(jnp.bfloat16),
        "w_mid": w_mid.astype(jnp.bfloat16),
        "w_out": w_out.astype(jnp.bfloat16),
        "t_in": t_in.astype(jnp.bfloat16),
        "t_mid": t_mid.astype(jnp.bfloat16),
        "t_out": t_out.astype(jnp.bfloat16),
        "gain_1": gain_1,
        "bias_1": bias_1,
        "gain_2": gain_2,
        "bias_2": bias_2,
        "off_weight": off_weight,
    }


def batch_norm(pre_norm):
    mean_u = jnp.mean(pre_norm, axis=0)
    centered = pre_norm - mean_u
    inv_std = lax.rsqrt(jnp.mean(centered * centered, axis=0) + NORM_EPS)
    return centered * inv_std, inv_std


def hidden_layer(layer_in, weight, gain_vec, bias_vec):
    normed, inv_std = batch_norm(jnp.dot(layer_in, weight, preferred_element_type=jnp.float32))
    pre_act = normed * gain_vec + bias_vec
    return jnp.maximum(pre_act, 0.0).astype(jnp.bfloat16), normed, inv_std, pre_act > 0.0


def norm_back(grad_n, normed, inv_std):
    mean_g = jnp.mean(grad_n, axis=0)
    mean_gn = jnp.mean(grad_n * normed, axis=0)
    return (grad_n - mean_g - normed * mean_gn) * inv_std


def reference(feat_a, feat_b, w_in, w_mid, w_out, t_in, t_mid, t_out, gain_1, bias_1, gain_2, bias_2, off_weight):
    row_count = feat_a.shape[0]
    act_1, normed_1, inv_1, mask_1 = hidden_layer(feat_a, w_in, gain_1, bias_1)
    act_2, normed_2, inv_2, mask_2 = hidden_layer(act_1, w_mid, gain_2, bias_2)
    zh_a, inv_z = batch_norm(jnp.dot(act_2, w_out, preferred_element_type=jnp.float32))
    teach_1 = hidden_layer(feat_b, t_in, gain_1, bias_1)[0]
    teach_2 = hidden_layer(teach_1, t_mid, gain_2, bias_2)[0]
    zh_b = batch_norm(jnp.dot(teach_2, t_out, preferred_element_type=jnp.float32))[0]
    emb_a = zh_a.astype(jnp.bfloat16)
    emb_b = zh_b.astype(jnp.bfloat16)
    corr_mat = jnp.dot(emb_a.T, emb_b, preferred_element_type=jnp.float32) / row_count
    proj_width = corr_mat.shape[0]
    on_diag = jnp.arange(proj_width)[:, None] == jnp.arange(proj_width)[None, :]
    loss_value = jnp.sum(jnp.square(1.0 - jnp.diagonal(corr_mat))) + off_weight * jnp.sum(jnp.square(jnp.where(on_diag, 0.0, corr_mat)))
    grad_c = jnp.where(on_diag, -2.0 * (1.0 - corr_mat), 2.0 * off_weight * corr_mat).astype(jnp.bfloat16)
    grad_emb = jnp.dot(emb_b, grad_c.T, preferred_element_type=jnp.float32) / row_count
    grad_z = norm_back(grad_emb, zh_a, inv_z).astype(jnp.bfloat16)
    grad_w_out = jnp.dot(act_2.T, grad_z, preferred_element_type=jnp.float32)
    grad_pre_2 = jnp.where(mask_2, jnp.dot(grad_z, w_out.T, preferred_element_type=jnp.float32), 0.0)
    grad_gain_2 = jnp.sum(grad_pre_2 * normed_2, axis=0)
    grad_bias_2 = jnp.sum(grad_pre_2, axis=0)
    grad_u_2 = norm_back(grad_pre_2 * gain_2, normed_2, inv_2).astype(jnp.bfloat16)
    grad_w_mid = jnp.dot(act_1.T, grad_u_2, preferred_element_type=jnp.float32)
    grad_pre_1 = jnp.where(mask_1, jnp.dot(grad_u_2, w_mid.T, preferred_element_type=jnp.float32), 0.0)
    grad_gain_1 = jnp.sum(grad_pre_1 * normed_1, axis=0)
    grad_bias_1 = jnp.sum(grad_pre_1, axis=0)
    grad_u_1 = norm_back(grad_pre_1 * gain_1, normed_1, inv_1).astype(jnp.bfloat16)
    grad_w_in = jnp.dot(feat_a.T, grad_u_1, preferred_element_type=jnp.float32)
    return (loss_value, grad_emb, grad_w_in, grad_w_mid, grad_w_out, grad_gain_1, grad_bias_1, grad_gain_2, grad_bias_2)
```

```python
import functools

import jax
import jax.numpy as jnp
from jax import lax
from jax.experimental import pallas as pl
from jax.experimental.pallas import tpu as pltpu
from jax.sharding import PartitionSpec as P

NORM_EPS = 1e-5
DATA_AXIS = "data"
MESH_ID = pl.DeviceIdType.MESH
UNIT = 128
VMEM_LIMIT = 66_000_000


def contract_rows(left_op, right_op):
    return lax.dot_general(left_op, right_op, (((0,), (0,)), ((), ())), preferred_element_type=jnp.float32)


def contract_cols(left_op, right_op):
    return lax.dot_general(left_op, right_op, (((1,), (1,)), ((), ())), preferred_element_type=jnp.float32)


def flip(me, mask):
    bit = lax.rem(lax.div(me, mask), 2)
    return me + mask * (1 - 2 * bit), bit


def stats_kernel(shards, x_ref, out_ref, parts, send_a, recv_a, send_b, recv_b):
    me = lax.axis_index(DATA_AXIS)
    lanes = x_ref.shape[1] // shards
    barrier = pltpu.get_barrier_semaphore()
    for step in range(1, shards):
        peer = lax.rem(me + step, shards)
        pl.semaphore_signal(barrier, inc=1, device_id=(peer,), device_id_type=MESH_ID)
    pl.semaphore_wait(barrier, shards - 1)

    def lane_block(index):
        return pl.ds(pl.multiple_of(index * lanes, lanes), lanes)

    def scatter(step):
        peer = lax.rem(me + step, shards)
        return pltpu.make_async_remote_copy(src_ref=x_ref.at[:, lane_block(peer)], dst_ref=parts.at[step], send_sem=send_a.at[step], recv_sem=recv_a.at[step], device_id=(peer,), device_id_type=MESH_ID)

    def gather(step):
        peer = lax.rem(me + step, shards)
        mine = lane_block(me)
        return pltpu.make_async_remote_copy(src_ref=parts.at[0], dst_ref=out_ref.at[:, mine], send_sem=send_b.at[step], recv_sem=recv_b.at[step], device_id=(peer,), device_id_type=MESH_ID)

    for step in range(1, shards):
        scatter(step).start()
    total = x_ref[:, lane_block(me)]
    for step in range(1, shards):
        scatter(step).wait()
        total = total + parts[step]
    parts[0] = total
    out_ref[:, lane_block(me)] = total
    for step in range(1, shards):
        gather(step).start()
    for step in range(1, shards):
        gather(step).wait()


def stats_all_reduce(rows, shards):
    pad = [jnp.zeros_like(rows[0])] * (8 - len(rows))
    packed = jnp.stack(list(rows) + pad)
    lanes = packed.shape[1] // shards
    vmem = pl.BlockSpec(memory_space=pltpu.VMEM)
    return pl.pallas_call(
        functools.partial(stats_kernel, shards),
        out_shape=jax.ShapeDtypeStruct(packed.shape, jnp.float32),
        in_specs=[vmem],
        out_specs=vmem,
        scratch_shapes=[pltpu.VMEM((shards, 8, lanes), jnp.float32)] + [pltpu.SemaphoreType.DMA((shards,))] * 4,
        compiler_params=pltpu.CompilerParams(collective_id=1, has_side_effects=True),
        name="stats_all_reduce",
    )(packed)


PAIR, RS1, RS2, RS3, AG3, AG2, AG1, AGP, LOCAL = range(9)


class Exchange:
    def __init__(self, me, ring, halves, gathered, recv_pair, recv_1, recv_2, recv_3, total, send_sems, recv_sems, row_of):
        self.me, self.ring, self.halves, self.gathered = me, ring, halves, gathered
        self.recv_pair, self.recv_1, self.recv_2, self.recv_3, self.total = recv_pair, recv_1, recv_2, recv_3, total
        self.send_sems, self.recv_sems, self.row_of = send_sems, recv_sems, row_of

    def axes(self, unit):
        def mask(shift):
            axis = lax.rem(unit + shift, 3)
            return 2 + axis + axis * axis

        (p1, b1), (p2, b2), (p3, b3) = (flip(self.me, mask(shift)) for shift in range(3))
        return (p1, p2, p3), (b1, b2, b3)

    def copy(self, unit, kind):
        (p1, p2, p3), (b1, b2, b3) = self.axes(unit)
        partner, half = flip(self.me, 1)

        def rows(start, size):
            return pl.ds(pl.multiple_of(start, 16), size)

        total = self.total.at[unit]
        row = self.row_of(unit, half)
        if kind == PAIR:
            src, dst, peer = self.halves.at[lax.rem(unit, self.ring)], self.recv_pair.at[unit], partner
        elif kind == RS1:
            src, dst, peer = total.at[rows((1 - b1) * 64, 64)], self.recv_1.at[unit], p1
        elif kind == RS2:
            src, dst, peer = total.at[rows(b1 * 64 + (1 - b2) * 32, 32)], self.recv_2.at[unit], p2
        elif kind == RS3:
            src, dst, peer = total.at[rows(b1 * 64 + b2 * 32 + (1 - b3) * 16, 16)], self.recv_3.at[unit], p3
        else:
            start, size, peer = {
                AG3: (b1 * 64 + b2 * 32 + b3 * 16, 16, p3),
                AG2: (b1 * 64 + b2 * 32, 32, p2),
                AG1: (b1 * 64, 64, p1),
                AGP: (0, 128, partner),
            }[kind]
            src = dst = self.gathered.at[rows(row + start, size)]
        return pltpu.make_async_remote_copy(src_ref=src, dst_ref=dst, send_sem=self.send_sems.at[unit, kind], recv_sem=self.recv_sems.at[unit, kind], device_id=(peer,), device_id_type=MESH_ID)

    def reduce_step(self, unit, kind):
        _, (b1, b2, b3) = self.axes(unit)
        self.copy(unit, kind).wait()
        if kind == PAIR:
            start, size, landed = 0, 128, self.recv_pair
        elif kind == RS1:
            start, size, landed = b1 * 64, 64, self.recv_1
        else:
            start, size, landed = b1 * 64 + b2 * 32, 32, self.recv_2
        keep = pl.ds(pl.multiple_of(start, 16), size)
        self.total[unit, keep] = self.total[unit, keep] + landed[unit]
        self.copy(unit, kind + 1).start()

    def owned(self, unit):
        _, (b1, b2, b3) = self.axes(unit)
        return b1 * 64 + b2 * 32 + b3 * 16


def enter(me):
    barrier = pltpu.get_barrier_semaphore()
    for mask in (1, 2, 4, 8):
        pl.semaphore_signal(barrier, inc=1, device_id=(flip(me, mask)[0],), device_id_type=MESH_ID)
    pl.semaphore_wait(barrier, 4)


def pipeline(units, lags, stages):
    def step(now, carry):
        for lag, stage in zip(lags, stages):
            unit = now - lag

            @pl.when((unit >= 0) & (unit < units))
            def _():
                stage(unit)

        return carry

    lax.fori_loop(0, units + max(lags), step, 0)


def product_unit(left_ref, right_ref, col_other, col_mine, halves, total, slot, unit, blocks):
    left = jnp.concatenate([left_ref[:, pl.ds(pl.multiple_of(col_other, UNIT), UNIT)], left_ref[:, pl.ds(pl.multiple_of(col_mine, UNIT), UNIT)]], axis=1)
    width = right_ref.shape[1] // blocks
    for block in range(blocks):
        cols = pl.ds(block * width, width)
        out = contract_rows(left, right_ref[:, cols])
        halves[slot, :, cols] = out[:UNIT]
        total[unit, :, cols] = out[UNIT:]


RING = 3
CORR_LAGS = (0, 1, 3, 5, 7, 8, 9, 10, 11)


def corr_kernel(row_count, off_ref, left_ref, right_ref, grad_ref, loss_ref, halves, recv_pair, recv_1, recv_2, recv_3, total, send_sems, recv_sems):
    me = lax.axis_index(DATA_AXIS)
    width = right_ref.shape[1]
    half_rows = left_ref.shape[1] // 2
    units = half_rows // UNIT
    _, half = flip(me, 1)
    enter(me)
    ex = Exchange(me, RING, halves, grad_ref, recv_pair, recv_1, recv_2, recv_3, total, send_sems, recv_sems, lambda unit, h: h * half_rows + unit * UNIT)
    loss_ref[...] = jnp.zeros_like(loss_ref)

    def produce(unit):
        @pl.when(unit >= RING)
        def _():
            ex.copy(unit - RING, PAIR).wait_send()

        product_unit(left_ref, right_ref, (1 - half) * half_rows + unit * UNIT, half * half_rows + unit * UNIT, halves, total, lax.rem(unit, RING), unit, 4)
        ex.copy(unit, PAIR).start()

    def pair_step(unit):
        ex.copy(unit, PAIR).wait_recv()
        total[unit] = total[unit] + recv_pair[unit]
        ex.copy(unit, RS1).start()

    def finish(unit):
        ex.copy(unit, RS3).wait()
        start = ex.owned(unit)
        keep = pl.ds(pl.multiple_of(start, 16), 16)
        corr = (total[unit, keep] + recv_3[unit]) * (1.0 / row_count)
        row = half * half_rows + unit * UNIT + start
        on_diag = lax.broadcasted_iota(jnp.int32, (16, width), 0) + row == lax.broadcasted_iota(jnp.int32, (16, width), 1)
        off_weight = off_ref[0, 0]
        miss = 1.0 - corr
        terms = jnp.where(on_diag, miss * miss, off_weight * (corr * corr))
        loss_ref[...] += terms[:8] + terms[8:]
        grad = jnp.where(on_diag, -2.0 * miss, 2.0 * off_weight * corr).astype(jnp.bfloat16)
        grad_ref[pl.ds(pl.multiple_of(row, 16), 16)] = grad
        ex.copy(unit, AG3).start()

    def forward(kind):
        def stage(unit):
            ex.copy(unit, kind).wait()
            if kind != AGP:
                ex.copy(unit, kind + 1).start()

        return stage

    pipeline(units, CORR_LAGS, [produce, pair_step, lambda u: ex.reduce_step(u, RS1), lambda u: ex.reduce_step(u, RS2), finish, forward(AG3), forward(AG2), forward(AG1), forward(AGP)])
    for unit in range(units - RING, units):
        ex.copy(unit, PAIR).wait_send()


def exchange_scratch(units, width):
    return [
        pltpu.VMEM((RING, UNIT, width), jnp.float32),
        pltpu.VMEM((units, UNIT, width), jnp.float32),
        pltpu.VMEM((units, 64, width), jnp.float32),
        pltpu.VMEM((units, 32, width), jnp.float32),
        pltpu.VMEM((units, 16, width), jnp.float32),
        pltpu.VMEM((units, UNIT, width), jnp.float32),
        pltpu.SemaphoreType.DMA((units, 9)),
        pltpu.SemaphoreType.DMA((units, 9)),
    ]


def corr_grad(emb_a, emb_b, off_weight, row_count):
    rows, width = emb_a.shape
    vmem = pl.BlockSpec(memory_space=pltpu.VMEM)
    return pl.pallas_call(
        functools.partial(corr_kernel, row_count),
        out_shape=(jax.ShapeDtypeStruct((width, width), jnp.bfloat16), jax.ShapeDtypeStruct((8, width), jnp.float32)),
        in_specs=[pl.BlockSpec(memory_space=pltpu.SMEM), vmem, vmem],
        out_specs=(vmem, vmem),
        scratch_shapes=exchange_scratch(width // 2 // UNIT, width),
        compiler_params=pltpu.CompilerParams(collective_id=2, has_side_effects=True, vmem_limit_bytes=VMEM_LIMIT),
        cost_estimate=pl.CostEstimate(flops=2 * rows * width * width, bytes_accessed=4 * width * width, transcendentals=0),
        name="corr_grad",
    )(off_weight.reshape(1, 1), emb_a, emb_b)


WEIGHT_LAGS = (0, 1, 3, 5, 7, 8, 9, 10, 11)


def weight_kernel(sizes, *refs):
    count = len(sizes)
    lefts, rights = refs[:count], refs[count : 2 * count]
    out_ref, halves, recv_pair, recv_1, recv_2, recv_3, total, send_sems, recv_sems = refs[2 * count :]
    me = lax.axis_index(DATA_AXIS)
    _, half = flip(me, 1)
    firsts, bases, units, base = [], [], 0, 0
    for size in sizes:
        firsts.append(units)
        bases.append(base)
        units += size // 2 // UNIT
        base += size
    enter(me)

    def row_of(unit, h):
        row = bases[0] + h * (sizes[0] // 2) + unit * UNIT
        for index in range(1, count):
            inside = lax.div(unit + units - firsts[index], units)
            inside = lax.min(inside, 1)
            row = row + inside * (bases[index] + h * (sizes[index] // 2) + (unit - firsts[index]) * UNIT - row)
        return row

    ex = Exchange(me, RING, halves, out_ref, recv_pair, recv_1, recv_2, recv_3, total, send_sems, recv_sems, row_of)

    def produce(unit):
        @pl.when(unit >= RING)
        def _():
            ex.copy(unit - RING, PAIR).wait_send()

        for index in range(count):
            last = firsts[index] + sizes[index] // 2 // UNIT

            @pl.when((unit >= firsts[index]) & (unit < last))
            def _():
                local = (unit - firsts[index]) * UNIT
                part = sizes[index] // 2
                product_unit(lefts[index], rights[index], (1 - half) * part + local, half * part + local, halves, total, lax.rem(unit, RING), unit, 4)

        ex.copy(unit, PAIR).start()

    def pair_step(unit):
        ex.copy(unit, PAIR).wait_recv()
        total[unit] = total[unit] + recv_pair[unit]
        ex.copy(unit, RS1).start()

    def to_out(unit):
        start = ex.owned(unit)
        return pltpu.make_async_copy(total.at[unit, pl.ds(pl.multiple_of(start, 16), 16)], out_ref.at[pl.ds(pl.multiple_of(row_of(unit, half) + start, 16), 16)], send_sems.at[unit, LOCAL])

    def finish(unit):
        ex.copy(unit, RS3).wait()
        keep = pl.ds(pl.multiple_of(ex.owned(unit), 16), 16)
        total[unit, keep] = total[unit, keep] + recv_3[unit]
        to_out(unit).start()
        to_out(unit).wait()
        ex.copy(unit, AG3).start()

    def forward(kind):
        def stage(unit):
            ex.copy(unit, kind).wait()
            if kind != AGP:
                ex.copy(unit, kind + 1).start()

        return stage

    pipeline(units, WEIGHT_LAGS, [produce, pair_step, lambda u: ex.reduce_step(u, RS1), lambda u: ex.reduce_step(u, RS2), finish, forward(AG3), forward(AG2), forward(AG1), forward(AGP)])
    for unit in range(units - RING, units):
        ex.copy(unit, PAIR).wait_send()


def weight_sums(lefts, rights, call_id):
    sizes = tuple(left.shape[1] for left in lefts)
    width = rights[0].shape[1]
    units = sum(size // 2 // UNIT for size in sizes)
    vmem = pl.BlockSpec(memory_space=pltpu.VMEM)
    return pl.pallas_call(
        functools.partial(weight_kernel, sizes),
        out_shape=jax.ShapeDtypeStruct((sum(sizes), width), jnp.float32),
        in_specs=[vmem] * (2 * len(sizes)),
        out_specs=pl.BlockSpec(memory_space=pl.ANY),
        scratch_shapes=exchange_scratch(units, width),
        compiler_params=pltpu.CompilerParams(collective_id=call_id, has_side_effects=True, vmem_limit_bytes=VMEM_LIMIT),
        cost_estimate=pl.CostEstimate(flops=2 * lefts[0].shape[0] * sum(sizes) * width, bytes_accessed=8 * sum(sizes) * width, transcendentals=0),
        name=f"weight_sums_{call_id}",
    )(*lefts, *rights)


def solution(mesh):
    shards = mesh.shape[DATA_AXIS]
    row_part = P(DATA_AXIS, None)
    replicated = P()

    def local_step(feat_a, feat_b, w_in, w_mid, w_out, t_in, t_mid, t_out, gain_1, bias_1, gain_2, bias_2, off_weight):
        row_count = feat_a.shape[0] * shards

        def norm_pair(pre_a, pre_b):
            stat_means = stats_all_reduce([jnp.sum(pre_a, axis=0), jnp.sum(pre_a * pre_a, axis=0), jnp.sum(pre_b, axis=0), jnp.sum(pre_b * pre_b, axis=0)], shards) / row_count
            inv_a = lax.rsqrt(stat_means[1] - stat_means[0] * stat_means[0] + NORM_EPS)
            inv_b = lax.rsqrt(stat_means[3] - stat_means[2] * stat_means[2] + NORM_EPS)
            return (pre_a - stat_means[0]) * inv_a, inv_a, (pre_b - stat_means[2]) * inv_b

        def hidden_pair(in_a, in_b, weight_a, weight_b, gain_vec, bias_vec):
            normed_a, inv_a, normed_b = norm_pair(jnp.dot(in_a, weight_a, preferred_element_type=jnp.float32), jnp.dot(in_b, weight_b, preferred_element_type=jnp.float32))
            pre_act = normed_a * gain_vec + bias_vec
            act_a = jnp.maximum(pre_act, 0.0).astype(jnp.bfloat16)
            act_b = jnp.maximum(normed_b * gain_vec + bias_vec, 0.0).astype(jnp.bfloat16)
            return act_a, act_b, normed_a, inv_a, pre_act > 0.0

        def affine_back(grad_pre, normed, inv_std, gain_vec):
            stat_sums = stats_all_reduce([jnp.sum(grad_pre * normed, axis=0), jnp.sum(grad_pre, axis=0)], shards)
            grad_u = (grad_pre - stat_sums[1] / row_count - normed * (stat_sums[0] / row_count)) * (gain_vec * inv_std)
            return grad_u.astype(jnp.bfloat16), stat_sums[0], stat_sums[1]

        act_1, teach_1, normed_1, inv_1, mask_1 = hidden_pair(feat_a, feat_b, w_in, t_in, gain_1, bias_1)
        act_2, teach_2, normed_2, inv_2, mask_2 = hidden_pair(act_1, teach_1, w_mid, t_mid, gain_2, bias_2)
        zh_a, inv_z, zh_b = norm_pair(jnp.dot(act_2, w_out, preferred_element_type=jnp.float32), jnp.dot(teach_2, t_out, preferred_element_type=jnp.float32))
        emb_a = zh_a.astype(jnp.bfloat16)
        emb_b = zh_b.astype(jnp.bfloat16)
        grad_c, loss_part = corr_grad(emb_a, emb_b, off_weight, row_count)
        grad_emb = contract_cols(emb_b, grad_c) / row_count
        stat_sums = stats_all_reduce([jnp.sum(grad_emb, axis=0), jnp.sum(grad_emb * zh_a, axis=0), jnp.sum(loss_part, axis=0)], shards)
        loss_value = jnp.sum(stat_sums[2])
        grad_z = ((grad_emb - stat_sums[0] / row_count - zh_a * (stat_sums[1] / row_count)) * inv_z).astype(jnp.bfloat16)
        grad_pre_2 = jnp.where(mask_2, contract_cols(grad_z, w_out), 0.0)
        grad_u_2, grad_gain_2, grad_bias_2 = affine_back(grad_pre_2, normed_2, inv_2, gain_2)
        grad_pre_1 = jnp.where(mask_1, contract_cols(grad_u_2, w_mid), 0.0)
        grad_u_1, grad_gain_1, grad_bias_1 = affine_back(grad_pre_1, normed_1, inv_1, gain_1)
        sums_out = weight_sums([act_2], [grad_z], 3)
        sums_rest = weight_sums([act_1, feat_a], [grad_u_2, grad_u_1], 4)
        width = w_mid.shape[0]
        return (loss_value, grad_emb, sums_rest[width:], sums_rest[:width], sums_out, grad_gain_1, grad_bias_1, grad_gain_2, grad_bias_2)

    return jax.shard_map(local_step, mesh=mesh, in_specs=(row_part, row_part) + (replicated,) * 11, out_specs=(replicated, row_part) + (replicated,) * 7, check_vma=False)
```

```python
import functools

import jax
import jax.numpy as jnp
from jax import lax
from jax.experimental import pallas as pl
from jax.experimental.pallas import tpu as pltpu
from jax.sharding import PartitionSpec as P

NORM_EPS = 1e-5
DATA_AXIS = "data"
MESH_ID = pl.DeviceIdType.MESH
UNIT = 128
VMEM_LIMIT = 66_000_000


def contract_rows(left_op, right_op):
    return lax.dot_general(left_op, right_op, (((0,), (0,)), ((), ())), preferred_element_type=jnp.float32)


def contract_cols(left_op, right_op):
    return lax.dot_general(left_op, right_op, (((1,), (1,)), ((), ())), preferred_element_type=jnp.float32)


def flip(me, mask):
    bit = lax.rem(lax.div(me, mask), 2)
    return me + mask * (1 - 2 * bit), bit


def stats_kernel(shards, x_ref, out_ref, parts, send_a, recv_a, send_b, recv_b):
    me = lax.axis_index(DATA_AXIS)
    lanes = x_ref.shape[1] // shards
    barrier = pltpu.get_barrier_semaphore()
    for step in range(1, shards):
        peer = lax.rem(me + step, shards)
        pl.semaphore_signal(barrier, inc=1, device_id=(peer,), device_id_type=MESH_ID)
    pl.semaphore_wait(barrier, shards - 1)

    def lane_block(index):
        return pl.ds(pl.multiple_of(index * lanes, lanes), lanes)

    def scatter(step):
        peer = lax.rem(me + step, shards)
        return pltpu.make_async_remote_copy(src_ref=x_ref.at[:, lane_block(peer)], dst_ref=parts.at[step], send_sem=send_a.at[step], recv_sem=recv_a.at[step], device_id=(peer,), device_id_type=MESH_ID)

    def gather(step):
        peer = lax.rem(me + step, shards)
        mine = lane_block(me)
        return pltpu.make_async_remote_copy(src_ref=parts.at[0], dst_ref=out_ref.at[:, mine], send_sem=send_b.at[step], recv_sem=recv_b.at[step], device_id=(peer,), device_id_type=MESH_ID)

    for step in range(1, shards):
        scatter(step).start()
    total = x_ref[:, lane_block(me)]
    for step in range(1, shards):
        scatter(step).wait()
        total = total + parts[step]
    parts[0] = total
    out_ref[:, lane_block(me)] = total
    for step in range(1, shards):
        gather(step).start()
    for step in range(1, shards):
        gather(step).wait()


def stats_all_reduce(rows, shards):
    pad = [jnp.zeros_like(rows[0])] * (8 - len(rows))
    packed = jnp.stack(list(rows) + pad)
    lanes = packed.shape[1] // shards
    vmem = pl.BlockSpec(memory_space=pltpu.VMEM)
    return pl.pallas_call(
        functools.partial(stats_kernel, shards),
        out_shape=jax.ShapeDtypeStruct(packed.shape, jnp.float32),
        in_specs=[vmem],
        out_specs=vmem,
        scratch_shapes=[pltpu.VMEM((shards, 8, lanes), jnp.float32)] + [pltpu.SemaphoreType.DMA((shards,))] * 4,
        compiler_params=pltpu.CompilerParams(collective_id=1, has_side_effects=True),
        name="stats_all_reduce",
    )(packed)


PAIR, RS1, RS2, RS3, AG3, AG2, AG1, AGP, LOCAL = range(9)


class Exchange:
    def __init__(self, me, ring, halves, gathered, recv_pair, recv_1, recv_2, recv_3, total, send_sems, recv_sems, row_of, depth, send_total=False):
        self.depth, self.send_total = depth, send_total
        self.me, self.ring, self.halves, self.gathered = me, ring, halves, gathered
        self.recv_pair, self.recv_1, self.recv_2, self.recv_3, self.total = recv_pair, recv_1, recv_2, recv_3, total
        self.send_sems, self.recv_sems, self.row_of = send_sems, recv_sems, row_of

    def axes(self, unit):
        def mask(shift):
            axis = lax.rem(unit + shift, 3)
            return 2 + axis + axis * axis

        (p1, b1), (p2, b2), (p3, b3) = (flip(self.me, mask(shift)) for shift in range(3))
        return (p1, p2, p3), (b1, b2, b3)

    def copy(self, unit, kind):
        (p1, p2, p3), (b1, b2, b3) = self.axes(unit)
        partner, half = flip(self.me, 1)

        def rows(start, size):
            return pl.ds(pl.multiple_of(start, 16), size)

        slot = lax.rem(unit, self.depth)
        total = self.total.at[slot]
        row = self.row_of(unit, half)
        if kind == PAIR:
            src, dst, peer = self.halves.at[lax.rem(unit, self.ring)], self.recv_pair.at[slot], partner
        elif kind == RS1:
            src, dst, peer = total.at[rows((1 - b1) * 64, 64)], self.recv_1.at[slot], p1
        elif kind == RS2:
            src, dst, peer = total.at[rows(b1 * 64 + (1 - b2) * 32, 32)], self.recv_2.at[slot], p2
        elif kind == RS3:
            src, dst, peer = total.at[rows(b1 * 64 + b2 * 32 + (1 - b3) * 16, 16)], self.recv_3.at[slot], p3
        else:
            start, size, peer = {
                AG3: (b1 * 64 + b2 * 32 + b3 * 16, 16, p3),
                AG2: (b1 * 64 + b2 * 32, 32, p2),
                AG1: (b1 * 64, 64, p1),
                AGP: (0, 128, partner),
            }[kind]
            src = dst = self.gathered.at[rows(row + start, size)]
            if kind == AG3 and self.send_total:
                src = total.at[rows(start, size)]
        return pltpu.make_async_remote_copy(src_ref=src, dst_ref=dst, send_sem=self.send_sems.at[slot, kind], recv_sem=self.recv_sems.at[slot, kind], device_id=(peer,), device_id_type=MESH_ID)

    def reduce_step(self, unit, kind):
        _, (b1, b2, b3) = self.axes(unit)
        self.copy(unit, kind).wait()
        if kind == PAIR:
            start, size, landed = 0, 128, self.recv_pair
        elif kind == RS1:
            start, size, landed = b1 * 64, 64, self.recv_1
        else:
            start, size, landed = b1 * 64 + b2 * 32, 32, self.recv_2
        keep = pl.ds(pl.multiple_of(start, 16), size)
        slot = lax.rem(unit, self.depth)
        self.total[slot, keep] = self.total[slot, keep] + landed[slot]
        self.copy(unit, kind + 1).start()

    def owned(self, unit):
        _, (b1, b2, b3) = self.axes(unit)
        return b1 * 64 + b2 * 32 + b3 * 16


def enter(me):
    barrier = pltpu.get_barrier_semaphore()
    for mask in (1, 2, 4, 8):
        pl.semaphore_signal(barrier, inc=1, device_id=(flip(me, mask)[0],), device_id_type=MESH_ID)
    pl.semaphore_wait(barrier, 4)


def pipeline(units, lags, stages):
    def step(now, carry):
        for lag, stage in zip(lags, stages):
            unit = now - lag

            @pl.when((unit >= 0) & (unit < units))
            def _():
                stage(unit)

        return carry

    lax.fori_loop(0, units + max(lags), step, 0)


def product_unit(left_ref, right_ref, col_other, col_mine, halves, total, slot, unit, blocks):
    left = jnp.concatenate([left_ref[:, pl.ds(pl.multiple_of(col_other, UNIT), UNIT)], left_ref[:, pl.ds(pl.multiple_of(col_mine, UNIT), UNIT)]], axis=1)
    width = right_ref.shape[1] // blocks
    for block in range(blocks):
        cols = pl.ds(block * width, width)
        out = contract_rows(left, right_ref[:, cols])
        halves[slot, :, cols] = out[:UNIT]
        total[unit, :, cols] = out[UNIT:]


RING = 3
CORR_LAGS = (0, 1, 4, 6, 8, 10, 13, 17, 19)


def corr_kernel(row_count, off_ref, left_ref, right_ref, grad_ref, loss_ref, halves, recv_pair, recv_1, recv_2, recv_3, total, send_sems, recv_sems):
    me = lax.axis_index(DATA_AXIS)
    width = right_ref.shape[1]
    half_rows = left_ref.shape[1] // 2
    units = half_rows // UNIT
    _, half = flip(me, 1)
    enter(me)
    ex = Exchange(me, RING, halves, grad_ref, recv_pair, recv_1, recv_2, recv_3, total, send_sems, recv_sems, lambda unit, h: h * half_rows + unit * UNIT, units)
    loss_ref[...] = jnp.zeros_like(loss_ref)

    def produce(unit):
        @pl.when(unit >= RING)
        def _():
            ex.copy(unit - RING, PAIR).wait_send()

        product_unit(left_ref, right_ref, (1 - half) * half_rows + unit * UNIT, half * half_rows + unit * UNIT, halves, total, lax.rem(unit, RING), unit, 4)
        ex.copy(unit, PAIR).start()

    def pair_step(unit):
        ex.copy(unit, PAIR).wait_recv()
        total[unit] = total[unit] + recv_pair[unit]
        ex.copy(unit, RS1).start()

    def finish(unit):
        ex.copy(unit, RS3).wait()
        start = ex.owned(unit)
        keep = pl.ds(pl.multiple_of(start, 16), 16)
        corr = (total[unit, keep] + recv_3[unit]) * (1.0 / row_count)
        row = half * half_rows + unit * UNIT + start
        on_diag = lax.broadcasted_iota(jnp.int32, (16, width), 0) + row == lax.broadcasted_iota(jnp.int32, (16, width), 1)
        off_weight = off_ref[0, 0]
        miss = 1.0 - corr
        terms = jnp.where(on_diag, miss * miss, off_weight * (corr * corr))
        loss_ref[...] += terms[:8] + terms[8:]
        grad = jnp.where(on_diag, -2.0 * miss, 2.0 * off_weight * corr).astype(jnp.bfloat16)
        grad_ref[pl.ds(pl.multiple_of(row, 16), 16)] = grad
        ex.copy(unit, AG3).start()

    def forward(kind):
        def stage(unit):
            ex.copy(unit, kind).wait()
            if kind != AGP:
                ex.copy(unit, kind + 1).start()

        return stage

    pipeline(units, CORR_LAGS, [produce, pair_step, lambda u: ex.reduce_step(u, RS1), lambda u: ex.reduce_step(u, RS2), finish, forward(AG3), forward(AG2), forward(AG1), forward(AGP)])
    for unit in range(units - RING, units):
        ex.copy(unit, PAIR).wait_send()


def exchange_scratch(units, width):
    return [
        pltpu.VMEM((RING, UNIT, width), jnp.float32),
        pltpu.VMEM((units, UNIT, width), jnp.float32),
        pltpu.VMEM((units, 64, width), jnp.float32),
        pltpu.VMEM((units, 32, width), jnp.float32),
        pltpu.VMEM((units, 16, width), jnp.float32),
        pltpu.VMEM((units, UNIT, width), jnp.float32),
        pltpu.SemaphoreType.DMA((units, 9)),
        pltpu.SemaphoreType.DMA((units, 9)),
    ]


def corr_grad(emb_a, emb_b, off_weight, row_count):
    rows, width = emb_a.shape
    vmem = pl.BlockSpec(memory_space=pltpu.VMEM)
    return pl.pallas_call(
        functools.partial(corr_kernel, row_count),
        out_shape=(jax.ShapeDtypeStruct((width, width), jnp.bfloat16), jax.ShapeDtypeStruct((8, width), jnp.float32)),
        in_specs=[pl.BlockSpec(memory_space=pltpu.SMEM), vmem, vmem],
        out_specs=(vmem, vmem),
        scratch_shapes=exchange_scratch(width // 2 // UNIT, width),
        compiler_params=pltpu.CompilerParams(collective_id=2, has_side_effects=True, vmem_limit_bytes=VMEM_LIMIT),
        cost_estimate=pl.CostEstimate(flops=2 * rows * width * width, bytes_accessed=4 * width * width, transcendentals=0),
        name="corr_grad",
    )(off_weight.reshape(1, 1), emb_a, emb_b)


DEPTH = 12
PERIOD = 12
BLOCK = 256
BACK_LAGS = (1, 4, 6, 7, 9, 12, 15, 16)


def backward_kernel(shards, row_count, left_2, grad_z, w_out, normed_2, left_1, w_mid, normed_1, feat, vecs, out_ref, stat_ref, left, feat_in, grad, weight, normed, deriv, halves, mine, total, recv_1, recv_2, recv_3, stat_part, stat_in, send_sems, recv_sems, load_sems, weight_sems, normed_sems, stat_sems):
    me = lax.axis_index(DATA_AXIS)
    _, half = flip(me, 1)
    rows, width = left.shape
    blocks = width // BLOCK
    units_full = width // 2 // UNIT
    units_last = feat_in.shape[1] // 2 // UNIT
    enters = 2 * PERIOD + units_last
    ticks = enters + max(BACK_LAGS)

    load_left = pltpu.make_async_copy(left_2, left, load_sems.at[0])
    load_grad = pltpu.make_async_copy(grad_z, grad, load_sems.at[1])
    load_feat = pltpu.make_async_copy(feat, feat_in, load_sems.at[2])

    def block_of(index):
        return pl.ds(pl.multiple_of(index * BLOCK, BLOCK), BLOCK)

    def load_weight(source, index):
        return pltpu.make_async_copy(source.at[block_of(index)], weight.at[block_of(index)], weight_sems.at[index])

    def load_normed(source, index):
        return pltpu.make_async_copy(source.at[:, block_of(index)], normed.at[:, block_of(index)], normed_sems.at[index])

    load_left.start()
    load_grad.start()
    for index in range(blocks):
        load_weight(w_out, index).start()
        load_normed(normed_2, index).start()
    load_feat.start()

    barrier = pltpu.get_barrier_semaphore()
    for shift in range(1, shards):
        pl.semaphore_signal(barrier, inc=1, device_id=(lax.rem(me + shift, shards),), device_id_type=MESH_ID)
    pl.semaphore_wait(barrier, shards - 1)

    def row_of(unit, h):
        layer = lax.div(unit, units_full)
        part = width // 2 - (width // 2 - feat_in.shape[1] // 2) * lax.div(layer, 2)
        return layer * width + h * part + lax.rem(unit, units_full) * UNIT

    ex = Exchange(me, 2, halves, out_ref, total, recv_1, recv_2, recv_3, total, send_sems, recv_sems, row_of, DEPTH, send_total=True)

    def produce(unit, source, part):
        @pl.when(unit >= 2)
        def _():
            ex.copy(unit - 2, PAIR).wait_send()

        local = lax.rem(unit, units_full) * UNIT
        ring = lax.rem(unit, 2)
        col_other, col_mine = (1 - half) * part + local, half * part + local
        lhs = jnp.concatenate([source[:, pl.ds(pl.multiple_of(col_other, UNIT), UNIT)], source[:, pl.ds(pl.multiple_of(col_mine, UNIT), UNIT)]], axis=1)
        chunk = width // 4
        for index in range(4):
            cols = pl.ds(index * chunk, chunk)
            prod = contract_rows(lhs, grad[:, cols])
            halves[ring, :, cols] = prod[:UNIT]
            mine[ring, :, cols] = prod[UNIT:]
        ex.copy(unit, PAIR).start()

    def pair_step(unit):
        slot = lax.rem(unit, DEPTH)
        ex.copy(unit, PAIR).wait_recv()
        total[slot] = total[slot] + mine[lax.rem(unit, 2)]
        ex.copy(unit, RS1).start()

    def to_out(unit):
        start = ex.owned(unit)
        slot = lax.rem(unit, DEPTH)
        return pltpu.make_async_copy(total.at[slot, pl.ds(pl.multiple_of(start, 16), 16)], out_ref.at[pl.ds(pl.multiple_of(row_of(unit, half) + start, 16), 16)], send_sems.at[slot, LOCAL])

    def finish(unit):
        ex.copy(unit, RS3).wait()
        slot = lax.rem(unit, DEPTH)
        keep = pl.ds(pl.multiple_of(ex.owned(unit), 16), 16)
        total[slot, keep] = total[slot, keep] + recv_3[slot]
        to_out(unit).start()
        ex.copy(unit, AG3).start()

    def forward(kind):
        def stage(unit):
            if kind == AG3:
                to_out(unit).wait()
            ex.copy(unit, kind).wait()
            if kind != AGP:
                ex.copy(unit, kind + 1).start()

        return stage

    stages = [pair_step, lambda u: ex.reduce_step(u, RS1), lambda u: ex.reduce_step(u, RS2), finish, forward(AG3), forward(AG2), forward(AG1), forward(AGP)]

    def derivative(layer, index):
        load_weight(w_out, index).wait()
        load_normed(normed_2, index).wait()
        cols = block_of(index)
        gain, bias = vecs[layer, 0:1, cols], vecs[layer, 1:2, cols]
        rhs = weight[cols]
        sum_n = jnp.zeros((1, BLOCK), jnp.float32)
        sum_d = jnp.zeros((1, BLOCK), jnp.float32)
        for chunk in range(rows // BLOCK):
            part = pl.ds(chunk * BLOCK, BLOCK)
            n = normed[part, cols]
            d = jnp.where(n * gain + bias > 0.0, contract_cols(grad[part], rhs), 0.0)
            deriv[part, cols] = d
            sum_n = sum_n + jnp.sum(d * n, axis=0, keepdims=True)
            sum_d = sum_d + jnp.sum(d, axis=0, keepdims=True)
        stat_part[layer, 0:1, cols] = sum_n
        stat_part[layer, 1:2, cols] = sum_d

    lanes = width // shards

    def lane_block(index):
        return pl.ds(pl.multiple_of(index * lanes, lanes), lanes)

    def stat_scatter(layer, shift):
        peer = lax.rem(me + shift, shards)
        return pltpu.make_async_remote_copy(src_ref=stat_part.at[layer, :, lane_block(peer)], dst_ref=stat_in.at[layer, shift], send_sem=stat_sems.at[0, layer, shift], recv_sem=stat_sems.at[1, layer, shift], device_id=(peer,), device_id_type=MESH_ID)

    def stat_gather(layer, shift):
        peer = lax.rem(me + shift, shards)
        return pltpu.make_async_remote_copy(src_ref=stat_in.at[layer, 0], dst_ref=stat_ref.at[layer, :, lane_block(me)], send_sem=stat_sems.at[2, layer, shift], recv_sem=stat_sems.at[3, layer, shift], device_id=(peer,), device_id_type=MESH_ID)

    def stat_send(layer):
        for shift in range(1, shards):
            stat_scatter(layer, shift).start()

    def stat_reduce(layer):
        summed = stat_part[layer, :, lane_block(me)]
        for shift in range(1, shards):
            stat_scatter(layer, shift).wait()
            summed = summed + stat_in[layer, shift]
        stat_in[layer, 0] = summed
        stat_ref[layer, :, lane_block(me)] = summed
        for shift in range(1, shards):
            stat_gather(layer, shift).start()

    def next_grad(layer):
        for shift in range(1, shards):
            stat_gather(layer, shift).wait()

        def one(index, carry):
            cols = block_of(index)
            mean_n = stat_ref[layer, 0:1, cols] / row_count
            mean_d = stat_ref[layer, 1:2, cols] / row_count
            scale = vecs[layer, 0:1, cols] * vecs[layer, 2:3, cols]
            for chunk in range(rows // BLOCK):
                part = pl.ds(chunk * BLOCK, BLOCK)
                grad[part, cols] = ((deriv[part, cols] - mean_d - normed[part, cols] * mean_n) * scale).astype(jnp.bfloat16)

            @pl.when(layer == 0)
            def _():
                load_normed(normed_1, index).start()

            return carry

        lax.fori_loop(0, blocks, one, 0)

    stat_part[...] = jnp.zeros_like(stat_part)

    def tick(now, carry):
        for lag, stage in reversed(list(zip(BACK_LAGS, stages))):
            entered = now - lag
            layer, place = lax.div(entered, PERIOD), lax.rem(entered, PERIOD)

            @pl.when((entered >= 0) & (entered < enters) & (place < units_full))
            def _(stage=stage, layer=layer, place=place):
                stage(layer * units_full + place)

        layer, place = lax.div(now, PERIOD), lax.rem(now, PERIOD)

        @pl.when((layer < 2) & (place < units_full))
        def _():
            @pl.when(place == 0)
            def _():
                load_left.wait()

                @pl.when(layer == 0)
                def _():
                    load_grad.wait()

            produce(layer * units_full + place, left, width // 2)
            derivative(layer, place)

        @pl.when((now >= 2 * PERIOD) & (now < enters))
        def _():
            @pl.when(place == 0)
            def _():
                load_feat.wait()

            produce(layer * units_full + place, feat_in, feat_in.shape[1] // 2)

        @pl.when((layer < 2) & (place == units_full))
        def _():
            stat_send(layer)

            @pl.when(layer == 0)
            def _():
                pltpu.make_async_copy(left_1, left, load_sems.at[0]).start()
                for index in range(blocks):
                    load_weight(w_mid, index).start()

            stat_reduce(layer)

        @pl.when((layer < 2) & (place == units_full + 3))
        def _():
            next_grad(layer)

        return carry

    lax.fori_loop(0, ticks, tick, 0)
    last = 2 * units_full + units_last
    for unit in (last - 2, last - 1):
        ex.copy(unit, PAIR).wait_send()


def backward(act_2, grad_z, w_out, normed_2, act_1, w_mid, normed_1, feat, vecs, shards, row_count):
    rows, width = act_2.shape
    feat_dim = feat.shape[1]
    total_rows = 2 * width + feat_dim
    vmem = pl.BlockSpec(memory_space=pltpu.VMEM)
    hbm = pl.BlockSpec(memory_space=pl.ANY)
    return pl.pallas_call(
        functools.partial(backward_kernel, shards, row_count),
        out_shape=(jax.ShapeDtypeStruct((total_rows, width), jnp.float32), jax.ShapeDtypeStruct((2, 8, width), jnp.float32)),
        in_specs=[hbm] * 8 + [vmem],
        out_specs=(hbm, vmem),
        scratch_shapes=[
            pltpu.VMEM((rows, width), jnp.bfloat16),
            pltpu.VMEM((rows, feat_dim), jnp.bfloat16),
            pltpu.VMEM((rows, width), jnp.bfloat16),
            pltpu.VMEM((width, width), jnp.bfloat16),
            pltpu.VMEM((rows, width), jnp.float32),
            pltpu.VMEM((rows, width), jnp.float32),
            pltpu.VMEM((2, UNIT, width), jnp.float32),
            pltpu.VMEM((2, UNIT, width), jnp.float32),
            pltpu.VMEM((DEPTH, UNIT, width), jnp.float32),
            pltpu.VMEM((DEPTH, 64, width), jnp.float32),
            pltpu.VMEM((DEPTH, 32, width), jnp.float32),
            pltpu.VMEM((DEPTH, 16, width), jnp.float32),
            pltpu.VMEM((2, 8, width), jnp.float32),
            pltpu.VMEM((2, shards, 8, width // shards), jnp.float32),
            pltpu.SemaphoreType.DMA((DEPTH, 9)),
            pltpu.SemaphoreType.DMA((DEPTH, 9)),
            pltpu.SemaphoreType.DMA((3,)),
            pltpu.SemaphoreType.DMA((width // BLOCK,)),
            pltpu.SemaphoreType.DMA((width // BLOCK,)),
            pltpu.SemaphoreType.DMA((4, 2, shards)),
        ],
        compiler_params=pltpu.CompilerParams(collective_id=3, has_side_effects=True, vmem_limit_bytes=VMEM_LIMIT),
        cost_estimate=pl.CostEstimate(flops=2 * rows * width * (2 * width + total_rows), bytes_accessed=16 * width * width, transcendentals=0),
        name="backward",
    )(act_2, grad_z, w_out, normed_2, act_1, w_mid, normed_1, feat, vecs)


def solution(mesh):
    shards = mesh.shape[DATA_AXIS]
    row_part = P(DATA_AXIS, None)
    replicated = P()

    def local_step(feat_a, feat_b, w_in, w_mid, w_out, t_in, t_mid, t_out, gain_1, bias_1, gain_2, bias_2, off_weight):
        row_count = feat_a.shape[0] * shards

        def norm_pair(pre_a, pre_b):
            stat_means = stats_all_reduce([jnp.sum(pre_a, axis=0), jnp.sum(pre_a * pre_a, axis=0), jnp.sum(pre_b, axis=0), jnp.sum(pre_b * pre_b, axis=0)], shards) / row_count
            inv_a = lax.rsqrt(stat_means[1] - stat_means[0] * stat_means[0] + NORM_EPS)
            inv_b = lax.rsqrt(stat_means[3] - stat_means[2] * stat_means[2] + NORM_EPS)
            return (pre_a - stat_means[0]) * inv_a, inv_a, (pre_b - stat_means[2]) * inv_b

        def hidden_pair(in_a, in_b, weight_a, weight_b, gain_vec, bias_vec):
            normed_a, inv_a, normed_b = norm_pair(jnp.dot(in_a, weight_a, preferred_element_type=jnp.float32), jnp.dot(in_b, weight_b, preferred_element_type=jnp.float32))
            pre_act = normed_a * gain_vec + bias_vec
            act_a = jnp.maximum(pre_act, 0.0).astype(jnp.bfloat16)
            act_b = jnp.maximum(normed_b * gain_vec + bias_vec, 0.0).astype(jnp.bfloat16)
            return act_a, act_b, normed_a, inv_a

        act_1, teach_1, normed_1, inv_1 = hidden_pair(feat_a, feat_b, w_in, t_in, gain_1, bias_1)
        act_2, teach_2, normed_2, inv_2 = hidden_pair(act_1, teach_1, w_mid, t_mid, gain_2, bias_2)
        zh_a, inv_z, zh_b = norm_pair(jnp.dot(act_2, w_out, preferred_element_type=jnp.float32), jnp.dot(teach_2, t_out, preferred_element_type=jnp.float32))
        emb_a = zh_a.astype(jnp.bfloat16)
        emb_b = zh_b.astype(jnp.bfloat16)
        grad_c, loss_part = corr_grad(emb_a, emb_b, off_weight, row_count)
        grad_emb = contract_cols(emb_b, grad_c) / row_count
        stat_sums = stats_all_reduce([jnp.sum(grad_emb, axis=0), jnp.sum(grad_emb * zh_a, axis=0), jnp.sum(loss_part, axis=0)], shards)
        loss_value = jnp.sum(stat_sums[2])
        grad_z = ((grad_emb - stat_sums[0] / row_count - zh_a * (stat_sums[1] / row_count)) * inv_z).astype(jnp.bfloat16)
        pad = jnp.zeros((5,) + gain_1.shape, jnp.float32)
        vecs = jnp.stack([jnp.concatenate([jnp.stack([gain_2, bias_2, inv_2]), pad]), jnp.concatenate([jnp.stack([gain_1, bias_1, inv_1]), pad])])
        sums, stats = backward(act_2, grad_z, w_out, normed_2, act_1, w_mid, normed_1, feat_a, vecs, shards, row_count)
        width = w_mid.shape[0]
        return (loss_value, grad_emb, sums[2 * width :], sums[width : 2 * width], sums[:width], stats[1, 0], stats[1, 1], stats[0, 0], stats[0, 1])

    return jax.shard_map(local_step, mesh=mesh, in_specs=(row_part, row_part) + (replicated,) * 11, out_specs=(replicated, row_part) + (replicated,) * 7, check_vma=False)
```

```python
import functools

import jax
import jax.numpy as jnp
from jax import lax
from jax.experimental import pallas as pl
from jax.experimental.pallas import tpu as pltpu
from jax.sharding import PartitionSpec as P

NORM_EPS = 1e-5
DATA_AXIS = "data"
MESH_ID = pl.DeviceIdType.MESH
UNIT = 128
VMEM_LIMIT = 66_000_000


def contract_rows(left_op, right_op):
    return lax.dot_general(left_op, right_op, (((0,), (0,)), ((), ())), preferred_element_type=jnp.float32)


def contract_cols(left_op, right_op):
    return lax.dot_general(left_op, right_op, (((1,), (1,)), ((), ())), preferred_element_type=jnp.float32)


def flip(me, mask):
    bit = lax.rem(lax.div(me, mask), 2)
    return me + mask * (1 - 2 * bit), bit


class SumExchange:
    def __init__(self, me, shards, slots, send_sems, recv_sems):
        self.me, self.shards, self.slots, self.send_sems, self.recv_sems = me, shards, slots, send_sems, recv_sems

    def copy(self, index, peer, slot):
        return pltpu.make_async_remote_copy(src_ref=self.slots.at[index, self.me], dst_ref=self.slots.at[index, slot], send_sem=self.send_sems.at[index, peer], recv_sem=self.recv_sems.at[index, slot], device_id=(peer,), device_id_type=MESH_ID)

    def peers(self):
        return [lax.rem(self.me + shift, self.shards) for shift in range(1, self.shards)]

    def start(self, index):
        for peer in self.peers():
            self.copy(index, peer, self.me).start()

    def finish(self, index):
        for peer in self.peers():
            self.copy(index, peer, peer).wait_recv()
            self.copy(index, peer, self.me).wait_send()
        summed = self.slots[index, 0]
        for slot in range(1, self.shards):
            summed = summed + self.slots[index, slot]
        return summed


def enter_all(me, shards):
    barrier = pltpu.get_barrier_semaphore()
    for shift in range(1, shards):
        pl.semaphore_signal(barrier, inc=1, device_id=(lax.rem(me + shift, shards),), device_id_type=MESH_ID)
    pl.semaphore_wait(barrier, shards - 1)


COLS = 512
ROWS = 256


def forward_kernel(shards, row_count, feat_a, feat_b, w_in, t_in, w_mid, t_mid, w_out, t_out, affine, act_1, act_2, normed_1, normed_2, normed_z, emb_a, emb_b, inv_ref, pre, act, feat, weight_in, weight, slots, sums, send_sems, recv_sems, load_sems, store_sems):
    me = lax.axis_index(DATA_AXIS)
    rows, width = act_1.shape
    groups = width // COLS
    copies = [pltpu.make_async_copy(src, dst, load_sems.at[index]) for index, (src, dst) in enumerate([(feat_a, feat.at[0]), (w_in, weight_in.at[0]), (feat_b, feat.at[1]), (t_in, weight_in.at[1]), (w_mid, weight.at[0]), (t_mid, weight.at[1]), (w_out, weight.at[0]), (t_out, weight.at[1])])]
    for index in range(6):
        copies[index].start()
    enter_all(me, shards)
    ex = SumExchange(me, shards, slots, send_sems, recv_sems)

    def product(index, source, matrix, target):
        def group(number, carry):
            cols = pl.ds(pl.multiple_of(number * COLS, COLS), COLS)
            total = jnp.zeros((1, COLS), jnp.float32)
            squares = jnp.zeros((1, COLS), jnp.float32)
            for chunk in range(rows // ROWS):
                part = pl.ds(chunk * ROWS, ROWS)
                out = jnp.dot(source[part], matrix[:, cols], preferred_element_type=jnp.float32)
                target[part, cols] = out
                total = total + jnp.sum(out, axis=0, keepdims=True)
                squares = squares + jnp.sum(out * out, axis=0, keepdims=True)
            slots[index, me, pl.ds(number, 1)] = total
            slots[index, me, pl.ds(number + groups, 1)] = squares
            return carry

        lax.fori_loop(0, groups, group, 0)
        ex.start(index)

    def normalise(index, source, target, layer, keep):
        summed = ex.finish(index) / row_count
        mean = summed[:groups]
        inv = lax.rsqrt(summed[groups:] - mean * mean + NORM_EPS)
        sums[index, :groups] = mean
        sums[index, groups:] = inv
        if keep is not None:
            inv_ref[layer, :groups] = inv

        def group(number, carry):
            cols = pl.ds(pl.multiple_of(number * COLS, COLS), COLS)
            col_mean = sums[index, pl.ds(number, 1)]
            col_inv = sums[index, pl.ds(number + groups, 1)]
            for chunk in range(rows // ROWS):
                part = pl.ds(chunk * ROWS, ROWS)
                out = (source[part, cols] - col_mean) * col_inv
                if keep is not None:
                    source[part, cols] = out
                if layer < 2:
                    out = jnp.maximum(out * affine[2 * layer : 2 * layer + 1, cols] + affine[2 * layer + 1 : 2 * layer + 2, cols], 0.0)
                target[part, cols] = out.astype(jnp.bfloat16)
            return carry

        lax.fori_loop(0, groups, group, 0)

    def store(number, src, dst):
        copy = pltpu.make_async_copy(src, dst, store_sems.at[number])
        copy.start()
        return copy

    copies[0].wait()
    copies[1].wait()
    product(0, feat.at[0], weight_in.at[0], pre.at[0])
    copies[2].wait()
    copies[3].wait()
    product(1, feat.at[1], weight_in.at[1], pre.at[1])
    normalise(0, pre.at[0], act.at[0], 0, normed_1)
    out_n1 = store(0, pre.at[0], normed_1)
    out_x1 = store(1, act.at[0], act_1)
    copies[4].wait()
    product(2, act.at[0], weight.at[0], pre.at[2])
    copies[6].start()
    normalise(1, pre.at[1], act.at[1], 0, None)
    copies[5].wait()
    out_n1.wait()
    product(3, act.at[1], weight.at[1], pre.at[0])
    copies[7].start()
    out_x1.wait()
    normalise(2, pre.at[2], act.at[0], 1, normed_2)
    out_n2 = store(2, pre.at[2], normed_2)
    out_x2 = store(3, act.at[0], act_2)
    copies[6].wait()
    product(4, act.at[0], weight.at[0], pre.at[1])
    normalise(3, pre.at[0], act.at[1], 1, None)
    copies[7].wait()
    out_n2.wait()
    product(5, act.at[1], weight.at[1], pre.at[2])
    out_x2.wait()
    normalise(4, pre.at[1], act.at[0], 2, normed_z)
    out_z = store(4, pre.at[1], normed_z)
    out_a = store(5, act.at[0], emb_a)
    normalise(5, pre.at[2], act.at[1], 2, None)
    out_b = store(6, act.at[1], emb_b)
    for copy in (out_z, out_a, out_b):
        copy.wait()


def forward_pass(feat_a, feat_b, w_in, t_in, w_mid, t_mid, w_out, t_out, affine, shards, row_count):
    rows, feat_dim = feat_a.shape
    width = w_mid.shape[0]
    groups = width // COLS
    vmem = pl.BlockSpec(memory_space=pltpu.VMEM)
    hbm = pl.BlockSpec(memory_space=pl.ANY)
    half_out = jax.ShapeDtypeStruct((rows, width), jnp.bfloat16)
    full_out = jax.ShapeDtypeStruct((rows, width), jnp.float32)
    return pl.pallas_call(
        functools.partial(forward_kernel, shards, row_count),
        out_shape=(half_out, half_out, full_out, full_out, full_out, half_out, half_out, jax.ShapeDtypeStruct((3, 8, COLS), jnp.float32)),
        in_specs=[hbm] * 8 + [vmem],
        out_specs=(hbm,) * 7 + (vmem,),
        scratch_shapes=[
            pltpu.VMEM((3, rows, width), jnp.float32),
            pltpu.VMEM((2, rows, width), jnp.bfloat16),
            pltpu.VMEM((2, rows, feat_dim), jnp.bfloat16),
            pltpu.VMEM((2, feat_dim, width), jnp.bfloat16),
            pltpu.VMEM((2, width, width), jnp.bfloat16),
            pltpu.VMEM((6, shards, 2 * groups, COLS), jnp.float32),
            pltpu.VMEM((6, 2 * groups, COLS), jnp.float32),
            pltpu.SemaphoreType.DMA((6, shards)),
            pltpu.SemaphoreType.DMA((6, shards)),
            pltpu.SemaphoreType.DMA((8,)),
            pltpu.SemaphoreType.DMA((7,)),
        ],
        compiler_params=pltpu.CompilerParams(collective_id=4, has_side_effects=True, vmem_limit_bytes=VMEM_LIMIT),
        cost_estimate=pl.CostEstimate(flops=4 * rows * width * (2 * width + feat_dim), bytes_accessed=24 * width * width, transcendentals=0),
        name="forward",
    )(feat_a, feat_b, w_in, t_in, w_mid, t_mid, w_out, t_out, affine)


PAIR, RS1, RS2, RS3, AG3, AG2, AG1, AGP, LOCAL = range(9)


class Exchange:
    def __init__(self, me, ring, halves, gathered, recv_pair, recv_1, recv_2, recv_3, total, send_sems, recv_sems, row_of, depth, send_total=False):
        self.depth, self.send_total = depth, send_total
        self.me, self.ring, self.halves, self.gathered = me, ring, halves, gathered
        self.recv_pair, self.recv_1, self.recv_2, self.recv_3, self.total = recv_pair, recv_1, recv_2, recv_3, total
        self.send_sems, self.recv_sems, self.row_of = send_sems, recv_sems, row_of

    def axes(self, unit):
        def mask(shift):
            axis = lax.rem(unit + shift, 3)
            return 2 + axis + axis * axis

        (p1, b1), (p2, b2), (p3, b3) = (flip(self.me, mask(shift)) for shift in range(3))
        return (p1, p2, p3), (b1, b2, b3)

    def copy(self, unit, kind):
        (p1, p2, p3), (b1, b2, b3) = self.axes(unit)
        partner, half = flip(self.me, 1)

        def rows(start, size):
            return pl.ds(pl.multiple_of(start, 16), size)

        slot = lax.rem(unit, self.depth)
        total = self.total.at[slot]
        row = self.row_of(unit, half)
        if kind == PAIR:
            src, dst, peer = self.halves.at[lax.rem(unit, self.ring)], self.recv_pair.at[slot], partner
        elif kind == RS1:
            src, dst, peer = total.at[rows((1 - b1) * 64, 64)], self.recv_1.at[slot], p1
        elif kind == RS2:
            src, dst, peer = total.at[rows(b1 * 64 + (1 - b2) * 32, 32)], self.recv_2.at[slot], p2
        elif kind == RS3:
            src, dst, peer = total.at[rows(b1 * 64 + b2 * 32 + (1 - b3) * 16, 16)], self.recv_3.at[slot], p3
        else:
            start, size, peer = {
                AG3: (b1 * 64 + b2 * 32 + b3 * 16, 16, p3),
                AG2: (b1 * 64 + b2 * 32, 32, p2),
                AG1: (b1 * 64, 64, p1),
                AGP: (0, 128, partner),
            }[kind]
            src = dst = self.gathered.at[rows(row + start, size)]
            if kind == AG3 and self.send_total:
                src = total.at[rows(start, size)]
        return pltpu.make_async_remote_copy(src_ref=src, dst_ref=dst, send_sem=self.send_sems.at[slot, kind], recv_sem=self.recv_sems.at[slot, kind], device_id=(peer,), device_id_type=MESH_ID)

    def reduce_step(self, unit, kind):
        _, (b1, b2, b3) = self.axes(unit)
        self.copy(unit, kind).wait()
        if kind == PAIR:
            start, size, landed = 0, 128, self.recv_pair
        elif kind == RS1:
            start, size, landed = b1 * 64, 64, self.recv_1
        else:
            start, size, landed = b1 * 64 + b2 * 32, 32, self.recv_2
        keep = pl.ds(pl.multiple_of(start, 16), size)
        slot = lax.rem(unit, self.depth)
        self.total[slot, keep] = self.total[slot, keep] + landed[slot]
        self.copy(unit, kind + 1).start()

    def owned(self, unit):
        _, (b1, b2, b3) = self.axes(unit)
        return b1 * 64 + b2 * 32 + b3 * 16


def enter(me):
    barrier = pltpu.get_barrier_semaphore()
    for mask in (1, 2, 4, 8):
        pl.semaphore_signal(barrier, inc=1, device_id=(flip(me, mask)[0],), device_id_type=MESH_ID)
    pl.semaphore_wait(barrier, 4)


def pipeline(units, lags, stages):
    def step(now, carry):
        for lag, stage in reversed(list(zip(lags, stages))):
            unit = now - lag

            @pl.when((unit >= 0) & (unit < units))
            def _(unit=unit, stage=stage):
                stage(unit)

        return carry

    lax.fori_loop(0, units + max(lags), step, 0)


def product_unit(left_ref, right_ref, col_other, col_mine, halves, total, slot, unit, blocks):
    left = jnp.concatenate([left_ref[:, pl.ds(pl.multiple_of(col_other, UNIT), UNIT)], left_ref[:, pl.ds(pl.multiple_of(col_mine, UNIT), UNIT)]], axis=1)
    width = right_ref.shape[1] // blocks
    for block in range(blocks):
        cols = pl.ds(block * width, width)
        out = contract_rows(left, right_ref[:, cols])
        halves[slot, :, cols] = out[:UNIT]
        total[unit, :, cols] = out[UNIT:]


RING = 3
CORR_LAGS = (0, 1, 4, 6, 8, 10, 13, 17, 18)


def corr_kernel(shards, row_count, off_ref, inv_ref, left_ref, right_ref, normed, emb_out, back_out, loss_ref, grad_ref, emb_grad, back, norm_in, loss_acc, wide, slots, halves, recv_pair, recv_1, recv_2, recv_3, total, send_sems, recv_sems, sum_send, sum_recv, norm_sems, store_sems):
    me = lax.axis_index(DATA_AXIS)
    rows, width = right_ref.shape
    half_rows = width // 2
    units = half_rows // UNIT
    groups = width // COLS
    _, half = flip(me, 1)
    enter_all(me, shards)
    ex = Exchange(me, RING, halves, grad_ref, recv_pair, recv_1, recv_2, recv_3, total, send_sems, recv_sems, lambda unit, h: h * half_rows + unit * UNIT, units)
    sums = SumExchange(me, shards, slots, sum_send, sum_recv)
    loss_acc[...] = jnp.zeros_like(loss_acc)

    def produce(unit):
        @pl.when(unit >= RING)
        def _():
            ex.copy(unit - RING, PAIR).wait_send()

        product_unit(left_ref, right_ref, (1 - half) * half_rows + unit * UNIT, half * half_rows + unit * UNIT, halves, total, lax.rem(unit, RING), unit, 4)
        ex.copy(unit, PAIR).start()

    def pair_step(unit):
        ex.copy(unit, PAIR).wait_recv()
        total[unit] = total[unit] + recv_pair[unit]
        ex.copy(unit, RS1).start()

    def finish(unit):
        ex.copy(unit, RS3).wait()
        start = ex.owned(unit)
        keep = pl.ds(pl.multiple_of(start, 16), 16)
        corr = (total[unit, keep] + recv_3[unit]) * (1.0 / row_count)
        row = half * half_rows + unit * UNIT + start
        on_diag = lax.broadcasted_iota(jnp.int32, (16, width), 0) + row == lax.broadcasted_iota(jnp.int32, (16, width), 1)
        off_weight = off_ref[0, 0]
        miss = 1.0 - corr
        terms = jnp.where(on_diag, miss * miss, off_weight * (corr * corr))
        loss_acc[...] += terms[:8] + terms[8:]
        grad = jnp.where(on_diag, -2.0 * miss, 2.0 * off_weight * corr).astype(jnp.bfloat16)
        grad_ref[pl.ds(pl.multiple_of(row, 16), 16)] = grad
        ex.copy(unit, AG3).start()

    def forward(kind):
        def stage(unit):
            ex.copy(unit, kind).wait()
            if kind != AGP:
                ex.copy(unit, kind + 1).start()

            if kind == AG1:
                for side in range(2):
                    load_norm(row_of(unit, side), lax.rem(unit, 2), side).start()

        return stage

    def row_of(unit, side):
        return (half + side * (1 - 2 * half)) * half_rows + unit * UNIT

    def lanes(start):
        return pl.ds(pl.multiple_of(start, UNIT), UNIT)

    def load_norm(start, slot, side):
        return pltpu.make_async_copy(normed.at[:, lanes(start)], norm_in.at[slot, side], norm_sems.at[slot, side])

    def embed(unit):
        ex.copy(unit, AGP).wait()
        slot = lax.rem(unit, 2)
        starts = [row_of(unit, side) for side in range(2)]
        rhs = jnp.concatenate([grad_ref[lanes(start)] for start in starts], axis=0)
        for side in range(2):
            load_norm(starts[side], slot, side).wait()
        plain = [jnp.zeros((1, UNIT), jnp.float32)] * 2
        crossed = [jnp.zeros((1, UNIT), jnp.float32)] * 2
        for chunk in range(rows // ROWS):
            part = pl.ds(chunk * ROWS, ROWS)
            out = contract_cols(right_ref[part], rhs) * (1.0 / row_count)
            for side in range(2):
                piece = out[:, side * UNIT : (side + 1) * UNIT]
                emb_grad[part, lanes(starts[side])] = piece
                plain[side] = plain[side] + jnp.sum(piece, axis=0, keepdims=True)
                crossed[side] = crossed[side] + jnp.sum(piece * norm_in[slot, side, part], axis=0, keepdims=True)
        for side in range(2):
            wide[0:1, lanes(starts[side])] = plain[side]
            wide[1:2, lanes(starts[side])] = crossed[side]

    pipeline(units, CORR_LAGS, [produce, pair_step, lambda u: ex.reduce_step(u, RS1), lambda u: ex.reduce_step(u, RS2), finish, forward(AG3), forward(AG2), forward(AG1), embed])
    for unit in range(units - RING, units):
        ex.copy(unit, PAIR).wait_send()
    folded = loss_acc[:, :UNIT]
    for index in range(1, width // UNIT):
        folded = folded + loss_acc[:, index * UNIT : (index + 1) * UNIT]
    slots[0, me, :, COLS:] = folded
    for index in range(groups):
        cols = pl.ds(index * COLS, COLS)
        slots[0, me, index : index + 1, :COLS] = wide[0:1, cols]
        slots[0, me, groups + index : groups + index + 1, :COLS] = wide[1:2, cols]
    sums.start(0)
    store_emb = pltpu.make_async_copy(emb_grad, emb_out, store_sems.at[0])
    store_emb.start()

    def load_block(index, slot):
        return [load_norm((2 * index + side) * UNIT, slot, side) for side in range(2)]

    for copy in load_block(0, 0) + load_block(1, 1):
        copy.start()
    summed = sums.finish(0)
    loss_ref[...] = summed[:, COLS:]
    means = summed[:, :COLS] / row_count
    for index in range(groups):
        cols = pl.ds(index * COLS, COLS)
        wide[0:1, cols] = means[index : index + 1]
        wide[1:2, cols] = means[groups + index : groups + index + 1]
        wide[2:3, cols] = inv_ref[2, index : index + 1]

    def norm_back(index, carry):
        slot = lax.rem(index, 2)
        for side, copy in enumerate(load_block(index, slot)):
            copy.wait()
            start = (2 * index + side) * UNIT
            mean_g, mean_gn, inv = wide[0:1, lanes(start)], wide[1:2, lanes(start)], wide[2:3, lanes(start)]
            for chunk in range(rows // ROWS):
                part = pl.ds(chunk * ROWS, ROWS)
                back[part, lanes(start)] = ((emb_grad[part, lanes(start)] - mean_g - norm_in[slot, side, part] * mean_gn) * inv).astype(jnp.bfloat16)

        @pl.when(index + 2 < width // (2 * UNIT))
        def _():
            for copy in load_block(index + 2, slot):
                copy.start()

        return carry

    lax.fori_loop(0, width // (2 * UNIT), norm_back, 0)
    store_back = pltpu.make_async_copy(back, back_out, store_sems.at[1])
    store_back.start()
    store_emb.wait()
    store_back.wait()


def exchange_scratch(units, width):
    return [
        pltpu.VMEM((RING, UNIT, width), jnp.float32),
        pltpu.VMEM((units, UNIT, width), jnp.float32),
        pltpu.VMEM((units, 64, width), jnp.float32),
        pltpu.VMEM((units, 32, width), jnp.float32),
        pltpu.VMEM((units, 16, width), jnp.float32),
        pltpu.VMEM((units, UNIT, width), jnp.float32),
        pltpu.SemaphoreType.DMA((units, 9)),
        pltpu.SemaphoreType.DMA((units, 9)),
    ]


def corr_grad(emb_a, emb_b, normed, inv_std, off_weight, shards, row_count):
    rows, width = emb_a.shape
    vmem = pl.BlockSpec(memory_space=pltpu.VMEM)
    hbm = pl.BlockSpec(memory_space=pl.ANY)
    return pl.pallas_call(
        functools.partial(corr_kernel, shards, row_count),
        out_shape=(jax.ShapeDtypeStruct((rows, width), jnp.float32), jax.ShapeDtypeStruct((rows, width), jnp.bfloat16), jax.ShapeDtypeStruct((8, UNIT), jnp.float32)),
        in_specs=[pl.BlockSpec(memory_space=pltpu.SMEM), vmem, vmem, vmem, hbm],
        out_specs=(hbm, hbm, vmem),
        scratch_shapes=[
            pltpu.VMEM((width, width), jnp.bfloat16),
            pltpu.VMEM((rows, width), jnp.float32),
            pltpu.VMEM((rows, width), jnp.bfloat16),
            pltpu.VMEM((2, 2, rows, UNIT), jnp.float32),
            pltpu.VMEM((8, width), jnp.float32),
            pltpu.VMEM((8, width), jnp.float32),
            pltpu.VMEM((1, shards, 8, COLS + UNIT), jnp.float32),
        ]
        + exchange_scratch(width // 2 // UNIT, width)
        + [pltpu.SemaphoreType.DMA((1, shards)), pltpu.SemaphoreType.DMA((1, shards)), pltpu.SemaphoreType.DMA((2, 2)), pltpu.SemaphoreType.DMA((2,))],
        compiler_params=pltpu.CompilerParams(collective_id=2, has_side_effects=True, vmem_limit_bytes=VMEM_LIMIT),
        cost_estimate=pl.CostEstimate(flops=4 * rows * width * width, bytes_accessed=8 * width * width, transcendentals=0),
        name="corr_grad",
    )(off_weight.reshape(1, 1), inv_std, emb_a, emb_b, normed)


DEPTH = 12
PERIOD = 12
BLOCK = 256
BACK_LAGS = (1, 4, 6, 7, 9, 12, 15, 16)


def backward_kernel(shards, row_count, left_2, grad_z, w_out, normed_2, left_1, w_mid, normed_1, feat, vecs, out_ref, stat_ref, left, feat_in, grad, weight, normed, deriv, halves, mine, total, recv_1, recv_2, recv_3, stat_part, stat_in, send_sems, recv_sems, load_sems, weight_sems, normed_sems, stat_sems):
    me = lax.axis_index(DATA_AXIS)
    _, half = flip(me, 1)
    rows, width = left.shape
    blocks = width // BLOCK
    units_full = width // 2 // UNIT
    units_last = feat_in.shape[1] // 2 // UNIT
    enters = 2 * PERIOD + units_last
    ticks = enters + max(BACK_LAGS)

    load_left = pltpu.make_async_copy(left_2, left, load_sems.at[0])
    load_grad = pltpu.make_async_copy(grad_z, grad, load_sems.at[1])
    load_feat = pltpu.make_async_copy(feat, feat_in, load_sems.at[2])

    def block_of(index):
        return pl.ds(pl.multiple_of(index * BLOCK, BLOCK), BLOCK)

    def load_weight(source, index):
        return pltpu.make_async_copy(source.at[block_of(index)], weight.at[block_of(index)], weight_sems.at[index])

    def load_normed(source, index):
        return pltpu.make_async_copy(source.at[:, block_of(index)], normed.at[:, block_of(index)], normed_sems.at[index])

    load_left.start()
    load_grad.start()
    for index in range(blocks):
        load_weight(w_out, index).start()
        load_normed(normed_2, index).start()
    load_feat.start()

    barrier = pltpu.get_barrier_semaphore()
    for shift in range(1, shards):
        pl.semaphore_signal(barrier, inc=1, device_id=(lax.rem(me + shift, shards),), device_id_type=MESH_ID)
    pl.semaphore_wait(barrier, shards - 1)

    def row_of(unit, h):
        layer = lax.div(unit, units_full)
        part = width // 2 - (width // 2 - feat_in.shape[1] // 2) * lax.div(layer, 2)
        return layer * width + h * part + lax.rem(unit, units_full) * UNIT

    ex = Exchange(me, 2, halves, out_ref, total, recv_1, recv_2, recv_3, total, send_sems, recv_sems, row_of, DEPTH, send_total=True)

    def produce(unit, source, part):
        @pl.when(unit >= 2)
        def _():
            ex.copy(unit - 2, PAIR).wait_send()

        local = lax.rem(unit, units_full) * UNIT
        ring = lax.rem(unit, 2)
        col_other, col_mine = (1 - half) * part + local, half * part + local
        lhs = jnp.concatenate([source[:, pl.ds(pl.multiple_of(col_other, UNIT), UNIT)], source[:, pl.ds(pl.multiple_of(col_mine, UNIT), UNIT)]], axis=1)
        chunk = width // 4
        for index in range(4):
            cols = pl.ds(index * chunk, chunk)
            prod = contract_rows(lhs, grad[:, cols])
            halves[ring, :, cols] = prod[:UNIT]
            mine[ring, :, cols] = prod[UNIT:]
        ex.copy(unit, PAIR).start()

    def pair_step(unit):
        slot = lax.rem(unit, DEPTH)
        ex.copy(unit, PAIR).wait_recv()
        total[slot] = total[slot] + mine[lax.rem(unit, 2)]
        ex.copy(unit, RS1).start()

    def to_out(unit):
        start = ex.owned(unit)
        slot = lax.rem(unit, DEPTH)
        return pltpu.make_async_copy(total.at[slot, pl.ds(pl.multiple_of(start, 16), 16)], out_ref.at[pl.ds(pl.multiple_of(row_of(unit, half) + start, 16), 16)], send_sems.at[slot, LOCAL])

    def finish(unit):
        ex.copy(unit, RS3).wait()
        slot = lax.rem(unit, DEPTH)
        keep = pl.ds(pl.multiple_of(ex.owned(unit), 16), 16)
        total[slot, keep] = total[slot, keep] + recv_3[slot]
        to_out(unit).start()
        ex.copy(unit, AG3).start()

    def forward(kind):
        def stage(unit):
            if kind == AG3:
                to_out(unit).wait()
            ex.copy(unit, kind).wait()
            if kind != AGP:
                ex.copy(unit, kind + 1).start()

        return stage

    stages = [pair_step, lambda u: ex.reduce_step(u, RS1), lambda u: ex.reduce_step(u, RS2), finish, forward(AG3), forward(AG2), forward(AG1), forward(AGP)]

    def derivative(layer, index):
        load_weight(w_out, index).wait()
        load_normed(normed_2, index).wait()
        cols = block_of(index)
        gain, bias = vecs[layer, 0:1, cols], vecs[layer, 1:2, cols]
        rhs = weight[cols]
        sum_n = jnp.zeros((1, BLOCK), jnp.float32)
        sum_d = jnp.zeros((1, BLOCK), jnp.float32)
        for chunk in range(rows // BLOCK):
            part = pl.ds(chunk * BLOCK, BLOCK)
            n = normed[part, cols]
            d = jnp.where(n * gain + bias > 0.0, contract_cols(grad[part], rhs), 0.0)
            deriv[part, cols] = d
            sum_n = sum_n + jnp.sum(d * n, axis=0, keepdims=True)
            sum_d = sum_d + jnp.sum(d, axis=0, keepdims=True)
        stat_part[layer, 0:1, cols] = sum_n
        stat_part[layer, 1:2, cols] = sum_d

    lanes = width // shards

    def lane_block(index):
        return pl.ds(pl.multiple_of(index * lanes, lanes), lanes)

    def stat_scatter(layer, shift):
        peer = lax.rem(me + shift, shards)
        return pltpu.make_async_remote_copy(src_ref=stat_part.at[layer, :, lane_block(peer)], dst_ref=stat_in.at[layer, shift], send_sem=stat_sems.at[0, layer, shift], recv_sem=stat_sems.at[1, layer, shift], device_id=(peer,), device_id_type=MESH_ID)

    def stat_gather(layer, shift):
        peer = lax.rem(me + shift, shards)
        return pltpu.make_async_remote_copy(src_ref=stat_in.at[layer, 0], dst_ref=stat_ref.at[layer, :, lane_block(me)], send_sem=stat_sems.at[2, layer, shift], recv_sem=stat_sems.at[3, layer, shift], device_id=(peer,), device_id_type=MESH_ID)

    def stat_send(layer):
        for shift in range(1, shards):
            stat_scatter(layer, shift).start()

    def stat_reduce(layer):
        summed = stat_part[layer, :, lane_block(me)]
        for shift in range(1, shards):
            stat_scatter(layer, shift).wait()
            summed = summed + stat_in[layer, shift]
        stat_in[layer, 0] = summed
        stat_ref[layer, :, lane_block(me)] = summed
        for shift in range(1, shards):
            stat_gather(layer, shift).start()

    def next_grad(layer):
        for shift in range(1, shards):
            stat_gather(layer, shift).wait()

        def one(index, carry):
            cols = block_of(index)
            mean_n = stat_ref[layer, 0:1, cols] / row_count
            mean_d = stat_ref[layer, 1:2, cols] / row_count
            scale = vecs[layer, 0:1, cols] * vecs[layer, 2:3, cols]
            for chunk in range(rows // BLOCK):
                part = pl.ds(chunk * BLOCK, BLOCK)
                grad[part, cols] = ((deriv[part, cols] - mean_d - normed[part, cols] * mean_n) * scale).astype(jnp.bfloat16)

            @pl.when(layer == 0)
            def _():
                load_normed(normed_1, index).start()

            return carry

        lax.fori_loop(0, blocks, one, 0)

    stat_part[...] = jnp.zeros_like(stat_part)

    def tick(now, carry):
        for lag, stage in reversed(list(zip(BACK_LAGS, stages))):
            entered = now - lag
            layer, place = lax.div(entered, PERIOD), lax.rem(entered, PERIOD)

            @pl.when((entered >= 0) & (entered < enters) & (place < units_full))
            def _(stage=stage, layer=layer, place=place):
                stage(layer * units_full + place)

        layer, place = lax.div(now, PERIOD), lax.rem(now, PERIOD)

        @pl.when((layer < 2) & (place < units_full))
        def _():
            @pl.when(place == 0)
            def _():
                load_left.wait()

                @pl.when(layer == 0)
                def _():
                    load_grad.wait()

            produce(layer * units_full + place, left, width // 2)
            derivative(layer, place)

        @pl.when((now >= 2 * PERIOD) & (now < enters))
        def _():
            @pl.when(place == 0)
            def _():
                load_feat.wait()

            produce(layer * units_full + place, feat_in, feat_in.shape[1] // 2)

        @pl.when((layer < 2) & (place == units_full))
        def _():
            stat_send(layer)

            @pl.when(layer == 0)
            def _():
                pltpu.make_async_copy(left_1, left, load_sems.at[0]).start()
                for index in range(blocks):
                    load_weight(w_mid, index).start()

            stat_reduce(layer)

        @pl.when((layer < 2) & (place == units_full + 3))
        def _():
            next_grad(layer)

        return carry

    lax.fori_loop(0, ticks, tick, 0)
    last = 2 * units_full + units_last
    for unit in (last - 2, last - 1):
        ex.copy(unit, PAIR).wait_send()


def backward(act_2, grad_z, w_out, normed_2, act_1, w_mid, normed_1, feat, vecs, shards, row_count):
    rows, width = act_2.shape
    feat_dim = feat.shape[1]
    total_rows = 2 * width + feat_dim
    vmem = pl.BlockSpec(memory_space=pltpu.VMEM)
    hbm = pl.BlockSpec(memory_space=pl.ANY)
    return pl.pallas_call(
        functools.partial(backward_kernel, shards, row_count),
        out_shape=(jax.ShapeDtypeStruct((total_rows, width), jnp.float32), jax.ShapeDtypeStruct((2, 8, width), jnp.float32)),
        in_specs=[hbm] * 8 + [vmem],
        out_specs=(hbm, vmem),
        scratch_shapes=[
            pltpu.VMEM((rows, width), jnp.bfloat16),
            pltpu.VMEM((rows, feat_dim), jnp.bfloat16),
            pltpu.VMEM((rows, width), jnp.bfloat16),
            pltpu.VMEM((width, width), jnp.bfloat16),
            pltpu.VMEM((rows, width), jnp.float32),
            pltpu.VMEM((rows, width), jnp.float32),
            pltpu.VMEM((2, UNIT, width), jnp.float32),
            pltpu.VMEM((2, UNIT, width), jnp.float32),
            pltpu.VMEM((DEPTH, UNIT, width), jnp.float32),
            pltpu.VMEM((DEPTH, 64, width), jnp.float32),
            pltpu.VMEM((DEPTH, 32, width), jnp.float32),
            pltpu.VMEM((DEPTH, 16, width), jnp.float32),
            pltpu.VMEM((2, 8, width), jnp.float32),
            pltpu.VMEM((2, shards, 8, width // shards), jnp.float32),
            pltpu.SemaphoreType.DMA((DEPTH, 9)),
            pltpu.SemaphoreType.DMA((DEPTH, 9)),
            pltpu.SemaphoreType.DMA((3,)),
            pltpu.SemaphoreType.DMA((width // BLOCK,)),
            pltpu.SemaphoreType.DMA((width // BLOCK,)),
            pltpu.SemaphoreType.DMA((4, 2, shards)),
        ],
        compiler_params=pltpu.CompilerParams(collective_id=3, has_side_effects=True, vmem_limit_bytes=VMEM_LIMIT),
        cost_estimate=pl.CostEstimate(flops=2 * rows * width * (2 * width + total_rows), bytes_accessed=16 * width * width, transcendentals=0),
        name="backward",
    )(act_2, grad_z, w_out, normed_2, act_1, w_mid, normed_1, feat, vecs)


def solution(mesh):
    shards = mesh.shape[DATA_AXIS]
    row_part = P(DATA_AXIS, None)
    replicated = P()

    def local_step(feat_a, feat_b, w_in, w_mid, w_out, t_in, t_mid, t_out, gain_1, bias_1, gain_2, bias_2, off_weight):
        row_count = feat_a.shape[0] * shards

        affine = jnp.stack([gain_1, bias_1, gain_2, bias_2])
        act_1, act_2, normed_1, normed_2, zh_a, emb_a, emb_b, inv_std = forward_pass(feat_a, feat_b, w_in, t_in, w_mid, t_mid, w_out, t_out, affine, shards, row_count)
        width = w_mid.shape[0]
        inv_1, inv_2 = inv_std[:2, : width // COLS].reshape(2, width)
        grad_emb, grad_z, loss_sums = corr_grad(emb_a, emb_b, zh_a, inv_std, off_weight, shards, row_count)
        loss_value = jnp.sum(loss_sums)
        pad = jnp.zeros((5,) + gain_1.shape, jnp.float32)
        vecs = jnp.stack([jnp.concatenate([jnp.stack([gain_2, bias_2, inv_2]), pad]), jnp.concatenate([jnp.stack([gain_1, bias_1, inv_1]), pad])])
        sums, stats = backward(act_2, grad_z, w_out, normed_2, act_1, w_mid, normed_1, feat_a, vecs, shards, row_count)
        return (loss_value, grad_emb, sums[2 * width :], sums[width : 2 * width], sums[:width], stats[1, 0], stats[1, 1], stats[0, 0], stats[0, 1])

    return jax.shard_map(local_step, mesh=mesh, in_specs=(row_part, row_part) + (replicated,) * 11, out_specs=(replicated, row_part) + (replicated,) * 7, check_vma=False)
```

```python
import functools

import jax
import jax.numpy as jnp
from jax import lax
from jax.experimental import pallas as pl
from jax.experimental.pallas import tpu as pltpu
from jax.sharding import PartitionSpec as P

NORM_EPS = 1e-5
DATA_AXIS = "data"
MESH_ID = pl.DeviceIdType.MESH
UNIT = 128
VMEM_LIMIT = 66_000_000


def contract_rows(left_op, right_op):
    return lax.dot_general(left_op, right_op, (((0,), (0,)), ((), ())), preferred_element_type=jnp.float32)


def contract_cols(left_op, right_op):
    return lax.dot_general(left_op, right_op, (((1,), (1,)), ((), ())), preferred_element_type=jnp.float32)


def flip(me, mask):
    bit = lax.rem(lax.div(me, mask), 2)
    return me + mask * (1 - 2 * bit), bit


class SumExchange:
    def __init__(self, me, shards, slots, send_sems, recv_sems):
        self.me, self.shards, self.slots, self.send_sems, self.recv_sems = me, shards, slots, send_sems, recv_sems

    def copy(self, index, peer, slot):
        return pltpu.make_async_remote_copy(src_ref=self.slots.at[index, self.me], dst_ref=self.slots.at[index, slot], send_sem=self.send_sems.at[index, peer], recv_sem=self.recv_sems.at[index, slot], device_id=(peer,), device_id_type=MESH_ID)

    def peers(self):
        return [lax.rem(self.me + shift, self.shards) for shift in range(1, self.shards)]

    def start(self, index):
        for peer in self.peers():
            self.copy(index, peer, self.me).start()

    def finish(self, index):
        for peer in self.peers():
            self.copy(index, peer, peer).wait_recv()
            self.copy(index, peer, self.me).wait_send()
        summed = self.slots[index, 0]
        for slot in range(1, self.shards):
            summed = summed + self.slots[index, slot]
        return summed


def enter_all(me, shards):
    barrier = pltpu.get_barrier_semaphore()
    for shift in range(1, shards):
        pl.semaphore_signal(barrier, inc=1, device_id=(lax.rem(me + shift, shards),), device_id_type=MESH_ID)
    pl.semaphore_wait(barrier, shards - 1)


COLS = 512
ROWS = 1024


def forward_kernel(shards, row_count, feat_a, feat_b, w_in, t_in, w_mid, t_mid, w_out, t_out, gain_1, bias_1, gain_2, bias_2, act_1, act_2, normed_1, normed_2, normed_z, emb_a, emb_b, inv_ref, pre, act, feat, weight_in, weight, slots, sums, send_sems, recv_sems, load_sems, store_sems):
    me = lax.axis_index(DATA_AXIS)
    rows, width = act_1.shape
    groups = width // COLS
    copies = [pltpu.make_async_copy(src, dst, load_sems.at[index]) for index, (src, dst) in enumerate([(feat_a, feat.at[0]), (w_in, weight_in.at[0]), (feat_b, feat.at[1]), (t_in, weight_in.at[1]), (w_mid, weight.at[0]), (t_mid, weight.at[1]), (w_out, weight.at[0]), (t_out, weight.at[1])])]
    for index in range(6):
        copies[index].start()
    enter_all(me, shards)
    ex = SumExchange(me, shards, slots, send_sems, recv_sems)

    def product(index, source, matrix, target):
        def group(number, carry):
            cols = pl.ds(pl.multiple_of(number * COLS, COLS), COLS)
            total = jnp.zeros((1, COLS), jnp.float32)
            squares = jnp.zeros((1, COLS), jnp.float32)
            for chunk in range(rows // ROWS):
                part = pl.ds(chunk * ROWS, ROWS)
                out = jnp.dot(source[part], matrix[:, cols], preferred_element_type=jnp.float32)
                target[part, cols] = out
                total = total + jnp.sum(out, axis=0, keepdims=True)
                squares = squares + jnp.sum(out * out, axis=0, keepdims=True)
            slots[index, me, pl.ds(number, 1)] = total
            slots[index, me, pl.ds(number + groups, 1)] = squares
            return carry

        lax.fori_loop(0, groups, group, 0)
        ex.start(index)

    def normalise(index, source, target, layer, keep):
        summed = ex.finish(index) / row_count
        mean = summed[:groups]
        inv = lax.rsqrt(summed[groups:] - mean * mean + NORM_EPS)
        sums[index, :groups] = mean
        sums[index, groups:] = inv
        if keep is not None:
            inv_ref[layer, :groups] = inv

        def group(number, carry):
            cols = pl.ds(pl.multiple_of(number * COLS, COLS), COLS)
            col_mean = sums[index, pl.ds(number, 1)]
            col_inv = sums[index, pl.ds(number + groups, 1)]
            for chunk in range(rows // ROWS):
                part = pl.ds(chunk * ROWS, ROWS)
                out = (source[part, cols] - col_mean) * col_inv
                if keep is not None:
                    source[part, cols] = out
                if layer < 2:
                    gain, bias = ((gain_1, bias_1), (gain_2, bias_2))[layer]
                    out = jnp.maximum(out * gain[:, cols] + bias[:, cols], 0.0)
                target[part, cols] = out.astype(jnp.bfloat16)
            return carry

        lax.fori_loop(0, groups, group, 0)

    def store(number, src, dst):
        copy = pltpu.make_async_copy(src, dst, store_sems.at[number])
        copy.start()
        return copy

    copies[0].wait()
    copies[1].wait()
    product(0, feat.at[0], weight_in.at[0], pre.at[0])
    copies[2].wait()
    copies[3].wait()
    product(1, feat.at[1], weight_in.at[1], pre.at[1])
    normalise(0, pre.at[0], act.at[0], 0, normed_1)
    out_n1 = store(0, pre.at[0], normed_1)
    out_x1 = store(1, act.at[0], act_1)
    copies[4].wait()
    product(2, act.at[0], weight.at[0], pre.at[2])
    copies[6].start()
    normalise(1, pre.at[1], act.at[1], 0, None)
    copies[5].wait()
    out_n1.wait()
    product(3, act.at[1], weight.at[1], pre.at[0])
    copies[7].start()
    out_x1.wait()
    normalise(2, pre.at[2], act.at[0], 1, normed_2)
    out_n2 = store(2, pre.at[2], normed_2)
    out_x2 = store(3, act.at[0], act_2)
    copies[6].wait()
    product(4, act.at[0], weight.at[0], pre.at[1])
    normalise(3, pre.at[0], act.at[1], 1, None)
    copies[7].wait()
    out_n2.wait()
    product(5, act.at[1], weight.at[1], pre.at[2])
    out_x2.wait()
    normalise(4, pre.at[1], act.at[0], 2, normed_z)
    out_z = store(4, pre.at[1], normed_z)
    out_a = store(5, act.at[0], emb_a)
    normalise(5, pre.at[2], act.at[1], 2, None)
    out_b = store(6, act.at[1], emb_b)
    for copy in (out_z, out_a, out_b):
        copy.wait()


def forward_pass(feat_a, feat_b, w_in, t_in, w_mid, t_mid, w_out, t_out, vectors, shards, row_count):
    rows, feat_dim = feat_a.shape
    width = w_mid.shape[0]
    groups = width // COLS
    vmem = pl.BlockSpec(memory_space=pltpu.VMEM)
    hbm = pl.BlockSpec(memory_space=pl.ANY)
    half_out = jax.ShapeDtypeStruct((rows, width), jnp.bfloat16)
    full_out = jax.ShapeDtypeStruct((rows, width), jnp.float32)
    return pl.pallas_call(
        functools.partial(forward_kernel, shards, row_count),
        out_shape=(half_out, half_out, full_out, full_out, full_out, half_out, half_out, jax.ShapeDtypeStruct((3, 8, COLS), jnp.float32)),
        in_specs=[hbm] * 8 + [vmem] * 4,
        out_specs=(hbm,) * 7 + (vmem,),
        scratch_shapes=[
            pltpu.VMEM((3, rows, width), jnp.float32),
            pltpu.VMEM((2, rows, width), jnp.bfloat16),
            pltpu.VMEM((2, rows, feat_dim), jnp.bfloat16),
            pltpu.VMEM((2, feat_dim, width), jnp.bfloat16),
            pltpu.VMEM((2, width, width), jnp.bfloat16),
            pltpu.VMEM((6, shards, 2 * groups, COLS), jnp.float32),
            pltpu.VMEM((6, 2 * groups, COLS), jnp.float32),
            pltpu.SemaphoreType.DMA((6, shards)),
            pltpu.SemaphoreType.DMA((6, shards)),
            pltpu.SemaphoreType.DMA((8,)),
            pltpu.SemaphoreType.DMA((7,)),
        ],
        compiler_params=pltpu.CompilerParams(collective_id=4, has_side_effects=True, vmem_limit_bytes=VMEM_LIMIT),
        cost_estimate=pl.CostEstimate(flops=4 * rows * width * (2 * width + feat_dim), bytes_accessed=24 * width * width, transcendentals=0),
        name="forward",
    )(feat_a, feat_b, w_in, t_in, w_mid, t_mid, w_out, t_out, *vectors)


PAIR, RS1, RS2, RS3, AG3, AG2, AG1, AGP, LOCAL = range(9)


class Exchange:
    def __init__(self, me, ring, halves, gathered, recv_pair, recv_1, recv_2, recv_3, total, send_sems, recv_sems, row_of, depth, send_total=False):
        self.depth, self.send_total = depth, send_total
        self.me, self.ring, self.halves, self.gathered = me, ring, halves, gathered
        self.recv_pair, self.recv_1, self.recv_2, self.recv_3, self.total = recv_pair, recv_1, recv_2, recv_3, total
        self.send_sems, self.recv_sems, self.row_of = send_sems, recv_sems, row_of

    def axes(self, unit):
        def mask(shift):
            axis = lax.rem(unit + shift, 3)
            return 2 + axis + axis * axis

        (p1, b1), (p2, b2), (p3, b3) = (flip(self.me, mask(shift)) for shift in range(3))
        return (p1, p2, p3), (b1, b2, b3)

    def copy(self, unit, kind):
        (p1, p2, p3), (b1, b2, b3) = self.axes(unit)
        partner, half = flip(self.me, 1)

        def rows(start, size):
            return pl.ds(pl.multiple_of(start, 16), size)

        slot = lax.rem(unit, self.depth)
        total = self.total.at[slot]
        row = self.row_of(unit, half)
        if kind == PAIR:
            src, dst, peer = self.halves.at[lax.rem(unit, self.ring)], self.recv_pair.at[slot], partner
        elif kind == RS1:
            src, dst, peer = total.at[rows((1 - b1) * 64, 64)], self.recv_1.at[lax.rem(unit, self.recv_1.shape[0])], p1
        elif kind == RS2:
            src, dst, peer = total.at[rows(b1 * 64 + (1 - b2) * 32, 32)], self.recv_2.at[lax.rem(unit, self.recv_2.shape[0])], p2
        elif kind == RS3:
            src, dst, peer = total.at[rows(b1 * 64 + b2 * 32 + (1 - b3) * 16, 16)], self.recv_3.at[lax.rem(unit, self.recv_3.shape[0])], p3
        else:
            start, size, peer = {
                AG3: (b1 * 64 + b2 * 32 + b3 * 16, 16, p3),
                AG2: (b1 * 64 + b2 * 32, 32, p2),
                AG1: (b1 * 64, 64, p1),
                AGP: (0, 128, partner),
            }[kind]
            src = dst = self.gathered.at[rows(row + start, size)]
            if kind == AG3 and self.send_total:
                src = total.at[rows(start, size)]
        return pltpu.make_async_remote_copy(src_ref=src, dst_ref=dst, send_sem=self.send_sems.at[slot, kind], recv_sem=self.recv_sems.at[slot, kind], device_id=(peer,), device_id_type=MESH_ID)

    def reduce_step(self, unit, kind):
        _, (b1, b2, b3) = self.axes(unit)
        self.copy(unit, kind).wait()
        if kind == PAIR:
            start, size, landed = 0, 128, self.recv_pair
        elif kind == RS1:
            start, size, landed = b1 * 64, 64, self.recv_1
        else:
            start, size, landed = b1 * 64 + b2 * 32, 32, self.recv_2
        keep = pl.ds(pl.multiple_of(start, 16), size)
        slot = lax.rem(unit, self.depth)
        self.total[slot, keep] = self.total[slot, keep] + landed[lax.rem(unit, landed.shape[0])]
        self.copy(unit, kind + 1).start()

    def owned(self, unit):
        _, (b1, b2, b3) = self.axes(unit)
        return b1 * 64 + b2 * 32 + b3 * 16


def enter(me):
    barrier = pltpu.get_barrier_semaphore()
    for mask in (1, 2, 4, 8):
        pl.semaphore_signal(barrier, inc=1, device_id=(flip(me, mask)[0],), device_id_type=MESH_ID)
    pl.semaphore_wait(barrier, 4)


def pipeline(units, lags, stages):
    def step(now, carry):
        for lag, stage in reversed(list(zip(lags, stages))):
            unit = now - lag

            @pl.when((unit >= 0) & (unit < units))
            def _(unit=unit, stage=stage):
                stage(unit)

        return carry

    lax.fori_loop(0, units + max(lags), step, 0)


def product_unit(left_ref, right_ref, col_other, col_mine, halves, total, slot, unit, blocks):
    left = jnp.concatenate([left_ref[:, pl.ds(pl.multiple_of(col_other, UNIT), UNIT)], left_ref[:, pl.ds(pl.multiple_of(col_mine, UNIT), UNIT)]], axis=1)
    width = right_ref.shape[1] // blocks
    for block in range(blocks):
        cols = pl.ds(block * width, width)
        out = contract_rows(left, right_ref[:, cols])
        halves[slot, :, cols] = out[:UNIT]
        total[unit, :, cols] = out[UNIT:]


RING = 3
CORR_LAGS = (0, 1, 4, 6, 9, 12, 15, 18, 20)


def corr_kernel(shards, row_count, off_ref, inv_ref, left_ref, right_ref, normed, emb_out, back_out, loss_ref, grad_ref, emb_grad, back, norm_in, loss_acc, wide, slots, halves, recv_pair, recv_1, recv_2, recv_3, total, send_sems, recv_sems, sum_send, sum_recv, norm_sems, store_sems):
    me = lax.axis_index(DATA_AXIS)
    rows, width = right_ref.shape
    half_rows = width // 2
    units = half_rows // UNIT
    groups = width // COLS
    _, half = flip(me, 1)
    enter_all(me, shards)
    ex = Exchange(me, RING, halves, grad_ref, recv_pair, recv_1, recv_2, recv_3, total, send_sems, recv_sems, lambda unit, h: h * half_rows + unit * UNIT, units)
    sums = SumExchange(me, shards, slots, sum_send, sum_recv)
    loss_acc[...] = jnp.zeros_like(loss_acc)

    def produce(unit):
        @pl.when(unit >= RING)
        def _():
            ex.copy(unit - RING, PAIR).wait_send()

        product_unit(left_ref, right_ref, (1 - half) * half_rows + unit * UNIT, half * half_rows + unit * UNIT, halves, total, lax.rem(unit, RING), unit, 4)
        ex.copy(unit, PAIR).start()

    def pair_step(unit):
        ex.copy(unit, PAIR).wait_recv()
        total[unit] = total[unit] + recv_pair[unit]
        ex.copy(unit, RS1).start()

    def finish(unit):
        ex.copy(unit, RS3).wait()
        start = ex.owned(unit)
        keep = pl.ds(pl.multiple_of(start, 16), 16)
        corr = (total[unit, keep] + recv_3[unit]) * (1.0 / row_count)
        row = half * half_rows + unit * UNIT + start
        on_diag = lax.broadcasted_iota(jnp.int32, (16, width), 0) + row == lax.broadcasted_iota(jnp.int32, (16, width), 1)
        off_weight = off_ref[0, 0]
        miss = 1.0 - corr
        terms = jnp.where(on_diag, miss * miss, off_weight * (corr * corr))
        loss_acc[...] += terms[:8] + terms[8:]
        grad = jnp.where(on_diag, -2.0 * miss, 2.0 * off_weight * corr).astype(jnp.bfloat16)
        grad_ref[pl.ds(pl.multiple_of(row, 16), 16)] = grad
        ex.copy(unit, AG3).start()

    def forward(kind):
        def stage(unit):
            ex.copy(unit, kind).wait()
            if kind != AGP:
                ex.copy(unit, kind + 1).start()

            if kind == AG1:
                for side in range(2):
                    load_norm(row_of(unit, side), lax.rem(unit, 2), side).start()

        return stage

    def row_of(unit, side):
        return (half + side * (1 - 2 * half)) * half_rows + unit * UNIT

    def lanes(start):
        return pl.ds(pl.multiple_of(start, UNIT), UNIT)

    def load_norm(start, slot, side):
        return pltpu.make_async_copy(normed.at[:, lanes(start)], norm_in.at[slot, side], norm_sems.at[slot, side])

    def embed(unit):
        ex.copy(unit, AGP).wait()
        slot = lax.rem(unit, 2)
        starts = [row_of(unit, side) for side in range(2)]
        rhs = jnp.concatenate([grad_ref[lanes(start)] for start in starts], axis=0)
        for side in range(2):
            load_norm(starts[side], slot, side).wait()
        plain = [jnp.zeros((1, UNIT), jnp.float32)] * 2
        crossed = [jnp.zeros((1, UNIT), jnp.float32)] * 2
        for chunk in range(rows // ROWS):
            part = pl.ds(chunk * ROWS, ROWS)
            out = contract_cols(right_ref[part], rhs) * (1.0 / row_count)
            for side in range(2):
                piece = out[:, side * UNIT : (side + 1) * UNIT]
                emb_grad[part, lanes(starts[side])] = piece
                plain[side] = plain[side] + jnp.sum(piece, axis=0, keepdims=True)
                crossed[side] = crossed[side] + jnp.sum(piece * norm_in[slot, side, part], axis=0, keepdims=True)
        for side in range(2):
            wide[0:1, lanes(starts[side])] = plain[side]
            wide[1:2, lanes(starts[side])] = crossed[side]

    pipeline(units, CORR_LAGS, [produce, pair_step, lambda u: ex.reduce_step(u, RS1), lambda u: ex.reduce_step(u, RS2), finish, forward(AG3), forward(AG2), forward(AG1), embed])
    for unit in range(units - RING, units):
        ex.copy(unit, PAIR).wait_send()
    folded = loss_acc[:, :UNIT]
    for index in range(1, width // UNIT):
        folded = folded + loss_acc[:, index * UNIT : (index + 1) * UNIT]
    slots[0, me, :, COLS:] = folded
    for index in range(groups):
        cols = pl.ds(index * COLS, COLS)
        slots[0, me, index : index + 1, :COLS] = wide[0:1, cols]
        slots[0, me, groups + index : groups + index + 1, :COLS] = wide[1:2, cols]
    sums.start(0)
    store_emb = pltpu.make_async_copy(emb_grad, emb_out, store_sems.at[0])
    store_emb.start()

    def load_block(index, slot):
        return [load_norm((2 * index + side) * UNIT, slot, side) for side in range(2)]

    for copy in load_block(0, 0) + load_block(1, 1):
        copy.start()
    summed = sums.finish(0)
    loss_ref[0, 0] = jnp.sum(summed[:, COLS:])
    means = summed[:, :COLS] / row_count
    for index in range(groups):
        cols = pl.ds(index * COLS, COLS)
        wide[0:1, cols] = means[index : index + 1]
        wide[1:2, cols] = means[groups + index : groups + index + 1]
        wide[2:3, cols] = inv_ref[2, index : index + 1]

    def norm_back(index, carry):
        slot = lax.rem(index, 2)
        for side, copy in enumerate(load_block(index, slot)):
            copy.wait()
            start = (2 * index + side) * UNIT
            mean_g, mean_gn, inv = wide[0:1, lanes(start)], wide[1:2, lanes(start)], wide[2:3, lanes(start)]
            for chunk in range(rows // ROWS):
                part = pl.ds(chunk * ROWS, ROWS)
                back[part, lanes(start)] = ((emb_grad[part, lanes(start)] - mean_g - norm_in[slot, side, part] * mean_gn) * inv).astype(jnp.bfloat16)

        @pl.when(index + 2 < width // (2 * UNIT))
        def _():
            for copy in load_block(index + 2, slot):
                copy.start()

        return carry

    lax.fori_loop(0, width // (2 * UNIT), norm_back, 0)
    store_back = pltpu.make_async_copy(back, back_out, store_sems.at[1])
    store_back.start()
    store_emb.wait()
    store_back.wait()


def exchange_scratch(units, width):
    return [
        pltpu.VMEM((RING, UNIT, width), jnp.float32),
        pltpu.VMEM((units, UNIT, width), jnp.float32),
        pltpu.VMEM((units, 64, width), jnp.float32),
        pltpu.VMEM((units, 32, width), jnp.float32),
        pltpu.VMEM((units, 16, width), jnp.float32),
        pltpu.VMEM((units, UNIT, width), jnp.float32),
        pltpu.SemaphoreType.DMA((units, 9)),
        pltpu.SemaphoreType.DMA((units, 9)),
    ]


def corr_grad(emb_a, emb_b, normed, inv_std, off_weight, shards, row_count):
    rows, width = emb_a.shape
    vmem = pl.BlockSpec(memory_space=pltpu.VMEM)
    hbm = pl.BlockSpec(memory_space=pl.ANY)
    return pl.pallas_call(
        functools.partial(corr_kernel, shards, row_count),
        out_shape=(jax.ShapeDtypeStruct((rows, width), jnp.float32), jax.ShapeDtypeStruct((rows, width), jnp.bfloat16), jax.ShapeDtypeStruct((1, 1), jnp.float32)),
        in_specs=[pl.BlockSpec(memory_space=pltpu.SMEM), vmem, vmem, vmem, hbm],
        out_specs=(hbm, hbm, pl.BlockSpec(memory_space=pltpu.SMEM)),
        scratch_shapes=[
            pltpu.VMEM((width, width), jnp.bfloat16),
            pltpu.VMEM((rows, width), jnp.float32),
            pltpu.VMEM((rows, width), jnp.bfloat16),
            pltpu.VMEM((2, 2, rows, UNIT), jnp.float32),
            pltpu.VMEM((8, width), jnp.float32),
            pltpu.VMEM((8, width), jnp.float32),
            pltpu.VMEM((1, shards, 8, COLS + UNIT), jnp.float32),
        ]
        + exchange_scratch(width // 2 // UNIT, width)
        + [pltpu.SemaphoreType.DMA((1, shards)), pltpu.SemaphoreType.DMA((1, shards)), pltpu.SemaphoreType.DMA((2, 2)), pltpu.SemaphoreType.DMA((2,))],
        compiler_params=pltpu.CompilerParams(collective_id=2, has_side_effects=True, vmem_limit_bytes=VMEM_LIMIT),
        cost_estimate=pl.CostEstimate(flops=4 * rows * width * width, bytes_accessed=8 * width * width, transcendentals=0),
        name="corr_grad",
    )(off_weight.reshape(1, 1), inv_std, emb_a, emb_b, normed)


DEPTH = 18
DEPTH_1, DEPTH_2, DEPTH_3 = 15, 9, 6
CHAIN = 6
PER_TICK = 2
BLOCK = 256
NORM_SLOTS = 3
WEIGHT_SLOTS = 3
BACK_LAGS = (1, 4, 6, 7, 9, 12, 16, 18)


def backward_kernel(shards, row_count, left_2, grad_z, w_out, normed_2, left_1, w_mid, normed_1, feat, gain_1, bias_1, gain_2, bias_2, inv_ref, out_ref, stat_ref, vecs, left, feat_in, grad, weight, normed, deriv, halves, mine, total, recv_1, recv_2, recv_3, wide, slots, send_sems, recv_sems, load_sems, weight_sems, normed_sems, sum_send, sum_recv):
    me = lax.axis_index(DATA_AXIS)
    _, half = flip(me, 1)
    rows, width = left.shape
    groups = width // COLS
    blocks = width // BLOCK
    units_full = width // 2 // UNIT
    units_last = feat_in.shape[1] // 2 // UNIT
    units = 2 * units_full + units_last
    ticks = units + max(BACK_LAGS)

    load_left = pltpu.make_async_copy(left_2, left, load_sems.at[0])
    load_grad = pltpu.make_async_copy(grad_z, grad.at[0], load_sems.at[1])
    load_feat = pltpu.make_async_copy(feat, feat_in, load_sems.at[2])

    def block_of(index):
        return pl.ds(pl.multiple_of(index * BLOCK, BLOCK), BLOCK)

    def weight_copy(source, number):
        slot = lax.rem(number, WEIGHT_SLOTS)
        return pltpu.make_async_copy(source.at[block_of(lax.rem(number, blocks))], weight.at[slot], weight_sems.at[slot])

    def weight_start(number):
        @pl.when(number < blocks)
        def _():
            weight_copy(w_out, number).start()

        @pl.when((number >= blocks) & (number < 2 * blocks))
        def _():
            weight_copy(w_mid, number).start()

    def normed_copy(source, number):
        slot = lax.rem(number, NORM_SLOTS)
        return pltpu.make_async_copy(source.at[:, block_of(lax.rem(number, blocks))], normed.at[slot], normed_sems.at[slot])

    def normed_start(number):
        @pl.when(number < 2 * blocks)
        def _():
            normed_copy(normed_2, number).start()

        @pl.when((number >= 2 * blocks) & (number < 4 * blocks))
        def _():
            normed_copy(normed_1, number).start()

    load_left.start()
    load_grad.start()
    for number in range(WEIGHT_SLOTS):
        weight_copy(w_out, number).start()
    for number in range(NORM_SLOTS):
        normed_copy(normed_2, number).start()
    load_feat.start()
    for layer, (gain, bias) in enumerate(((gain_2, bias_2), (gain_1, bias_1))):
        vecs[layer, 0:1] = gain[...]
        vecs[layer, 1:2] = bias[...]
        for index in range(groups):
            vecs[layer, 2:3, index * COLS : (index + 1) * COLS] = inv_ref[1 - layer, index : index + 1]
    enter_all(me, shards)

    def row_of(unit, h):
        layer = lax.div(unit, units_full)
        part = width // 2 - (width // 2 - feat_in.shape[1] // 2) * lax.div(layer, 2)
        return layer * width + h * part + lax.rem(unit, units_full) * UNIT

    ex = Exchange(me, 2, halves, out_ref, total, recv_1, recv_2, recv_3, total, send_sems, recv_sems, row_of, DEPTH, send_total=True)
    sums = SumExchange(me, shards, slots, sum_send, sum_recv)

    def produce(unit, source, part):
        @pl.when(unit >= 2)
        def _():
            ex.copy(unit - 2, PAIR).wait_send()

        which = lax.rem(lax.div(unit, units_full), 2)
        local = lax.rem(unit, units_full) * UNIT
        ring = lax.rem(unit, 2)
        col_other, col_mine = (1 - half) * part + local, half * part + local
        lhs = jnp.concatenate([source[:, pl.ds(pl.multiple_of(col_other, UNIT), UNIT)], source[:, pl.ds(pl.multiple_of(col_mine, UNIT), UNIT)]], axis=1)
        chunk = width // 4
        for index in range(4):
            cols = pl.ds(index * chunk, chunk)
            prod = contract_rows(lhs, grad[which, :, cols])
            halves[ring, :, cols] = prod[:UNIT]
            mine[ring, :, cols] = prod[UNIT:]
        ex.copy(unit, PAIR).start()

    def pair_step(unit):
        slot = lax.rem(unit, DEPTH)
        ex.copy(unit, PAIR).wait_recv()
        total[slot] = total[slot] + mine[lax.rem(unit, 2)]
        ex.copy(unit, RS1).start()

    def to_out(unit):
        start = ex.owned(unit)
        slot = lax.rem(unit, DEPTH)
        return pltpu.make_async_copy(total.at[slot, pl.ds(pl.multiple_of(start, 16), 16)], out_ref.at[pl.ds(pl.multiple_of(row_of(unit, half) + start, 16), 16)], send_sems.at[slot, LOCAL])

    def finish(unit):
        ex.copy(unit, RS3).wait()
        slot = lax.rem(unit, DEPTH)
        keep = pl.ds(pl.multiple_of(ex.owned(unit), 16), 16)
        total[slot, keep] = total[slot, keep] + recv_3[lax.rem(unit, DEPTH_3)]
        to_out(unit).start()
        ex.copy(unit, AG3).start()

    def forward(kind):
        def stage(unit):
            if kind == AG3:
                to_out(unit).wait()
            ex.copy(unit, kind).wait()
            if kind != AGP:
                ex.copy(unit, kind + 1).start()

        return stage

    stages = [pair_step, lambda u: ex.reduce_step(u, RS1), lambda u: ex.reduce_step(u, RS2), finish, forward(AG3), forward(AG2), forward(AG1), forward(AGP)]

    def derivative(layer, index):
        number = layer * blocks + index
        stream = 2 * layer * blocks + index
        weight_copy(w_out, number).wait()
        normed_copy(normed_2, stream).wait()
        slot, weight_slot = lax.rem(stream, NORM_SLOTS), lax.rem(number, WEIGHT_SLOTS)
        cols = block_of(index)
        gain, bias = vecs[layer, 0:1, cols], vecs[layer, 1:2, cols]
        rhs = weight[weight_slot]
        sum_n = jnp.zeros((1, BLOCK), jnp.float32)
        sum_d = jnp.zeros((1, BLOCK), jnp.float32)
        for chunk in range(rows // BLOCK):
            part = pl.ds(chunk * BLOCK, BLOCK)
            n = normed[slot, part]
            d = jnp.where(n * gain + bias > 0.0, contract_cols(grad[layer, part], rhs), 0.0)
            deriv[part, cols] = d
            sum_n = sum_n + jnp.sum(d * n, axis=0, keepdims=True)
            sum_d = sum_d + jnp.sum(d, axis=0, keepdims=True)
        wide[0:1, cols] = sum_n
        wide[1:2, cols] = sum_d
        weight_start(number + WEIGHT_SLOTS)
        normed_start(stream + NORM_SLOTS)

    def send_sums(layer):
        for index in range(groups):
            cols = pl.ds(index * COLS, COLS)
            slots[layer, me, index : index + 1] = wide[0:1, cols]
            slots[layer, me, groups + index : groups + index + 1] = wide[1:2, cols]
        sums.start(layer)

    def next_grad(layer):
        summed = sums.finish(layer)
        for index in range(groups):
            cols = pl.ds(index * COLS, COLS)
            for row in range(2):
                line = summed[row * groups + index : row * groups + index + 1]
                stat_ref[layer, row : row + 1, cols] = line
                wide[2 + row : 3 + row, cols] = line / row_count

        def one(index, carry):
            stream = (2 * layer + 1) * blocks + index
            normed_copy(normed_2, stream).wait()
            slot = lax.rem(stream, NORM_SLOTS)
            cols = block_of(index)
            mean_n, mean_d = wide[2:3, cols], wide[3:4, cols]
            scale = vecs[layer, 0:1, cols] * vecs[layer, 2:3, cols]
            for chunk in range(rows // BLOCK):
                part = pl.ds(chunk * BLOCK, BLOCK)
                grad[1 - layer, part, cols] = ((deriv[part, cols] - mean_d - normed[slot, part] * mean_n) * scale).astype(jnp.bfloat16)
            normed_start(stream + NORM_SLOTS)
            return carry

        lax.fori_loop(0, blocks, one, 0)

    def tick(now, carry):
        for lag, stage in reversed(list(zip(BACK_LAGS, stages))):
            unit = now - lag

            @pl.when((unit >= 0) & (unit < units))
            def _(stage=stage, unit=unit):
                stage(unit)

        @pl.when(now < 2 * units_full)
        def _():
            @pl.when(lax.rem(now, units_full) == 0)
            def _():
                load_left.wait()

                @pl.when(now == 0)
                def _():
                    load_grad.wait()

            produce(now, left, width // 2)

            @pl.when(now == units_full - 1)
            def _():
                pltpu.make_async_copy(left_1, left, load_sems.at[0]).start()

        @pl.when((now >= 2 * units_full) & (now < units))
        def _():
            @pl.when(now == 2 * units_full)
            def _():
                load_feat.wait()

            produce(now, feat_in, feat_in.shape[1] // 2)

        layer, place = lax.div(now, CHAIN), lax.rem(now, CHAIN)
        steps = blocks // PER_TICK

        @pl.when((layer < 2) & (place < steps))
        def _():
            def one(index, carry):
                derivative(layer, place * PER_TICK + index)
                return carry

            lax.fori_loop(0, PER_TICK, one, 0)

            @pl.when(place == steps - 1)
            def _():
                send_sums(layer)

        @pl.when((layer < 2) & (place == CHAIN - 1))
        def _():
            next_grad(layer)

        return carry

    lax.fori_loop(0, ticks, tick, 0)
    for unit in (units - 2, units - 1):
        ex.copy(unit, PAIR).wait_send()


def backward(act_2, grad_z, w_out, normed_2, act_1, w_mid, normed_1, feat, vectors, inv_std, shards, row_count):
    rows, width = act_2.shape
    feat_dim = feat.shape[1]
    total_rows = 2 * width + feat_dim
    vmem = pl.BlockSpec(memory_space=pltpu.VMEM)
    hbm = pl.BlockSpec(memory_space=pl.ANY)
    return pl.pallas_call(
        functools.partial(backward_kernel, shards, row_count),
        out_shape=(jax.ShapeDtypeStruct((total_rows, width), jnp.float32), jax.ShapeDtypeStruct((2, 2, width), jnp.float32)),
        in_specs=[hbm] * 8 + [vmem] * 5,
        out_specs=(hbm, vmem),
        scratch_shapes=[
            pltpu.VMEM((2, 8, width), jnp.float32),
            pltpu.VMEM((rows, width), jnp.bfloat16),
            pltpu.VMEM((rows, feat_dim), jnp.bfloat16),
            pltpu.VMEM((2, rows, width), jnp.bfloat16),
            pltpu.VMEM((WEIGHT_SLOTS, BLOCK, width), jnp.bfloat16),
            pltpu.VMEM((NORM_SLOTS, rows, BLOCK), jnp.float32),
            pltpu.VMEM((rows, width), jnp.float32),
            pltpu.VMEM((2, UNIT, width), jnp.float32),
            pltpu.VMEM((2, UNIT, width), jnp.float32),
            pltpu.VMEM((DEPTH, UNIT, width), jnp.float32),
            pltpu.VMEM((DEPTH_1, 64, width), jnp.float32),
            pltpu.VMEM((DEPTH_2, 32, width), jnp.float32),
            pltpu.VMEM((DEPTH_3, 16, width), jnp.float32),
            pltpu.VMEM((8, width), jnp.float32),
            pltpu.VMEM((2, shards, 8, COLS), jnp.float32),
            pltpu.SemaphoreType.DMA((DEPTH, 9)),
            pltpu.SemaphoreType.DMA((DEPTH, 9)),
            pltpu.SemaphoreType.DMA((3,)),
            pltpu.SemaphoreType.DMA((WEIGHT_SLOTS,)),
            pltpu.SemaphoreType.DMA((NORM_SLOTS,)),
            pltpu.SemaphoreType.DMA((2, shards)),
            pltpu.SemaphoreType.DMA((2, shards)),
        ],
        compiler_params=pltpu.CompilerParams(collective_id=3, has_side_effects=True, vmem_limit_bytes=VMEM_LIMIT),
        cost_estimate=pl.CostEstimate(flops=2 * rows * width * (2 * width + total_rows), bytes_accessed=16 * width * width, transcendentals=0),
        name="backward",
    )(act_2, grad_z, w_out, normed_2, act_1, w_mid, normed_1, feat, *vectors, inv_std)


CHUNK = 256
FLIGHT = 8


def output_kernel(sums_ref, emb_ref, stat_ref, emb_out, in_out, mid_out, last_out, gain_1, bias_1, gain_2, bias_2, buffer, read_sems, write_sems):
    width = mid_out.shape[0]
    reads, writes = [], []
    for source, first, target in ((sums_ref, 0, last_out), (sums_ref, width, mid_out), (sums_ref, 2 * width, in_out), (emb_ref, 0, emb_out)):
        for start in range(0, target.shape[0], CHUNK):
            slot = len(reads) % FLIGHT
            reads.append(pltpu.make_async_copy(source.at[pl.ds(first + start, CHUNK)], buffer.at[slot], read_sems.at[slot]))
            writes.append(pltpu.make_async_copy(buffer.at[slot], target.at[pl.ds(start, CHUNK)], write_sems.at[slot]))
    for copy in reads[:FLIGHT]:
        copy.start()
    gain_1[...] = stat_ref[1, 0:1]
    bias_1[...] = stat_ref[1, 1:2]
    gain_2[...] = stat_ref[0, 0:1]
    bias_2[...] = stat_ref[0, 1:2]
    behind = FLIGHT // 2
    for index in range(len(reads) + behind):
        if index < len(reads):
            reads[index].wait()
            writes[index].start()
        if index >= behind:
            writes[index - behind].wait()
            if index - behind + FLIGHT < len(reads):
                reads[index - behind + FLIGHT].start()


def to_outputs(sums, emb_grad, stats, width):
    feat_dim = sums.shape[0] - 2 * width
    vmem = pl.BlockSpec(memory_space=pltpu.VMEM)
    hbm = pl.BlockSpec(memory_space=pl.ANY)
    row = jax.ShapeDtypeStruct((1, width), jnp.float32)
    return pl.pallas_call(
        output_kernel,
        out_shape=(jax.ShapeDtypeStruct(emb_grad.shape, jnp.float32), jax.ShapeDtypeStruct((feat_dim, width), jnp.float32), jax.ShapeDtypeStruct((width, width), jnp.float32), jax.ShapeDtypeStruct((width, width), jnp.float32)) + (row,) * 4,
        in_specs=[hbm, hbm, vmem],
        out_specs=(hbm,) * 4 + (vmem,) * 4,
        scratch_shapes=[pltpu.VMEM((FLIGHT, CHUNK, width), jnp.float32), pltpu.SemaphoreType.DMA((FLIGHT,)), pltpu.SemaphoreType.DMA((FLIGHT,))],
        compiler_params=pltpu.CompilerParams(vmem_limit_bytes=VMEM_LIMIT),
        name="to_outputs",
    )(sums, emb_grad, stats)


def solution(mesh):
    shards = mesh.shape[DATA_AXIS]
    row_part = P(DATA_AXIS, None)
    replicated = P()

    def local_step(feat_a, feat_b, w_in, w_mid, w_out, t_in, t_mid, t_out, gain_1, bias_1, gain_2, bias_2, off_weight):
        row_count = feat_a.shape[0] * shards

        vectors = [vector.reshape(1, -1) for vector in (gain_1, bias_1, gain_2, bias_2)]
        act_1, act_2, normed_1, normed_2, zh_a, emb_a, emb_b, inv_std = forward_pass(feat_a, feat_b, w_in, t_in, w_mid, t_mid, w_out, t_out, vectors, shards, row_count)
        width = w_mid.shape[0]
        grad_emb, grad_z, loss_sums = corr_grad(emb_a, emb_b, zh_a, inv_std, off_weight, shards, row_count)
        loss_value = loss_sums[0, 0]
        sums, stats = backward(act_2, grad_z, w_out, normed_2, act_1, w_mid, normed_1, feat_a, vectors, inv_std, shards, row_count)
        grad_emb, grad_in, grad_mid, grad_out, *vector_grads = to_outputs(sums, grad_emb, stats, width)
        return (loss_value, grad_emb, grad_in, grad_mid, grad_out, *[vector.reshape(-1) for vector in vector_grads])

    return jax.shard_map(local_step, mesh=mesh, in_specs=(row_part, row_part) + (replicated,) * 11, out_specs=(replicated, row_part) + (replicated,) * 7, check_vma=False)
```

```python
import functools

import jax
import jax.numpy as jnp
from jax import lax
from jax.experimental import pallas as pl
from jax.experimental.pallas import tpu as pltpu
from jax.sharding import PartitionSpec as P

NORM_EPS = 1e-5
DATA_AXIS = "data"
MESH_ID = pl.DeviceIdType.MESH
UNIT = 128
VMEM_LIMIT = 66_000_000


def contract_rows(left_op, right_op):
    return lax.dot_general(left_op, right_op, (((0,), (0,)), ((), ())), preferred_element_type=jnp.float32)


def contract_cols(left_op, right_op):
    return lax.dot_general(left_op, right_op, (((1,), (1,)), ((), ())), preferred_element_type=jnp.float32)


def flip(me, mask):
    bit = lax.rem(lax.div(me, mask), 2)
    return me + mask * (1 - 2 * bit), bit


class SumExchange:
    def __init__(self, me, shards, slots, send_sems, recv_sems):
        self.me, self.shards, self.slots, self.send_sems, self.recv_sems = me, shards, slots, send_sems, recv_sems

    def copy(self, index, peer, slot):
        return pltpu.make_async_remote_copy(src_ref=self.slots.at[index, self.me], dst_ref=self.slots.at[index, slot], send_sem=self.send_sems.at[index, peer], recv_sem=self.recv_sems.at[index, slot], device_id=(peer,), device_id_type=MESH_ID)

    def peers(self):
        return [lax.rem(self.me + shift, self.shards) for shift in range(1, self.shards)]

    def start(self, index):
        for peer in self.peers():
            self.copy(index, peer, self.me).start()

    def finish(self, index):
        for peer in self.peers():
            self.copy(index, peer, peer).wait_recv()
            self.copy(index, peer, self.me).wait_send()
        summed = self.slots[index, 0]
        for slot in range(1, self.shards):
            summed = summed + self.slots[index, slot]
        return summed


def enter_all(me, shards):
    barrier = pltpu.get_barrier_semaphore()
    for shift in range(1, shards):
        pl.semaphore_signal(barrier, inc=1, device_id=(lax.rem(me + shift, shards),), device_id_type=MESH_ID)
    pl.semaphore_wait(barrier, shards - 1)


COLS = 512
ROWS = 1024


def forward_kernel(shards, row_count, feat_a, feat_b, w_in, t_in, w_mid, t_mid, w_out, t_out, gain_1, bias_1, gain_2, bias_2, act_1, act_2, normed_1, normed_2, normed_z, emb_a, emb_b, inv_ref, pre, act, feat, weight_in, weight, slots, sums, send_sems, recv_sems, load_sems, store_sems):
    me = lax.axis_index(DATA_AXIS)
    rows, width = act_1.shape
    groups = width // COLS
    copies = [pltpu.make_async_copy(src, dst, load_sems.at[index]) for index, (src, dst) in enumerate([(feat_a, feat.at[0]), (w_in, weight_in.at[0]), (feat_b, feat.at[1]), (t_in, weight_in.at[1]), (w_mid, weight.at[0]), (t_mid, weight.at[1]), (w_out, weight.at[0]), (t_out, weight.at[1])])]
    for index in range(6):
        copies[index].start()
    enter_all(me, shards)
    ex = SumExchange(me, shards, slots, send_sems, recv_sems)

    def product(index, source, matrix, target):
        def group(number, carry):
            cols = pl.ds(pl.multiple_of(number * COLS, COLS), COLS)
            total = jnp.zeros((1, COLS), jnp.float32)
            squares = jnp.zeros((1, COLS), jnp.float32)
            for chunk in range(rows // ROWS):
                part = pl.ds(chunk * ROWS, ROWS)
                out = jnp.dot(source[part], matrix[:, cols], preferred_element_type=jnp.float32)
                target[part, cols] = out
                total = total + jnp.sum(out, axis=0, keepdims=True)
                squares = squares + jnp.sum(out * out, axis=0, keepdims=True)
            slots[index, me, pl.ds(number, 1)] = total
            slots[index, me, pl.ds(number + groups, 1)] = squares
            return carry

        lax.fori_loop(0, groups, group, 0)
        ex.start(index)

    def normalise(index, source, target, layer, keep):
        summed = ex.finish(index) / row_count
        mean = summed[:groups]
        inv = lax.rsqrt(summed[groups:] - mean * mean + NORM_EPS)
        sums[index, :groups] = mean
        sums[index, groups:] = inv
        if keep is not None:
            inv_ref[layer, :groups] = inv

        def group(number, carry):
            cols = pl.ds(pl.multiple_of(number * COLS, COLS), COLS)
            col_mean = sums[index, pl.ds(number, 1)]
            col_inv = sums[index, pl.ds(number + groups, 1)]
            for chunk in range(rows // ROWS):
                part = pl.ds(chunk * ROWS, ROWS)
                out = (source[part, cols] - col_mean) * col_inv
                if keep is not None:
                    source[part, cols] = out
                if layer < 2:
                    gain, bias = ((gain_1, bias_1), (gain_2, bias_2))[layer]
                    out = jnp.maximum(out * gain[:, cols] + bias[:, cols], 0.0)
                target[part, cols] = out.astype(jnp.bfloat16)
            return carry

        lax.fori_loop(0, groups, group, 0)

    def store(number, src, dst):
        copy = pltpu.make_async_copy(src, dst, store_sems.at[number])
        copy.start()
        return copy

    copies[0].wait()
    copies[1].wait()
    product(0, feat.at[0], weight_in.at[0], pre.at[0])
    copies[2].wait()
    copies[3].wait()
    product(1, feat.at[1], weight_in.at[1], pre.at[1])
    normalise(0, pre.at[0], act.at[0], 0, normed_1)
    out_n1 = store(0, pre.at[0], normed_1)
    out_x1 = store(1, act.at[0], act_1)
    copies[4].wait()
    product(2, act.at[0], weight.at[0], pre.at[2])
    copies[6].start()
    normalise(1, pre.at[1], act.at[1], 0, None)
    copies[5].wait()
    out_n1.wait()
    product(3, act.at[1], weight.at[1], pre.at[0])
    copies[7].start()
    out_x1.wait()
    normalise(2, pre.at[2], act.at[0], 1, normed_2)
    out_n2 = store(2, pre.at[2], normed_2)
    out_x2 = store(3, act.at[0], act_2)
    copies[6].wait()
    product(4, act.at[0], weight.at[0], pre.at[1])
    normalise(3, pre.at[0], act.at[1], 1, None)
    copies[7].wait()
    out_n2.wait()
    product(5, act.at[1], weight.at[1], pre.at[2])
    out_x2.wait()
    normalise(4, pre.at[1], act.at[0], 2, normed_z)
    out_z = store(4, pre.at[1], normed_z)
    out_a = store(5, act.at[0], emb_a)
    normalise(5, pre.at[2], act.at[1], 2, None)
    out_b = store(6, act.at[1], emb_b)
    for copy in (out_z, out_a, out_b):
        copy.wait()


def forward_pass(feat_a, feat_b, w_in, t_in, w_mid, t_mid, w_out, t_out, vectors, shards, row_count):
    rows, feat_dim = feat_a.shape
    width = w_mid.shape[0]
    groups = width // COLS
    vmem = pl.BlockSpec(memory_space=pltpu.VMEM)
    hbm = pl.BlockSpec(memory_space=pl.ANY)
    half_out = jax.ShapeDtypeStruct((rows, width), jnp.bfloat16)
    full_out = jax.ShapeDtypeStruct((rows, width), jnp.float32)
    return pl.pallas_call(
        functools.partial(forward_kernel, shards, row_count),
        out_shape=(half_out, half_out, full_out, full_out, full_out, half_out, half_out, jax.ShapeDtypeStruct((3, 8, COLS), jnp.float32)),
        in_specs=[hbm] * 8 + [vmem] * 4,
        out_specs=(hbm,) * 7 + (vmem,),
        scratch_shapes=[
            pltpu.VMEM((3, rows, width), jnp.float32),
            pltpu.VMEM((2, rows, width), jnp.bfloat16),
            pltpu.VMEM((2, rows, feat_dim), jnp.bfloat16),
            pltpu.VMEM((2, feat_dim, width), jnp.bfloat16),
            pltpu.VMEM((2, width, width), jnp.bfloat16),
            pltpu.VMEM((6, shards, 2 * groups, COLS), jnp.float32),
            pltpu.VMEM((6, 2 * groups, COLS), jnp.float32),
            pltpu.SemaphoreType.DMA((6, shards)),
            pltpu.SemaphoreType.DMA((6, shards)),
            pltpu.SemaphoreType.DMA((8,)),
            pltpu.SemaphoreType.DMA((7,)),
        ],
        compiler_params=pltpu.CompilerParams(collective_id=4, has_side_effects=True, vmem_limit_bytes=VMEM_LIMIT),
        cost_estimate=pl.CostEstimate(flops=4 * rows * width * (2 * width + feat_dim), bytes_accessed=24 * width * width, transcendentals=0),
        name="forward",
    )(feat_a, feat_b, w_in, t_in, w_mid, t_mid, w_out, t_out, *vectors)


PAIR, RS1, RS2, RS3, AG3, AG2, AG1, AGP, LOCAL = range(9)


PARTS = 2


def columns_of(unit, width):
    return pl.ds(pl.multiple_of(lax.rem(unit, PARTS) * width, UNIT), width)


class Exchange:
    def __init__(self, me, ring, halves, gathered, recv_pair, recv_1, recv_2, recv_3, total, send_sems, recv_sems, row_of, depth, send_total=False):
        self.depth, self.send_total = depth, send_total
        self.me, self.ring, self.halves, self.gathered = me, ring, halves, gathered
        self.recv_pair, self.recv_1, self.recv_2, self.recv_3, self.total = recv_pair, recv_1, recv_2, recv_3, total
        self.send_sems, self.recv_sems, self.row_of = send_sems, recv_sems, row_of

    def axes(self, unit):
        def mask(shift):
            axis = lax.rem(unit + shift, 3)
            return 2 + axis + axis * axis

        (p1, b1), (p2, b2), (p3, b3) = (flip(self.me, mask(shift)) for shift in range(3))
        return (p1, p2, p3), (b1, b2, b3)

    def copy(self, unit, kind):
        (p1, p2, p3), (b1, b2, b3) = self.axes(unit)
        partner, half = flip(self.me, 1)

        def rows(start, size):
            return pl.ds(pl.multiple_of(start, 16), size)

        slot = lax.rem(unit, self.depth)
        total = self.total.at[slot]
        row = self.row_of(unit, half)
        if kind == PAIR:
            src, dst, peer = self.halves.at[lax.rem(unit, self.ring)], self.recv_pair.at[slot], partner
        elif kind == RS1:
            src, dst, peer = total.at[rows((1 - b1) * 64, 64)], self.recv_1.at[lax.rem(unit, self.recv_1.shape[0])], p1
        elif kind == RS2:
            src, dst, peer = total.at[rows(b1 * 64 + (1 - b2) * 32, 32)], self.recv_2.at[lax.rem(unit, self.recv_2.shape[0])], p2
        elif kind == RS3:
            src, dst, peer = total.at[rows(b1 * 64 + b2 * 32 + (1 - b3) * 16, 16)], self.recv_3.at[lax.rem(unit, self.recv_3.shape[0])], p3
        else:
            start, size, peer = {
                AG3: (b1 * 64 + b2 * 32 + b3 * 16, 16, p3),
                AG2: (b1 * 64 + b2 * 32, 32, p2),
                AG1: (b1 * 64, 64, p1),
                AGP: (0, 128, partner),
            }[kind]
            src = dst = self.gathered.at[rows(row + start, size), columns_of(unit, total.shape[1])]
            if kind == AG3 and self.send_total:
                src = total.at[rows(start, size)]
        return pltpu.make_async_remote_copy(src_ref=src, dst_ref=dst, send_sem=self.send_sems.at[slot, kind], recv_sem=self.recv_sems.at[slot, kind], device_id=(peer,), device_id_type=MESH_ID)

    def reduce_step(self, unit, kind):
        _, (b1, b2, b3) = self.axes(unit)
        self.copy(unit, kind).wait()
        if kind == PAIR:
            start, size, landed = 0, 128, self.recv_pair
        elif kind == RS1:
            start, size, landed = b1 * 64, 64, self.recv_1
        else:
            start, size, landed = b1 * 64 + b2 * 32, 32, self.recv_2
        keep = pl.ds(pl.multiple_of(start, 16), size)
        slot = lax.rem(unit, self.depth)
        self.total[slot, keep] = self.total[slot, keep] + landed[lax.rem(unit, landed.shape[0])]
        self.copy(unit, kind + 1).start()

    def owned(self, unit):
        _, (b1, b2, b3) = self.axes(unit)
        return b1 * 64 + b2 * 32 + b3 * 16


def enter(me):
    barrier = pltpu.get_barrier_semaphore()
    for mask in (1, 2, 4, 8):
        pl.semaphore_signal(barrier, inc=1, device_id=(flip(me, mask)[0],), device_id_type=MESH_ID)
    pl.semaphore_wait(barrier, 4)


def pipeline(units, lags, stages):
    def step(now, carry):
        for lag, stage in reversed(list(zip(lags, stages))):
            unit = now - lag

            @pl.when((unit >= 0) & (unit < units))
            def _(unit=unit, stage=stage):
                stage(unit)

        return carry

    lax.fori_loop(0, units + max(lags), step, 0)


def product_unit(left_ref, right_ref, col_other, col_mine, halves, mine, ring, slot, unit, blocks):
    left = jnp.concatenate([left_ref[:, pl.ds(pl.multiple_of(col_other, UNIT), UNIT)], left_ref[:, pl.ds(pl.multiple_of(col_mine, UNIT), UNIT)]], axis=1)
    part = halves.shape[2]
    width = part // blocks
    for block in range(blocks):
        cols = pl.ds(block * width, width)
        source = pl.ds(pl.multiple_of(lax.rem(unit, PARTS) * part + block * width, UNIT), width)
        out = contract_rows(left, right_ref[:, source])
        halves[ring, :, cols] = out[:UNIT]
        mine[slot, :, cols] = out[UNIT:]


RING = 3
CORR_LAGS = (0, 2, 5, 7, 10, 13, 16, 19, 21)


def corr_kernel(shards, row_count, off_ref, inv_ref, emb_a, emb_b, normed, emb_out, back_out, loss_ref, left_ref, right_ref, grad_ref, emb_grad, back, norm_in, loss_acc, wide, slots, halves, recv_pair, recv_1, recv_2, recv_3, total, send_sems, recv_sems, sum_send, sum_recv, norm_sems, store_sems):
    me = lax.axis_index(DATA_AXIS)
    loads = [pltpu.make_async_copy(emb_b, right_ref, store_sems.at[0]), pltpu.make_async_copy(emb_a, left_ref, store_sems.at[1])]
    for copy in loads:
        copy.start()
    rows, width = right_ref.shape
    half_rows = width // 2
    units = half_rows // UNIT * PARTS
    part_width = width // PARTS
    groups = width // COLS
    _, half = flip(me, 1)
    enter_all(me, shards)
    ex = Exchange(me, RING, halves, grad_ref, recv_pair, recv_1, recv_2, recv_3, total, send_sems, recv_sems, lambda unit, h: h * half_rows + lax.div(unit, PARTS) * UNIT, units)
    sums = SumExchange(me, shards, slots, sum_send, sum_recv)
    loss_acc[...] = jnp.zeros_like(loss_acc)
    for copy in loads:
        copy.wait()

    def produce(unit):
        @pl.when(unit >= RING)
        def _():
            ex.copy(unit - RING, PAIR).wait_send()

        local = lax.div(unit, PARTS) * UNIT
        product_unit(left_ref, right_ref, (1 - half) * half_rows + local, half * half_rows + local, halves, total, lax.rem(unit, RING), unit, unit, 2)
        ex.copy(unit, PAIR).start()

    def pair_step(unit):
        ex.copy(unit, PAIR).wait_recv()
        total[unit] = total[unit] + recv_pair[unit]
        ex.copy(unit, RS1).start()

    def finish(unit):
        ex.copy(unit, RS3).wait()
        start = ex.owned(unit)
        keep = pl.ds(pl.multiple_of(start, 16), 16)
        corr = (total[unit, keep] + recv_3[unit]) * (1.0 / row_count)
        row = half * half_rows + lax.div(unit, PARTS) * UNIT + start
        shift = row - lax.rem(unit, PARTS) * part_width
        on_diag = lax.broadcasted_iota(jnp.int32, (16, part_width), 0) + shift == lax.broadcasted_iota(jnp.int32, (16, part_width), 1)
        off_weight = off_ref[0, 0]
        miss = 1.0 - corr
        terms = jnp.where(on_diag, miss * miss, off_weight * (corr * corr))
        loss_acc[...] += terms[:8] + terms[8:]
        grad = jnp.where(on_diag, -2.0 * miss, 2.0 * off_weight * corr).astype(jnp.bfloat16)
        grad_ref[pl.ds(pl.multiple_of(row, 16), 16), columns_of(unit, part_width)] = grad
        ex.copy(unit, AG3).start()

    def forward(kind):
        def stage(unit):
            ex.copy(unit, kind).wait()
            if kind != AGP:
                ex.copy(unit, kind + 1).start()

            if kind == AG1:

                @pl.when(lax.rem(unit, PARTS) == PARTS - 1)
                def _():
                    block = lax.div(unit, PARTS)
                    for side in range(2):
                        load_norm(row_of(block, side), lax.rem(block, 2), side).start()

        return stage

    def row_of(unit, side):
        return (half + side * (1 - 2 * half)) * half_rows + unit * UNIT

    def lanes(start):
        return pl.ds(pl.multiple_of(start, UNIT), UNIT)

    def load_norm(start, slot, side):
        return pltpu.make_async_copy(normed.at[:, lanes(start)], norm_in.at[slot, side], norm_sems.at[slot, side])

    def arrive(unit):
        ex.copy(unit, AGP).wait()

        @pl.when(lax.rem(unit, PARTS) == PARTS - 1)
        def _():
            embed(lax.div(unit, PARTS))

    def embed(unit):
        slot = lax.rem(unit, 2)
        starts = [row_of(unit, side) for side in range(2)]
        rhs = jnp.concatenate([grad_ref[lanes(start)] for start in starts], axis=0)
        for side in range(2):
            load_norm(starts[side], slot, side).wait()
        plain = [jnp.zeros((1, UNIT), jnp.float32)] * 2
        crossed = [jnp.zeros((1, UNIT), jnp.float32)] * 2
        for chunk in range(rows // ROWS):
            part = pl.ds(chunk * ROWS, ROWS)
            out = contract_cols(right_ref[part], rhs) * (1.0 / row_count)
            for side in range(2):
                piece = out[:, side * UNIT : (side + 1) * UNIT]
                emb_grad[part, lanes(starts[side])] = piece
                plain[side] = plain[side] + jnp.sum(piece, axis=0, keepdims=True)
                crossed[side] = crossed[side] + jnp.sum(piece * norm_in[slot, side, part], axis=0, keepdims=True)
        for side in range(2):
            wide[0:1, lanes(starts[side])] = plain[side]
            wide[1:2, lanes(starts[side])] = crossed[side]

    pipeline(units, CORR_LAGS, [produce, pair_step, lambda u: ex.reduce_step(u, RS1), lambda u: ex.reduce_step(u, RS2), finish, forward(AG3), forward(AG2), forward(AG1), arrive])
    for unit in range(units - RING, units):
        ex.copy(unit, PAIR).wait_send()
    folded = loss_acc[:, :UNIT]
    for index in range(1, part_width // UNIT):
        folded = folded + loss_acc[:, index * UNIT : (index + 1) * UNIT]
    slots[0, me, :, COLS:] = folded
    for index in range(groups):
        cols = pl.ds(index * COLS, COLS)
        slots[0, me, index : index + 1, :COLS] = wide[0:1, cols]
        slots[0, me, groups + index : groups + index + 1, :COLS] = wide[1:2, cols]
    sums.start(0)
    store_emb = pltpu.make_async_copy(emb_grad, emb_out, store_sems.at[0])
    store_emb.start()

    def load_block(index, slot):
        return [load_norm((2 * index + side) * UNIT, slot, side) for side in range(2)]

    for copy in load_block(0, 0) + load_block(1, 1):
        copy.start()
    summed = sums.finish(0)
    loss_ref[0, 0] = jnp.sum(summed[:, COLS:])
    means = summed[:, :COLS] / row_count
    for index in range(groups):
        cols = pl.ds(index * COLS, COLS)
        wide[0:1, cols] = means[index : index + 1]
        wide[1:2, cols] = means[groups + index : groups + index + 1]
        wide[2:3, cols] = inv_ref[2, index : index + 1]

    def norm_back(index, carry):
        slot = lax.rem(index, 2)
        for side, copy in enumerate(load_block(index, slot)):
            copy.wait()
            start = (2 * index + side) * UNIT
            mean_g, mean_gn, inv = wide[0:1, lanes(start)], wide[1:2, lanes(start)], wide[2:3, lanes(start)]
            for chunk in range(rows // ROWS):
                part = pl.ds(chunk * ROWS, ROWS)
                back[part, lanes(start)] = ((emb_grad[part, lanes(start)] - mean_g - norm_in[slot, side, part] * mean_gn) * inv).astype(jnp.bfloat16)

        @pl.when(index + 2 < width // (2 * UNIT))
        def _():
            for copy in load_block(index + 2, slot):
                copy.start()

        return carry

    lax.fori_loop(0, width // (2 * UNIT), norm_back, 0)
    store_back = pltpu.make_async_copy(back, back_out, store_sems.at[1])
    store_back.start()
    store_emb.wait()
    store_back.wait()


def exchange_scratch(units, width):
    return [
        pltpu.VMEM((RING, UNIT, width), jnp.float32),
        pltpu.VMEM((units, UNIT, width), jnp.float32),
        pltpu.VMEM((units, 64, width), jnp.float32),
        pltpu.VMEM((units, 32, width), jnp.float32),
        pltpu.VMEM((units, 16, width), jnp.float32),
        pltpu.VMEM((units, UNIT, width), jnp.float32),
        pltpu.SemaphoreType.DMA((units, 9)),
        pltpu.SemaphoreType.DMA((units, 9)),
    ]


def corr_grad(emb_a, emb_b, normed, inv_std, off_weight, shards, row_count):
    rows, width = emb_a.shape
    vmem = pl.BlockSpec(memory_space=pltpu.VMEM)
    hbm = pl.BlockSpec(memory_space=pl.ANY)
    return pl.pallas_call(
        functools.partial(corr_kernel, shards, row_count),
        out_shape=(jax.ShapeDtypeStruct((rows, width), jnp.float32), jax.ShapeDtypeStruct((rows, width), jnp.bfloat16), jax.ShapeDtypeStruct((1, 1), jnp.float32)),
        in_specs=[pl.BlockSpec(memory_space=pltpu.SMEM), vmem, hbm, hbm, hbm],
        out_specs=(hbm, hbm, pl.BlockSpec(memory_space=pltpu.SMEM)),
        scratch_shapes=[
            pltpu.VMEM((rows, width), jnp.bfloat16),
            pltpu.VMEM((rows, width), jnp.bfloat16),
            pltpu.VMEM((width, width), jnp.bfloat16),
            pltpu.VMEM((rows, width), jnp.float32),
            pltpu.VMEM((rows, width), jnp.bfloat16),
            pltpu.VMEM((2, 2, rows, UNIT), jnp.float32),
            pltpu.VMEM((8, width // PARTS), jnp.float32),
            pltpu.VMEM((8, width), jnp.float32),
            pltpu.VMEM((1, shards, 8, COLS + UNIT), jnp.float32),
        ]
        + exchange_scratch(width // 2 // UNIT * PARTS, width // PARTS)
        + [pltpu.SemaphoreType.DMA((1, shards)), pltpu.SemaphoreType.DMA((1, shards)), pltpu.SemaphoreType.DMA((2, 2)), pltpu.SemaphoreType.DMA((2,))],
        compiler_params=pltpu.CompilerParams(collective_id=2, has_side_effects=True, vmem_limit_bytes=VMEM_LIMIT),
        cost_estimate=pl.CostEstimate(flops=4 * rows * width * width, bytes_accessed=8 * width * width, transcendentals=0),
        name="corr_grad",
    )(off_weight.reshape(1, 1), inv_std, emb_a, emb_b, normed)


DEPTH = 36
DEPTH_1, DEPTH_2, DEPTH_3 = 21, 12, 6
CHAIN = 11
PER_TICK = 1
BLOCK = 256
NORM_SLOTS = 3
WEIGHT_SLOTS = 3
BACK_LAGS = (1, 4, 6, 8, 11, 15, 20, 24)


def backward_kernel(shards, row_count, left_2, grad_z, w_out, normed_2, left_1, w_mid, normed_1, feat, gain_1, bias_1, gain_2, bias_2, inv_ref, out_ref, stat_ref, vecs, left, feat_in, grad, weight, normed, deriv, halves, mine, total, recv_1, recv_2, recv_3, wide, slots, send_sems, recv_sems, load_sems, weight_sems, normed_sems, sum_send, sum_recv):
    me = lax.axis_index(DATA_AXIS)
    _, half = flip(me, 1)
    rows, width = left.shape
    groups = width // COLS
    blocks = width // BLOCK
    units_full = width // 2 // UNIT * PARTS
    units_last = feat_in.shape[1] // 2 // UNIT * PARTS
    part_width = width // PARTS
    units = 2 * units_full + units_last
    ticks = units + max(BACK_LAGS)

    load_left = pltpu.make_async_copy(left_2, left, load_sems.at[0])
    load_grad = pltpu.make_async_copy(grad_z, grad.at[0], load_sems.at[1])
    load_feat = pltpu.make_async_copy(feat, feat_in, load_sems.at[2])

    def block_of(index):
        return pl.ds(pl.multiple_of(index * BLOCK, BLOCK), BLOCK)

    def weight_copy(source, number):
        slot = lax.rem(number, WEIGHT_SLOTS)
        return pltpu.make_async_copy(source.at[block_of(lax.rem(number, blocks))], weight.at[slot], weight_sems.at[slot])

    def weight_start(number):
        @pl.when(number < blocks)
        def _():
            weight_copy(w_out, number).start()

        @pl.when((number >= blocks) & (number < 2 * blocks))
        def _():
            weight_copy(w_mid, number).start()

    def normed_copy(source, number):
        slot = lax.rem(number, NORM_SLOTS)
        return pltpu.make_async_copy(source.at[:, block_of(lax.rem(number, blocks))], normed.at[slot], normed_sems.at[slot])

    def normed_start(number):
        @pl.when(number < 2 * blocks)
        def _():
            normed_copy(normed_2, number).start()

        @pl.when((number >= 2 * blocks) & (number < 4 * blocks))
        def _():
            normed_copy(normed_1, number).start()

    load_left.start()
    load_grad.start()
    for number in range(WEIGHT_SLOTS):
        weight_copy(w_out, number).start()
    for number in range(NORM_SLOTS):
        normed_copy(normed_2, number).start()
    load_feat.start()
    for layer, (gain, bias) in enumerate(((gain_2, bias_2), (gain_1, bias_1))):
        vecs[layer, 0:1] = gain[...]
        vecs[layer, 1:2] = bias[...]
        for index in range(groups):
            vecs[layer, 2:3, index * COLS : (index + 1) * COLS] = inv_ref[1 - layer, index : index + 1]
    enter_all(me, shards)

    def row_of(unit, h):
        layer = lax.div(unit, units_full)
        part = width // 2 - (width // 2 - feat_in.shape[1] // 2) * lax.div(layer, 2)
        return layer * width + h * part + lax.div(lax.rem(unit, units_full), PARTS) * UNIT

    ex = Exchange(me, 2, halves, out_ref, total, recv_1, recv_2, recv_3, total, send_sems, recv_sems, row_of, DEPTH, send_total=True)
    sums = SumExchange(me, shards, slots, sum_send, sum_recv)

    def produce(unit, source, part):
        @pl.when(unit >= 2)
        def _():
            ex.copy(unit - 2, PAIR).wait_send()

        which = lax.rem(lax.div(unit, units_full), 2)
        local = lax.div(lax.rem(unit, units_full), PARTS) * UNIT
        ring = lax.rem(unit, 2)
        product_unit(source, grad.at[which], (1 - half) * part + local, half * part + local, halves, mine, ring, ring, unit, 2)
        ex.copy(unit, PAIR).start()

    def pair_step(unit):
        slot = lax.rem(unit, DEPTH)
        ex.copy(unit, PAIR).wait_recv()
        total[slot] = total[slot] + mine[lax.rem(unit, 2)]
        ex.copy(unit, RS1).start()

    def to_out(unit):
        start = ex.owned(unit)
        slot = lax.rem(unit, DEPTH)
        return pltpu.make_async_copy(total.at[slot, pl.ds(pl.multiple_of(start, 16), 16)], out_ref.at[pl.ds(pl.multiple_of(row_of(unit, half) + start, 16), 16), columns_of(unit, part_width)], send_sems.at[slot, LOCAL])

    def finish(unit):
        ex.copy(unit, RS3).wait()
        slot = lax.rem(unit, DEPTH)
        keep = pl.ds(pl.multiple_of(ex.owned(unit), 16), 16)
        total[slot, keep] = total[slot, keep] + recv_3[lax.rem(unit, DEPTH_3)]
        to_out(unit).start()
        ex.copy(unit, AG3).start()

    def forward(kind):
        def stage(unit):
            if kind == AG3:
                to_out(unit).wait()
            ex.copy(unit, kind).wait()
            if kind != AGP:
                ex.copy(unit, kind + 1).start()

        return stage

    stages = [pair_step, lambda u: ex.reduce_step(u, RS1), lambda u: ex.reduce_step(u, RS2), finish, forward(AG3), forward(AG2), forward(AG1), forward(AGP)]

    def derivative(layer, index):
        number = layer * blocks + index
        stream = 2 * layer * blocks + index
        weight_copy(w_out, number).wait()
        normed_copy(normed_2, stream).wait()
        slot, weight_slot = lax.rem(stream, NORM_SLOTS), lax.rem(number, WEIGHT_SLOTS)
        cols = block_of(index)
        gain, bias = vecs[layer, 0:1, cols], vecs[layer, 1:2, cols]
        rhs = weight[weight_slot]
        sum_n = jnp.zeros((1, BLOCK), jnp.float32)
        sum_d = jnp.zeros((1, BLOCK), jnp.float32)
        for chunk in range(rows // BLOCK):
            part = pl.ds(chunk * BLOCK, BLOCK)
            n = normed[slot, part]
            d = jnp.where(n * gain + bias > 0.0, contract_cols(grad[layer, part], rhs), 0.0)
            deriv[part, cols] = d
            sum_n = sum_n + jnp.sum(d * n, axis=0, keepdims=True)
            sum_d = sum_d + jnp.sum(d, axis=0, keepdims=True)
        wide[0:1, cols] = sum_n
        wide[1:2, cols] = sum_d
        weight_start(number + WEIGHT_SLOTS)
        normed_start(stream + NORM_SLOTS)

    def send_sums(layer):
        for index in range(groups):
            cols = pl.ds(index * COLS, COLS)
            slots[layer, me, index : index + 1] = wide[0:1, cols]
            slots[layer, me, groups + index : groups + index + 1] = wide[1:2, cols]
        sums.start(layer)

    def next_grad(layer):
        summed = sums.finish(layer)
        for index in range(groups):
            cols = pl.ds(index * COLS, COLS)
            for row in range(2):
                line = summed[row * groups + index : row * groups + index + 1]
                stat_ref[layer, row : row + 1, cols] = line
                wide[2 + row : 3 + row, cols] = line / row_count

        def one(index, carry):
            stream = (2 * layer + 1) * blocks + index
            normed_copy(normed_2, stream).wait()
            slot = lax.rem(stream, NORM_SLOTS)
            cols = block_of(index)
            mean_n, mean_d = wide[2:3, cols], wide[3:4, cols]
            scale = vecs[layer, 0:1, cols] * vecs[layer, 2:3, cols]
            for chunk in range(rows // BLOCK):
                part = pl.ds(chunk * BLOCK, BLOCK)
                grad[1 - layer, part, cols] = ((deriv[part, cols] - mean_d - normed[slot, part] * mean_n) * scale).astype(jnp.bfloat16)
            normed_start(stream + NORM_SLOTS)
            return carry

        lax.fori_loop(0, blocks, one, 0)

    def tick(now, carry):
        for lag, stage in reversed(list(zip(BACK_LAGS, stages))):
            unit = now - lag

            @pl.when((unit >= 0) & (unit < units))
            def _(stage=stage, unit=unit):
                stage(unit)

        @pl.when(now < 2 * units_full)
        def _():
            @pl.when(lax.rem(now, units_full) == 0)
            def _():
                load_left.wait()

                @pl.when(now == 0)
                def _():
                    load_grad.wait()

            produce(now, left, width // 2)

            @pl.when(now == units_full - 1)
            def _():
                pltpu.make_async_copy(left_1, left, load_sems.at[0]).start()

        @pl.when((now >= 2 * units_full) & (now < units))
        def _():
            @pl.when(now == 2 * units_full)
            def _():
                load_feat.wait()

            produce(now, feat_in, feat_in.shape[1] // 2)

        layer, place = lax.div(now, CHAIN), lax.rem(now, CHAIN)
        steps = blocks // PER_TICK

        @pl.when((layer < 2) & (place < steps))
        def _():
            def one(index, carry):
                derivative(layer, place * PER_TICK + index)
                return carry

            lax.fori_loop(0, PER_TICK, one, 0)

            @pl.when(place == steps - 1)
            def _():
                send_sums(layer)

        @pl.when((layer < 2) & (place == CHAIN - 1))
        def _():
            next_grad(layer)

        return carry

    lax.fori_loop(0, ticks, tick, 0)
    for unit in (units - 2, units - 1):
        ex.copy(unit, PAIR).wait_send()


def backward(act_2, grad_z, w_out, normed_2, act_1, w_mid, normed_1, feat, vectors, inv_std, shards, row_count):
    rows, width = act_2.shape
    feat_dim = feat.shape[1]
    total_rows = 2 * width + feat_dim
    vmem = pl.BlockSpec(memory_space=pltpu.VMEM)
    hbm = pl.BlockSpec(memory_space=pl.ANY)
    return pl.pallas_call(
        functools.partial(backward_kernel, shards, row_count),
        out_shape=(jax.ShapeDtypeStruct((total_rows, width), jnp.float32), jax.ShapeDtypeStruct((2, 2, width), jnp.float32)),
        in_specs=[hbm] * 8 + [vmem] * 5,
        out_specs=(hbm, vmem),
        scratch_shapes=[
            pltpu.VMEM((2, 8, width), jnp.float32),
            pltpu.VMEM((rows, width), jnp.bfloat16),
            pltpu.VMEM((rows, feat_dim), jnp.bfloat16),
            pltpu.VMEM((2, rows, width), jnp.bfloat16),
            pltpu.VMEM((WEIGHT_SLOTS, BLOCK, width), jnp.bfloat16),
            pltpu.VMEM((NORM_SLOTS, rows, BLOCK), jnp.float32),
            pltpu.VMEM((rows, width), jnp.float32),
            pltpu.VMEM((2, UNIT, width // PARTS), jnp.float32),
            pltpu.VMEM((2, UNIT, width // PARTS), jnp.float32),
            pltpu.VMEM((DEPTH, UNIT, width // PARTS), jnp.float32),
            pltpu.VMEM((DEPTH_1, 64, width // PARTS), jnp.float32),
            pltpu.VMEM((DEPTH_2, 32, width // PARTS), jnp.float32),
            pltpu.VMEM((DEPTH_3, 16, width // PARTS), jnp.float32),
            pltpu.VMEM((8, width), jnp.float32),
            pltpu.VMEM((2, shards, 8, COLS), jnp.float32),
            pltpu.SemaphoreType.DMA((DEPTH, 9)),
            pltpu.SemaphoreType.DMA((DEPTH, 9)),
            pltpu.SemaphoreType.DMA((3,)),
            pltpu.SemaphoreType.DMA((WEIGHT_SLOTS,)),
            pltpu.SemaphoreType.DMA((NORM_SLOTS,)),
            pltpu.SemaphoreType.DMA((2, shards)),
            pltpu.SemaphoreType.DMA((2, shards)),
        ],
        compiler_params=pltpu.CompilerParams(collective_id=3, has_side_effects=True, vmem_limit_bytes=VMEM_LIMIT),
        cost_estimate=pl.CostEstimate(flops=2 * rows * width * (2 * width + total_rows), bytes_accessed=16 * width * width, transcendentals=0),
        name="backward",
    )(act_2, grad_z, w_out, normed_2, act_1, w_mid, normed_1, feat, *vectors, inv_std)


CHUNK = 256
FLIGHT = 8


def output_kernel(sums_ref, emb_ref, stat_ref, emb_out, in_out, mid_out, last_out, gain_1, bias_1, gain_2, bias_2, buffer, read_sems, write_sems):
    width = mid_out.shape[0]
    reads, writes = [], []
    for source, first, target in ((sums_ref, 0, last_out), (sums_ref, width, mid_out), (sums_ref, 2 * width, in_out), (emb_ref, 0, emb_out)):
        for start in range(0, target.shape[0], CHUNK):
            slot = len(reads) % FLIGHT
            reads.append(pltpu.make_async_copy(source.at[pl.ds(first + start, CHUNK)], buffer.at[slot], read_sems.at[slot]))
            writes.append(pltpu.make_async_copy(buffer.at[slot], target.at[pl.ds(start, CHUNK)], write_sems.at[slot]))
    for copy in reads[:FLIGHT]:
        copy.start()
    gain_1[...] = stat_ref[1, 0:1]
    bias_1[...] = stat_ref[1, 1:2]
    gain_2[...] = stat_ref[0, 0:1]
    bias_2[...] = stat_ref[0, 1:2]
    behind = FLIGHT // 2
    for index in range(len(reads) + behind):
        if index < len(reads):
            reads[index].wait()
            writes[index].start()
        if index >= behind:
            writes[index - behind].wait()
            if index - behind + FLIGHT < len(reads):
                reads[index - behind + FLIGHT].start()


def to_outputs(sums, emb_grad, stats, width):
    feat_dim = sums.shape[0] - 2 * width
    vmem = pl.BlockSpec(memory_space=pltpu.VMEM)
    hbm = pl.BlockSpec(memory_space=pl.ANY)
    row = jax.ShapeDtypeStruct((1, width), jnp.float32)
    return pl.pallas_call(
        output_kernel,
        out_shape=(jax.ShapeDtypeStruct(emb_grad.shape, jnp.float32), jax.ShapeDtypeStruct((feat_dim, width), jnp.float32), jax.ShapeDtypeStruct((width, width), jnp.float32), jax.ShapeDtypeStruct((width, width), jnp.float32)) + (row,) * 4,
        in_specs=[hbm, hbm, vmem],
        out_specs=(hbm,) * 4 + (vmem,) * 4,
        scratch_shapes=[pltpu.VMEM((FLIGHT, CHUNK, width), jnp.float32), pltpu.SemaphoreType.DMA((FLIGHT,)), pltpu.SemaphoreType.DMA((FLIGHT,))],
        compiler_params=pltpu.CompilerParams(vmem_limit_bytes=VMEM_LIMIT),
        name="to_outputs",
    )(sums, emb_grad, stats)


def solution(mesh):
    shards = mesh.shape[DATA_AXIS]
    row_part = P(DATA_AXIS, None)
    replicated = P()

    def local_step(feat_a, feat_b, w_in, w_mid, w_out, t_in, t_mid, t_out, gain_1, bias_1, gain_2, bias_2, off_weight):
        row_count = feat_a.shape[0] * shards

        vectors = [vector.reshape(1, -1) for vector in (gain_1, bias_1, gain_2, bias_2)]
        act_1, act_2, normed_1, normed_2, zh_a, emb_a, emb_b, inv_std = forward_pass(feat_a, feat_b, w_in, t_in, w_mid, t_mid, w_out, t_out, vectors, shards, row_count)
        width = w_mid.shape[0]
        grad_emb, grad_z, loss_sums = corr_grad(emb_a, emb_b, zh_a, inv_std, off_weight, shards, row_count)
        loss_value = loss_sums[0, 0]
        sums, stats = backward(act_2, grad_z, w_out, normed_2, act_1, w_mid, normed_1, feat_a, vectors, inv_std, shards, row_count)
        grad_emb, grad_in, grad_mid, grad_out, *vector_grads = to_outputs(sums, grad_emb, stats, width)
        return (loss_value, grad_emb, grad_in, grad_mid, grad_out, *[vector.reshape(-1) for vector in vector_grads])

    return jax.shard_map(local_step, mesh=mesh, in_specs=(row_part, row_part) + (replicated,) * 11, out_specs=(replicated, row_part) + (replicated,) * 7, check_vma=False)
```

```python
import functools

import jax
import jax.numpy as jnp
from jax import lax
from jax.experimental import pallas as pl
from jax.experimental.pallas import tpu as pltpu
from jax.sharding import PartitionSpec as P

NORM_EPS = 1e-5
DATA_AXIS = "data"
MESH_ID = pl.DeviceIdType.MESH
UNIT = 128
VMEM_LIMIT = 66_000_000


def contract_rows(left_op, right_op):
    return lax.dot_general(left_op, right_op, (((0,), (0,)), ((), ())), preferred_element_type=jnp.float32)


def contract_cols(left_op, right_op):
    return lax.dot_general(left_op, right_op, (((1,), (1,)), ((), ())), preferred_element_type=jnp.float32)


def flip(me, mask):
    bit = lax.rem(lax.div(me, mask), 2)
    return me + mask * (1 - 2 * bit), bit


class SumExchange:
    def __init__(self, me, shards, slots, send_sems, recv_sems):
        self.me, self.shards, self.slots, self.send_sems, self.recv_sems = me, shards, slots, send_sems, recv_sems

    def copy(self, index, peer, slot):
        return pltpu.make_async_remote_copy(src_ref=self.slots.at[index, self.me], dst_ref=self.slots.at[index, slot], send_sem=self.send_sems.at[index, peer], recv_sem=self.recv_sems.at[index, slot], device_id=(peer,), device_id_type=MESH_ID)

    def peers(self):
        return [lax.rem(self.me + shift, self.shards) for shift in range(1, self.shards)]

    def start(self, index):
        for peer in self.peers():
            self.copy(index, peer, self.me).start()

    def finish(self, index):
        for peer in self.peers():
            self.copy(index, peer, peer).wait_recv()
            self.copy(index, peer, self.me).wait_send()
        summed = self.slots[index, 0]
        for slot in range(1, self.shards):
            summed = summed + self.slots[index, slot]
        return summed


def enter_all(me, shards):
    barrier = pltpu.get_barrier_semaphore()
    for shift in range(1, shards):
        pl.semaphore_signal(barrier, inc=1, device_id=(lax.rem(me + shift, shards),), device_id_type=MESH_ID)
    pl.semaphore_wait(barrier, shards - 1)


COLS = 512
ROWS = 1024


def forward_kernel(shards, row_count, feat_a, feat_b, w_in, t_in, w_mid, t_mid, w_out, t_out, gain_1, bias_1, gain_2, bias_2, act_1, act_2, normed_1, normed_2, normed_z, emb_a, emb_b, inv_ref, pre, act, feat, weight_in, weight, slots, sums, send_sems, recv_sems, load_sems, store_sems):
    me = lax.axis_index(DATA_AXIS)
    rows, width = act_1.shape
    groups = width // COLS
    copies = [pltpu.make_async_copy(src, dst, load_sems.at[index]) for index, (src, dst) in enumerate([(feat_a, feat.at[0]), (w_in, weight_in.at[0]), (feat_b, feat.at[1]), (t_in, weight_in.at[1]), (w_mid, weight.at[0]), (t_mid, weight.at[1]), (w_out, weight.at[0]), (t_out, weight.at[1])])]
    for index in range(4):
        copies[index].start()
    enter_all(me, shards)
    ex = SumExchange(me, shards, slots, send_sems, recv_sems)

    def product(index, source, matrix, target):
        def group(number, carry):
            cols = pl.ds(pl.multiple_of(number * COLS, COLS), COLS)
            total = jnp.zeros((1, COLS), jnp.float32)
            squares = jnp.zeros((1, COLS), jnp.float32)
            for chunk in range(rows // ROWS):
                part = pl.ds(chunk * ROWS, ROWS)
                out = jnp.dot(source[part], matrix[:, cols], preferred_element_type=jnp.float32)
                target[part, cols] = out
                total = total + jnp.sum(out, axis=0, keepdims=True)
                squares = squares + jnp.sum(out * out, axis=0, keepdims=True)
            slots[index, me, pl.ds(number, 1)] = total
            slots[index, me, pl.ds(number + groups, 1)] = squares
            return carry

        lax.fori_loop(0, groups, group, 0)
        ex.start(index)

    def normalise(index, source, target, layer, keep):
        summed = ex.finish(index) / row_count
        mean = summed[:groups]
        inv = lax.rsqrt(summed[groups:] - mean * mean + NORM_EPS)
        sums[index, :groups] = mean
        sums[index, groups:] = inv
        if keep is not None:
            inv_ref[layer, :groups] = inv

        def group(number, carry):
            cols = pl.ds(pl.multiple_of(number * COLS, COLS), COLS)
            col_mean = sums[index, pl.ds(number, 1)]
            col_inv = sums[index, pl.ds(number + groups, 1)]
            for chunk in range(rows // ROWS):
                part = pl.ds(chunk * ROWS, ROWS)
                out = (source[part, cols] - col_mean) * col_inv
                if keep is not None:
                    source[part, cols] = out
                if layer < 2:
                    gain, bias = ((gain_1, bias_1), (gain_2, bias_2))[layer]
                    out = jnp.maximum(out * gain[:, cols] + bias[:, cols], 0.0)
                target[part, cols] = out.astype(jnp.bfloat16)
            return carry

        lax.fori_loop(0, groups, group, 0)

    def store(number, src, dst):
        copy = pltpu.make_async_copy(src, dst, store_sems.at[number])
        copy.start()
        return copy

    copies[0].wait()
    copies[1].wait()
    copies[4].start()
    copies[5].start()
    product(0, feat.at[0], weight_in.at[0], pre.at[0])
    copies[2].wait()
    copies[3].wait()
    product(1, feat.at[1], weight_in.at[1], pre.at[1])
    normalise(0, pre.at[0], act.at[0], 0, normed_1)
    out_n1 = store(0, pre.at[0], normed_1)
    out_x1 = store(1, act.at[0], act_1)
    copies[4].wait()
    product(2, act.at[0], weight.at[0], pre.at[2])
    copies[6].start()
    normalise(1, pre.at[1], act.at[1], 0, None)
    copies[5].wait()
    out_n1.wait()
    product(3, act.at[1], weight.at[1], pre.at[0])
    copies[7].start()
    out_x1.wait()
    normalise(2, pre.at[2], act.at[0], 1, normed_2)
    out_n2 = store(2, pre.at[2], normed_2)
    out_x2 = store(3, act.at[0], act_2)
    copies[6].wait()
    product(4, act.at[0], weight.at[0], pre.at[1])
    normalise(3, pre.at[0], act.at[1], 1, None)
    copies[7].wait()
    out_n2.wait()
    product(5, act.at[1], weight.at[1], pre.at[2])
    out_x2.wait()
    normalise(4, pre.at[1], act.at[0], 2, normed_z)
    out_z = store(4, pre.at[1], normed_z)
    out_a = store(5, act.at[0], emb_a)
    normalise(5, pre.at[2], act.at[1], 2, None)
    out_b = store(6, act.at[1], emb_b)
    for copy in (out_z, out_a, out_b):
        copy.wait()


def forward_pass(feat_a, feat_b, w_in, t_in, w_mid, t_mid, w_out, t_out, vectors, shards, row_count):
    rows, feat_dim = feat_a.shape
    width = w_mid.shape[0]
    groups = width // COLS
    vmem = pl.BlockSpec(memory_space=pltpu.VMEM)
    hbm = pl.BlockSpec(memory_space=pl.ANY)
    half_out = jax.ShapeDtypeStruct((rows, width), jnp.bfloat16)
    full_out = jax.ShapeDtypeStruct((rows, width), jnp.float32)
    return pl.pallas_call(
        functools.partial(forward_kernel, shards, row_count),
        out_shape=(half_out, half_out, full_out, full_out, full_out, half_out, half_out, jax.ShapeDtypeStruct((3, 8, COLS), jnp.float32)),
        in_specs=[hbm] * 8 + [vmem] * 4,
        out_specs=(hbm,) * 7 + (vmem,),
        scratch_shapes=[
            pltpu.VMEM((3, rows, width), jnp.float32),
            pltpu.VMEM((2, rows, width), jnp.bfloat16),
            pltpu.VMEM((2, rows, feat_dim), jnp.bfloat16),
            pltpu.VMEM((2, feat_dim, width), jnp.bfloat16),
            pltpu.VMEM((2, width, width), jnp.bfloat16),
            pltpu.VMEM((6, shards, 2 * groups, COLS), jnp.float32),
            pltpu.VMEM((6, 2 * groups, COLS), jnp.float32),
            pltpu.SemaphoreType.DMA((6, shards)),
            pltpu.SemaphoreType.DMA((6, shards)),
            pltpu.SemaphoreType.DMA((8,)),
            pltpu.SemaphoreType.DMA((7,)),
        ],
        compiler_params=pltpu.CompilerParams(collective_id=4, has_side_effects=True, vmem_limit_bytes=VMEM_LIMIT),
        cost_estimate=pl.CostEstimate(flops=4 * rows * width * (2 * width + feat_dim), bytes_accessed=24 * width * width, transcendentals=0),
        name="forward",
    )(feat_a, feat_b, w_in, t_in, w_mid, t_mid, w_out, t_out, *vectors)


PAIR, RS1, RS2, RS3, AG3, AG2, AG1, AGP, LOCAL = range(9)


PARTS = 2


def columns_of(unit, width):
    return pl.ds(pl.multiple_of(lax.rem(unit, PARTS) * width, UNIT), width)


class Exchange:
    def __init__(self, me, ring, halves, gathered, recv_pair, recv_1, recv_2, recv_3, total, send_sems, recv_sems, row_of, depth, send_total=False):
        self.depth, self.send_total = depth, send_total
        self.me, self.ring, self.halves, self.gathered = me, ring, halves, gathered
        self.recv_pair, self.recv_1, self.recv_2, self.recv_3, self.total = recv_pair, recv_1, recv_2, recv_3, total
        self.send_sems, self.recv_sems, self.row_of = send_sems, recv_sems, row_of

    def axes(self, unit):
        def mask(shift):
            axis = lax.rem(unit + shift, 3)
            return 2 + axis + axis * axis

        (p1, b1), (p2, b2), (p3, b3) = (flip(self.me, mask(shift)) for shift in range(3))
        return (p1, p2, p3), (b1, b2, b3)

    def copy(self, unit, kind):
        (p1, p2, p3), (b1, b2, b3) = self.axes(unit)
        partner, half = flip(self.me, 1)

        def rows(start, size):
            return pl.ds(pl.multiple_of(start, 16), size)

        slot = lax.rem(unit, self.depth)
        total = self.total.at[slot]
        row = self.row_of(unit, half)
        if kind == PAIR:
            src, dst, peer = self.halves.at[lax.rem(unit, self.ring)], self.recv_pair.at[slot], partner
        elif kind == RS1:
            src, dst, peer = total.at[rows((1 - b1) * 64, 64)], self.recv_1.at[lax.rem(unit, self.recv_1.shape[0])], p1
        elif kind == RS2:
            src, dst, peer = total.at[rows(b1 * 64 + (1 - b2) * 32, 32)], self.recv_2.at[lax.rem(unit, self.recv_2.shape[0])], p2
        elif kind == RS3:
            src, dst, peer = total.at[rows(b1 * 64 + b2 * 32 + (1 - b3) * 16, 16)], self.recv_3.at[lax.rem(unit, self.recv_3.shape[0])], p3
        else:
            start, size, peer = {
                AG3: (b1 * 64 + b2 * 32 + b3 * 16, 16, p3),
                AG2: (b1 * 64 + b2 * 32, 32, p2),
                AG1: (b1 * 64, 64, p1),
                AGP: (0, 128, partner),
            }[kind]
            src = dst = self.gathered.at[rows(row + start, size), columns_of(unit, total.shape[1])]
            if kind == AG3 and self.send_total:
                src = total.at[rows(start, size)]
        return pltpu.make_async_remote_copy(src_ref=src, dst_ref=dst, send_sem=self.send_sems.at[slot, kind], recv_sem=self.recv_sems.at[slot, kind], device_id=(peer,), device_id_type=MESH_ID)

    def reduce_step(self, unit, kind):
        _, (b1, b2, b3) = self.axes(unit)
        self.copy(unit, kind).wait()
        if kind == PAIR:
            start, size, landed = 0, 128, self.recv_pair
        elif kind == RS1:
            start, size, landed = b1 * 64, 64, self.recv_1
        else:
            start, size, landed = b1 * 64 + b2 * 32, 32, self.recv_2
        keep = pl.ds(pl.multiple_of(start, 16), size)
        slot = lax.rem(unit, self.depth)
        self.total[slot, keep] = self.total[slot, keep] + landed[lax.rem(unit, landed.shape[0])]
        self.copy(unit, kind + 1).start()

    def owned(self, unit):
        _, (b1, b2, b3) = self.axes(unit)
        return b1 * 64 + b2 * 32 + b3 * 16


def enter(me):
    barrier = pltpu.get_barrier_semaphore()
    for mask in (1, 2, 4, 8):
        pl.semaphore_signal(barrier, inc=1, device_id=(flip(me, mask)[0],), device_id_type=MESH_ID)
    pl.semaphore_wait(barrier, 4)


def pipeline(units, lags, stages):
    def step(now, carry):
        for lag, stage in reversed(list(zip(lags, stages))):
            unit = now - lag

            @pl.when((unit >= 0) & (unit < units))
            def _(unit=unit, stage=stage):
                stage(unit)

        return carry

    lax.fori_loop(0, units + max(lags), step, 0)


def product_unit(left_ref, right_ref, col_other, col_mine, halves, mine, ring, slot, unit, blocks):
    left = jnp.concatenate([left_ref[:, pl.ds(pl.multiple_of(col_other, UNIT), UNIT)], left_ref[:, pl.ds(pl.multiple_of(col_mine, UNIT), UNIT)]], axis=1)
    part = halves.shape[2]
    width = part // blocks
    for block in range(blocks):
        cols = pl.ds(block * width, width)
        source = pl.ds(pl.multiple_of(lax.rem(unit, PARTS) * part + block * width, UNIT), width)
        out = contract_rows(left, right_ref[:, source])
        halves[ring, :, cols] = out[:UNIT]
        mine[slot, :, cols] = out[UNIT:]


RING = 3
BACK_ROWS = 1024
CORR_LAGS = (0, 2, 5, 7, 10, 13, 16, 19, 21)


def corr_kernel(shards, row_count, off_ref, inv_ref, emb_a, emb_b, normed, emb_out, back_out, loss_ref, left_ref, right_ref, grad_ref, emb_grad, back, norm_in, loss_acc, wide, slots, halves, recv_pair, recv_1, recv_2, recv_3, total, send_sems, recv_sems, sum_send, sum_recv, norm_sems, store_sems, back_sems):
    me = lax.axis_index(DATA_AXIS)
    loads = [pltpu.make_async_copy(emb_b, right_ref, store_sems.at[0]), pltpu.make_async_copy(emb_a, left_ref, store_sems.at[1])]
    for copy in loads:
        copy.start()
    rows, width = right_ref.shape
    half_rows = width // 2
    units = half_rows // UNIT * PARTS
    part_width = width // PARTS
    groups = width // COLS
    _, half = flip(me, 1)
    enter_all(me, shards)
    ex = Exchange(me, RING, halves, grad_ref, recv_pair, recv_1, recv_2, recv_3, total, send_sems, recv_sems, lambda unit, h: h * half_rows + lax.div(unit, PARTS) * UNIT, units)
    sums = SumExchange(me, shards, slots, sum_send, sum_recv)
    loss_acc[...] = jnp.zeros_like(loss_acc)
    for copy in loads:
        copy.wait()

    def produce(unit):
        @pl.when(unit >= RING)
        def _():
            ex.copy(unit - RING, PAIR).wait_send()

        local = lax.div(unit, PARTS) * UNIT
        product_unit(left_ref, right_ref, (1 - half) * half_rows + local, half * half_rows + local, halves, total, lax.rem(unit, RING), unit, unit, 2)
        ex.copy(unit, PAIR).start()

    def pair_step(unit):
        ex.copy(unit, PAIR).wait_recv()
        total[unit] = total[unit] + recv_pair[unit]
        ex.copy(unit, RS1).start()

    def finish(unit):
        ex.copy(unit, RS3).wait()
        start = ex.owned(unit)
        keep = pl.ds(pl.multiple_of(start, 16), 16)
        corr = (total[unit, keep] + recv_3[unit]) * (1.0 / row_count)
        row = half * half_rows + lax.div(unit, PARTS) * UNIT + start
        shift = row - lax.rem(unit, PARTS) * part_width
        on_diag = lax.broadcasted_iota(jnp.int32, (16, part_width), 0) + shift == lax.broadcasted_iota(jnp.int32, (16, part_width), 1)
        off_weight = off_ref[0, 0]
        miss = 1.0 - corr
        terms = jnp.where(on_diag, miss * miss, off_weight * (corr * corr))
        loss_acc[...] += terms[:8] + terms[8:]
        grad = jnp.where(on_diag, -2.0 * miss, 2.0 * off_weight * corr).astype(jnp.bfloat16)
        grad_ref[pl.ds(pl.multiple_of(row, 16), 16), columns_of(unit, part_width)] = grad
        ex.copy(unit, AG3).start()

    def forward(kind):
        def stage(unit):
            ex.copy(unit, kind).wait()
            if kind != AGP:
                ex.copy(unit, kind + 1).start()

            if kind == AG1:

                @pl.when(lax.rem(unit, PARTS) == PARTS - 1)
                def _():
                    block = lax.div(unit, PARTS)
                    for side in range(2):
                        load_norm(row_of(block, side), lax.rem(block, 2), side).start()

        return stage

    for index in range(groups):
        wide[2:3, index * COLS : (index + 1) * COLS] = inv_ref[2, index : index + 1]

    def packed(which):
        piece = width // 8
        return [(4 * row + 2 * side + index, row, pl.ds(side * half_rows + (2 * which + index) * piece, piece)) for row in range(2) for side in range(2) for index in range(2)]

    def row_of(unit, side):
        return (half + side * (1 - 2 * half)) * half_rows + unit * UNIT

    def lanes(start):
        return pl.ds(pl.multiple_of(start, UNIT), UNIT)

    def load_norm(start, slot, side):
        return pltpu.make_async_copy(normed.at[:, lanes(start)], norm_in.at[slot, side], norm_sems.at[slot, side])

    def arrive(unit):
        ex.copy(unit, AGP).wait()

        @pl.when(lax.rem(unit, PARTS) == PARTS - 1)
        def _():
            embed(lax.div(unit, PARTS))

    def embed(unit):
        slot = lax.rem(unit, 2)
        starts = [row_of(unit, side) for side in range(2)]
        rhs = jnp.concatenate([grad_ref[lanes(start)] for start in starts], axis=0)
        for side in range(2):
            load_norm(starts[side], slot, side).wait()
        plain = [jnp.zeros((1, UNIT), jnp.float32)] * 2
        crossed = [jnp.zeros((1, UNIT), jnp.float32)] * 2
        for chunk in range(rows // ROWS):
            part = pl.ds(chunk * ROWS, ROWS)
            out = contract_cols(right_ref[part], rhs) * (1.0 / row_count)
            for side in range(2):
                piece = out[:, side * UNIT : (side + 1) * UNIT]
                emb_grad[part, lanes(starts[side])] = piece
                plain[side] = plain[side] + jnp.sum(piece, axis=0, keepdims=True)
                crossed[side] = crossed[side] + jnp.sum(piece * norm_in[slot, side, part], axis=0, keepdims=True)
        for side in range(2):
            wide[0:1, lanes(starts[side])] = plain[side]
            wide[1:2, lanes(starts[side])] = crossed[side]

        @pl.when(unit == half_rows // UNIT // 2 - 1)
        def _():
            for line, row, cols in packed(0):
                slots[0, me, line : line + 1, : width // 8] = wide[row : row + 1, cols]
            slots[0, me, :, width // 8 :] = jnp.zeros((8, UNIT), jnp.float32)
            sums.start(0)

    pipeline(units, CORR_LAGS, [produce, pair_step, lambda u: ex.reduce_step(u, RS1), lambda u: ex.reduce_step(u, RS2), finish, forward(AG3), forward(AG2), forward(AG1), arrive])
    for unit in range(units - RING, units):
        ex.copy(unit, PAIR).wait_send()
    folded = loss_acc[:, :UNIT]
    for index in range(1, part_width // UNIT):
        folded = folded + loss_acc[:, index * UNIT : (index + 1) * UNIT]
    for line, row, cols in packed(1):
        slots[1, me, line : line + 1, : width // 8] = wide[row : row + 1, cols]
    slots[1, me, :, width // 8 :] = folded
    sums.start(1)
    store_emb = pltpu.make_async_copy(emb_grad, emb_out, store_sems.at[0])
    store_emb.start()
    steps = width // (2 * UNIT)

    def block_at(position):
        place = lax.rem(position, steps // 2)
        return 2 * lax.div(position, steps // 2) + lax.rem(place, 2) + (steps // 2) * lax.div(place, 2)

    def load_block(position):
        return [load_norm((2 * block_at(position) + side) * UNIT, lax.rem(position, 2), side) for side in range(2)]

    def store_block(position):
        cols = pl.ds(pl.multiple_of(2 * block_at(position) * UNIT, 2 * UNIT), 2 * UNIT)
        return pltpu.make_async_copy(back.at[:, cols], back_out.at[:, cols], back_sems.at[position])

    for position in range(2):
        for copy in load_block(position):
            copy.start()

    def norm_back(position, carry):
        slot = lax.rem(position, 2)
        for side, copy in enumerate(load_block(position)):
            copy.wait()
            start = (2 * block_at(position) + side) * UNIT
            mean_g, mean_gn, inv = wide[0:1, lanes(start)], wide[1:2, lanes(start)], wide[2:3, lanes(start)]
            for chunk in range(rows // BACK_ROWS):
                part = pl.ds(chunk * BACK_ROWS, BACK_ROWS)
                back[part, lanes(start)] = ((emb_grad[part, lanes(start)] - mean_g - norm_in[slot, side, part] * mean_gn) * inv).astype(jnp.bfloat16)
        store_block(position).start()

        @pl.when(position + 2 < steps)
        def _():
            for copy in load_block(position + 2):
                copy.start()

        return carry

    for which in range(2):
        summed = sums.finish(which)
        if which == 1:
            loss_ref[0, 0] = jnp.sum(summed[:, width // 8 :])
        for line, row, cols in packed(which):
            wide[row : row + 1, cols] = summed[line : line + 1, : width // 8] / row_count
        lax.fori_loop(which * (steps // 2), (which + 1) * (steps // 2), norm_back, 0)
    for position in range(steps):
        store_block(position).wait()
    store_emb.wait()


def exchange_scratch(units, width):
    return [
        pltpu.VMEM((RING, UNIT, width), jnp.float32),
        pltpu.VMEM((units, UNIT, width), jnp.float32),
        pltpu.VMEM((units, 64, width), jnp.float32),
        pltpu.VMEM((units, 32, width), jnp.float32),
        pltpu.VMEM((units, 16, width), jnp.float32),
        pltpu.VMEM((units, UNIT, width), jnp.float32),
        pltpu.SemaphoreType.DMA((units, 9)),
        pltpu.SemaphoreType.DMA((units, 9)),
    ]


def corr_grad(emb_a, emb_b, normed, inv_std, off_weight, shards, row_count):
    rows, width = emb_a.shape
    vmem = pl.BlockSpec(memory_space=pltpu.VMEM)
    hbm = pl.BlockSpec(memory_space=pl.ANY)
    return pl.pallas_call(
        functools.partial(corr_kernel, shards, row_count),
        out_shape=(jax.ShapeDtypeStruct((rows, width), jnp.float32), jax.ShapeDtypeStruct((rows, width), jnp.bfloat16), jax.ShapeDtypeStruct((1, 1), jnp.float32)),
        in_specs=[pl.BlockSpec(memory_space=pltpu.SMEM), vmem, hbm, hbm, hbm],
        out_specs=(hbm, hbm, pl.BlockSpec(memory_space=pltpu.SMEM)),
        scratch_shapes=[
            pltpu.VMEM((rows, width), jnp.bfloat16),
            pltpu.VMEM((rows, width), jnp.bfloat16),
            pltpu.VMEM((width, width), jnp.bfloat16),
            pltpu.VMEM((rows, width), jnp.float32),
            pltpu.VMEM((rows, width), jnp.bfloat16),
            pltpu.VMEM((2, 2, rows, UNIT), jnp.float32),
            pltpu.VMEM((8, width // PARTS), jnp.float32),
            pltpu.VMEM((8, width), jnp.float32),
            pltpu.VMEM((2, shards, 8, width // 8 + UNIT), jnp.float32),
        ]
        + exchange_scratch(width // 2 // UNIT * PARTS, width // PARTS)
        + [pltpu.SemaphoreType.DMA((2, shards)), pltpu.SemaphoreType.DMA((2, shards)), pltpu.SemaphoreType.DMA((2, 2)), pltpu.SemaphoreType.DMA((2,)), pltpu.SemaphoreType.DMA((width // (2 * UNIT),))],
        compiler_params=pltpu.CompilerParams(collective_id=2, has_side_effects=True, vmem_limit_bytes=VMEM_LIMIT),
        cost_estimate=pl.CostEstimate(flops=4 * rows * width * width, bytes_accessed=8 * width * width, transcendentals=0),
        name="corr_grad",
    )(off_weight.reshape(1, 1), inv_std, emb_a, emb_b, normed)


DEPTH = 36
DEPTH_1, DEPTH_2, DEPTH_3 = 21, 12, 6
CHAIN = 11
PER_TICK = 1
CHAIN_START = 2
BLOCK = 256
NORM_SLOTS = 3
WEIGHT_SLOTS = 3
BACK_LAGS = (1, 4, 6, 8, 11, 14, 18, 21)


def backward_kernel(shards, row_count, left_2, grad_z, w_out, normed_2, left_1, w_mid, normed_1, feat, gain_1, bias_1, gain_2, bias_2, inv_ref, out_ref, stat_ref, vecs, left, feat_in, grad, weight, normed, deriv, halves, mine, total, recv_1, recv_2, recv_3, wide, slots, send_sems, recv_sems, load_sems, weight_sems, normed_sems, sum_send, sum_recv):
    me = lax.axis_index(DATA_AXIS)
    _, half = flip(me, 1)
    rows, width = left.shape
    groups = width // COLS
    blocks = width // BLOCK
    units_full = width // 2 // UNIT * PARTS
    units_last = feat_in.shape[1] // 2 // UNIT * PARTS
    part_width = width // PARTS
    units = 2 * units_full + units_last
    ticks = units + max(BACK_LAGS)

    load_left = pltpu.make_async_copy(left_2, left, load_sems.at[0])
    load_grad = pltpu.make_async_copy(grad_z, grad.at[0], load_sems.at[1])
    load_feat = pltpu.make_async_copy(feat, feat_in, load_sems.at[2])

    def block_of(index):
        return pl.ds(pl.multiple_of(index * BLOCK, BLOCK), BLOCK)

    def weight_copy(source, number):
        slot = lax.rem(number, WEIGHT_SLOTS)
        return pltpu.make_async_copy(source.at[block_of(lax.rem(number, blocks))], weight.at[slot], weight_sems.at[slot])

    def weight_start(number):
        @pl.when(number < blocks)
        def _():
            weight_copy(w_out, number).start()

        @pl.when((number >= blocks) & (number < 2 * blocks))
        def _():
            weight_copy(w_mid, number).start()

    def normed_copy(source, number):
        slot = lax.rem(number, NORM_SLOTS)
        return pltpu.make_async_copy(source.at[:, block_of(lax.rem(number, blocks))], normed.at[slot], normed_sems.at[slot])

    def normed_start(number):
        @pl.when(number < 2 * blocks)
        def _():
            normed_copy(normed_2, number).start()

        @pl.when((number >= 2 * blocks) & (number < 4 * blocks))
        def _():
            normed_copy(normed_1, number).start()

    load_left.start()
    load_grad.start()
    for layer, (gain, bias) in enumerate(((gain_2, bias_2), (gain_1, bias_1))):
        vecs[layer, 0:1] = gain[...]
        vecs[layer, 1:2] = bias[...]
        for index in range(groups):
            vecs[layer, 2:3, index * COLS : (index + 1) * COLS] = inv_ref[1 - layer, index : index + 1]
    enter_all(me, shards)

    def row_of(unit, h):
        layer = lax.div(unit, units_full)
        part = width // 2 - (width // 2 - feat_in.shape[1] // 2) * lax.div(layer, 2)
        return layer * width + h * part + lax.div(lax.rem(unit, units_full), PARTS) * UNIT

    ex = Exchange(me, 2, halves, out_ref, total, recv_1, recv_2, recv_3, total, send_sems, recv_sems, row_of, DEPTH, send_total=True)
    sums = SumExchange(me, shards, slots, sum_send, sum_recv)

    def produce(unit, source, part):
        @pl.when(unit >= 2)
        def _():
            ex.copy(unit - 2, PAIR).wait_send()

        which = lax.rem(lax.div(unit, units_full), 2)
        local = lax.div(lax.rem(unit, units_full), PARTS) * UNIT
        ring = lax.rem(unit, 2)
        product_unit(source, grad.at[which], (1 - half) * part + local, half * part + local, halves, mine, ring, ring, unit, 2)
        ex.copy(unit, PAIR).start()

    def pair_step(unit):
        slot = lax.rem(unit, DEPTH)
        ex.copy(unit, PAIR).wait_recv()
        total[slot] = total[slot] + mine[lax.rem(unit, 2)]
        ex.copy(unit, RS1).start()

    def to_out(unit):
        start = ex.owned(unit)
        slot = lax.rem(unit, DEPTH)
        return pltpu.make_async_copy(total.at[slot, pl.ds(pl.multiple_of(start, 16), 16)], out_ref.at[pl.ds(pl.multiple_of(row_of(unit, half) + start, 16), 16), columns_of(unit, part_width)], send_sems.at[slot, LOCAL])

    def finish(unit):
        ex.copy(unit, RS3).wait()
        slot = lax.rem(unit, DEPTH)
        keep = pl.ds(pl.multiple_of(ex.owned(unit), 16), 16)
        total[slot, keep] = total[slot, keep] + recv_3[lax.rem(unit, DEPTH_3)]
        to_out(unit).start()
        ex.copy(unit, AG3).start()

    def forward(kind):
        def stage(unit):
            if kind == AG3:
                to_out(unit).wait()
            ex.copy(unit, kind).wait()
            if kind != AGP:
                ex.copy(unit, kind + 1).start()

        return stage

    stages = [pair_step, lambda u: ex.reduce_step(u, RS1), lambda u: ex.reduce_step(u, RS2), finish, forward(AG3), forward(AG2), forward(AG1), forward(AGP)]

    def derivative(layer, index):
        number = layer * blocks + index
        stream = 2 * layer * blocks + index
        weight_copy(w_out, number).wait()
        normed_copy(normed_2, stream).wait()
        slot, weight_slot = lax.rem(stream, NORM_SLOTS), lax.rem(number, WEIGHT_SLOTS)
        cols = block_of(index)
        gain, bias = vecs[layer, 0:1, cols], vecs[layer, 1:2, cols]
        rhs = weight[weight_slot]
        sum_n = jnp.zeros((1, BLOCK), jnp.float32)
        sum_d = jnp.zeros((1, BLOCK), jnp.float32)
        for chunk in range(rows // BLOCK):
            part = pl.ds(chunk * BLOCK, BLOCK)
            n = normed[slot, part]
            d = jnp.where(n * gain + bias > 0.0, contract_cols(grad[layer, part], rhs), 0.0)
            deriv[part, cols] = d
            sum_n = sum_n + jnp.sum(d * n, axis=0, keepdims=True)
            sum_d = sum_d + jnp.sum(d, axis=0, keepdims=True)
        wide[0:1, cols] = sum_n
        wide[1:2, cols] = sum_d
        weight_start(number + WEIGHT_SLOTS)
        normed_start(stream + NORM_SLOTS)

    def send_sums(layer):
        for index in range(groups):
            cols = pl.ds(index * COLS, COLS)
            slots[layer, me, index : index + 1] = wide[0:1, cols]
            slots[layer, me, groups + index : groups + index + 1] = wide[1:2, cols]
        sums.start(layer)

    def next_grad(layer):
        summed = sums.finish(layer)
        for index in range(groups):
            cols = pl.ds(index * COLS, COLS)
            for row in range(2):
                line = summed[row * groups + index : row * groups + index + 1]
                stat_ref[layer, row : row + 1, cols] = line
                wide[2 + row : 3 + row, cols] = line / row_count

        def one(index, carry):
            stream = (2 * layer + 1) * blocks + index
            normed_copy(normed_2, stream).wait()
            slot = lax.rem(stream, NORM_SLOTS)
            cols = block_of(index)
            mean_n, mean_d = wide[2:3, cols], wide[3:4, cols]
            scale = vecs[layer, 0:1, cols] * vecs[layer, 2:3, cols]
            for chunk in range(rows // BLOCK):
                part = pl.ds(chunk * BLOCK, BLOCK)
                grad[1 - layer, part, cols] = ((deriv[part, cols] - mean_d - normed[slot, part] * mean_n) * scale).astype(jnp.bfloat16)
            normed_start(stream + NORM_SLOTS)
            return carry

        lax.fori_loop(0, blocks, one, 0)

    def tick(now, carry):
        for lag, stage in reversed(list(zip(BACK_LAGS, stages))):
            unit = now - lag

            @pl.when((unit >= 0) & (unit < units))
            def _(stage=stage, unit=unit):
                stage(unit)

        @pl.when(now < 2 * units_full)
        def _():
            @pl.when(lax.rem(now, units_full) == 0)
            def _():
                load_left.wait()

                @pl.when(now == 0)
                def _():
                    load_grad.wait()
                    for number in range(WEIGHT_SLOTS):
                        weight_copy(w_out, number).start()
                    for number in range(NORM_SLOTS):
                        normed_copy(normed_2, number).start()
                    load_feat.start()

            produce(now, left, width // 2)

            @pl.when(now == units_full - 1)
            def _():
                pltpu.make_async_copy(left_1, left, load_sems.at[0]).start()

        @pl.when((now >= 2 * units_full) & (now < units))
        def _():
            @pl.when(now == 2 * units_full)
            def _():
                load_feat.wait()

            produce(now, feat_in, feat_in.shape[1] // 2)

        layer, place = lax.div(now - CHAIN_START, CHAIN), lax.rem(now - CHAIN_START, CHAIN)
        steps = blocks // PER_TICK

        @pl.when((now >= CHAIN_START) & (layer < 2) & (place < steps))
        def _():
            def one(index, carry):
                derivative(layer, place * PER_TICK + index)
                return carry

            lax.fori_loop(0, PER_TICK, one, 0)

            @pl.when(place == steps - 1)
            def _():
                send_sums(layer)

        @pl.when((now >= CHAIN_START) & (layer < 2) & (place == CHAIN - 1))
        def _():
            next_grad(layer)

        return carry

    lax.fori_loop(0, ticks, tick, 0)
    for unit in (units - 2, units - 1):
        ex.copy(unit, PAIR).wait_send()


def backward(act_2, grad_z, w_out, normed_2, act_1, w_mid, normed_1, feat, vectors, inv_std, shards, row_count):
    rows, width = act_2.shape
    feat_dim = feat.shape[1]
    total_rows = 2 * width + feat_dim
    vmem = pl.BlockSpec(memory_space=pltpu.VMEM)
    hbm = pl.BlockSpec(memory_space=pl.ANY)
    return pl.pallas_call(
        functools.partial(backward_kernel, shards, row_count),
        out_shape=(jax.ShapeDtypeStruct((total_rows, width), jnp.float32), jax.ShapeDtypeStruct((2, 2, width), jnp.float32)),
        in_specs=[hbm] * 8 + [vmem] * 5,
        out_specs=(hbm, vmem),
        scratch_shapes=[
            pltpu.VMEM((2, 8, width), jnp.float32),
            pltpu.VMEM((rows, width), jnp.bfloat16),
            pltpu.VMEM((rows, feat_dim), jnp.bfloat16),
            pltpu.VMEM((2, rows, width), jnp.bfloat16),
            pltpu.VMEM((WEIGHT_SLOTS, BLOCK, width), jnp.bfloat16),
            pltpu.VMEM((NORM_SLOTS, rows, BLOCK), jnp.float32),
            pltpu.VMEM((rows, width), jnp.float32),
            pltpu.VMEM((2, UNIT, width // PARTS), jnp.float32),
            pltpu.VMEM((2, UNIT, width // PARTS), jnp.float32),
            pltpu.VMEM((DEPTH, UNIT, width // PARTS), jnp.float32),
            pltpu.VMEM((DEPTH_1, 64, width // PARTS), jnp.float32),
            pltpu.VMEM((DEPTH_2, 32, width // PARTS), jnp.float32),
            pltpu.VMEM((DEPTH_3, 16, width // PARTS), jnp.float32),
            pltpu.VMEM((8, width), jnp.float32),
            pltpu.VMEM((2, shards, 8, COLS), jnp.float32),
            pltpu.SemaphoreType.DMA((DEPTH, 9)),
            pltpu.SemaphoreType.DMA((DEPTH, 9)),
            pltpu.SemaphoreType.DMA((3,)),
            pltpu.SemaphoreType.DMA((WEIGHT_SLOTS,)),
            pltpu.SemaphoreType.DMA((NORM_SLOTS,)),
            pltpu.SemaphoreType.DMA((2, shards)),
            pltpu.SemaphoreType.DMA((2, shards)),
        ],
        compiler_params=pltpu.CompilerParams(collective_id=3, has_side_effects=True, vmem_limit_bytes=VMEM_LIMIT),
        cost_estimate=pl.CostEstimate(flops=2 * rows * width * (2 * width + total_rows), bytes_accessed=16 * width * width, transcendentals=0),
        name="backward",
    )(act_2, grad_z, w_out, normed_2, act_1, w_mid, normed_1, feat, *vectors, inv_std)


CHUNK = 128
FLIGHT = 12


def output_kernel(sums_ref, emb_ref, stat_ref, emb_out, in_out, mid_out, last_out, gain_1, bias_1, gain_2, bias_2, buffer, read_sems, write_sems):
    width = mid_out.shape[0]
    reads, writes = [], []
    for source, first, target in ((sums_ref, 0, last_out), (sums_ref, width, mid_out), (sums_ref, 2 * width, in_out), (emb_ref, 0, emb_out)):
        for start in range(0, target.shape[0], CHUNK):
            slot = len(reads) % FLIGHT
            reads.append(pltpu.make_async_copy(source.at[pl.ds(first + start, CHUNK)], buffer.at[slot], read_sems.at[slot]))
            writes.append(pltpu.make_async_copy(buffer.at[slot], target.at[pl.ds(start, CHUNK)], write_sems.at[slot]))
    for copy in reads[:FLIGHT]:
        copy.start()
    gain_1[...] = stat_ref[1, 0:1]
    bias_1[...] = stat_ref[1, 1:2]
    gain_2[...] = stat_ref[0, 0:1]
    bias_2[...] = stat_ref[0, 1:2]
    behind = FLIGHT // 2
    for index in range(len(reads) + behind):
        if index < len(reads):
            reads[index].wait()
            writes[index].start()
        if index >= behind:
            writes[index - behind].wait()
            if index - behind + FLIGHT < len(reads):
                reads[index - behind + FLIGHT].start()


def to_outputs(sums, emb_grad, stats, width):
    feat_dim = sums.shape[0] - 2 * width
    vmem = pl.BlockSpec(memory_space=pltpu.VMEM)
    hbm = pl.BlockSpec(memory_space=pl.ANY)
    row = jax.ShapeDtypeStruct((1, width), jnp.float32)
    return pl.pallas_call(
        output_kernel,
        out_shape=(jax.ShapeDtypeStruct(emb_grad.shape, jnp.float32), jax.ShapeDtypeStruct((feat_dim, width), jnp.float32), jax.ShapeDtypeStruct((width, width), jnp.float32), jax.ShapeDtypeStruct((width, width), jnp.float32)) + (row,) * 4,
        in_specs=[hbm, hbm, vmem],
        out_specs=(hbm,) * 4 + (vmem,) * 4,
        scratch_shapes=[pltpu.VMEM((FLIGHT, CHUNK, width), jnp.float32), pltpu.SemaphoreType.DMA((FLIGHT,)), pltpu.SemaphoreType.DMA((FLIGHT,))],
        compiler_params=pltpu.CompilerParams(vmem_limit_bytes=VMEM_LIMIT),
        name="to_outputs",
    )(sums, emb_grad, stats)


def solution(mesh):
    shards = mesh.shape[DATA_AXIS]
    row_part = P(DATA_AXIS, None)
    replicated = P()

    def local_step(feat_a, feat_b, w_in, w_mid, w_out, t_in, t_mid, t_out, gain_1, bias_1, gain_2, bias_2, off_weight):
        row_count = feat_a.shape[0] * shards

        vectors = [vector.reshape(1, -1) for vector in (gain_1, bias_1, gain_2, bias_2)]
        act_1, act_2, normed_1, normed_2, zh_a, emb_a, emb_b, inv_std = forward_pass(feat_a, feat_b, w_in, t_in, w_mid, t_mid, w_out, t_out, vectors, shards, row_count)
        width = w_mid.shape[0]
        grad_emb, grad_z, loss_sums = corr_grad(emb_a, emb_b, zh_a, inv_std, off_weight, shards, row_count)
        loss_value = loss_sums[0, 0]
        sums, stats = backward(act_2, grad_z, w_out, normed_2, act_1, w_mid, normed_1, feat_a, vectors, inv_std, shards, row_count)
        grad_emb, grad_in, grad_mid, grad_out, *vector_grads = to_outputs(sums, grad_emb, stats, width)
        return (loss_value, grad_emb, grad_in, grad_mid, grad_out, *[vector.reshape(-1) for vector in vector_grads])

    return jax.shard_map(local_step, mesh=mesh, in_specs=(row_part, row_part) + (replicated,) * 11, out_specs=(replicated, row_part) + (replicated,) * 7, check_vma=False)
```

```python
import functools

import jax
import jax.numpy as jnp
from jax import lax
from jax.experimental import pallas as pl
from jax.experimental.pallas import tpu as pltpu
from jax.sharding import PartitionSpec as P

NORM_EPS = 1e-5
DATA_AXIS = "data"
MESH_ID = pl.DeviceIdType.MESH
UNIT = 128
VMEM_LIMIT = 66_000_000


def contract_rows(left_op, right_op):
    return lax.dot_general(left_op, right_op, (((0,), (0,)), ((), ())), preferred_element_type=jnp.float32)


def contract_cols(left_op, right_op):
    return lax.dot_general(left_op, right_op, (((1,), (1,)), ((), ())), preferred_element_type=jnp.float32)


def flip(me, mask):
    bit = lax.rem(lax.div(me, mask), 2)
    return me + mask * (1 - 2 * bit), bit


class SumExchange:
    def __init__(self, me, shards, slots, send_sems, recv_sems):
        self.me, self.shards, self.slots, self.send_sems, self.recv_sems = me, shards, slots, send_sems, recv_sems

    def copy(self, index, peer, slot):
        return pltpu.make_async_remote_copy(src_ref=self.slots.at[index, self.me], dst_ref=self.slots.at[index, slot], send_sem=self.send_sems.at[index, peer], recv_sem=self.recv_sems.at[index, slot], device_id=(peer,), device_id_type=MESH_ID)

    def peers(self):
        return [lax.rem(self.me + shift, self.shards) for shift in range(1, self.shards)]

    def start(self, index):
        for peer in self.peers():
            self.copy(index, peer, self.me).start()

    def finish(self, index):
        for peer in self.peers():
            self.copy(index, peer, peer).wait_recv()
            self.copy(index, peer, self.me).wait_send()
        summed = self.slots[index, 0]
        for slot in range(1, self.shards):
            summed = summed + self.slots[index, slot]
        return summed


def enter_all(me, shards):
    barrier = pltpu.get_barrier_semaphore()
    for shift in range(1, shards):
        pl.semaphore_signal(barrier, inc=1, device_id=(lax.rem(me + shift, shards),), device_id_type=MESH_ID)
    pl.semaphore_wait(barrier, shards - 1)


COLS = 512
ROWS = 1024


def forward_kernel(shards, row_count, feat_a, feat_b, w_in, t_in, w_mid, t_mid, w_out, t_out, gain_1, bias_1, gain_2, bias_2, act_1, act_2, normed_1, normed_2, normed_z, emb_a, emb_b, inv_ref, pre, act, feat, weight_in, weight, slots, sums, send_sems, recv_sems, load_sems, store_sems):
    me = lax.axis_index(DATA_AXIS)
    rows, width = act_1.shape
    groups = width // COLS
    copies = [pltpu.make_async_copy(src, dst, load_sems.at[index]) for index, (src, dst) in enumerate([(feat_a, feat.at[0]), (w_in, weight_in.at[0]), (feat_b, feat.at[1]), (t_in, weight_in.at[1]), (w_mid, weight.at[0]), (t_mid, weight.at[1]), (w_out, weight.at[0]), (t_out, weight.at[1])])]
    for index in range(4):
        copies[index].start()
    enter_all(me, shards)
    ex = SumExchange(me, shards, slots, send_sems, recv_sems)

    def product(index, source, matrix, target):
        def group(number, carry):
            cols = pl.ds(pl.multiple_of(number * COLS, COLS), COLS)
            total = jnp.zeros((1, COLS), jnp.float32)
            squares = jnp.zeros((1, COLS), jnp.float32)
            for chunk in range(rows // ROWS):
                part = pl.ds(chunk * ROWS, ROWS)
                out = jnp.dot(source[part], matrix[:, cols], preferred_element_type=jnp.float32)
                target[part, cols] = out
                total = total + jnp.sum(out, axis=0, keepdims=True)
                squares = squares + jnp.sum(out * out, axis=0, keepdims=True)
            slots[index, me, pl.ds(number, 1)] = total
            slots[index, me, pl.ds(number + groups, 1)] = squares
            return carry

        lax.fori_loop(0, groups, group, 0)
        ex.start(index)

    def normalise(index, source, target, layer, keep, out_group=None):
        summed = ex.finish(index) / row_count
        mean = summed[:groups]
        inv = lax.rsqrt(summed[groups:] - mean * mean + NORM_EPS)
        sums[index, :groups] = mean
        sums[index, groups:] = inv
        if keep is not None:
            inv_ref[layer, :groups] = inv

        def group(number, carry):
            cols = pl.ds(pl.multiple_of(number * COLS, COLS), COLS)
            col_mean = sums[index, pl.ds(number, 1)]
            col_inv = sums[index, pl.ds(number + groups, 1)]
            for chunk in range(rows // ROWS):
                part = pl.ds(chunk * ROWS, ROWS)
                out = (source[part, cols] - col_mean) * col_inv
                if keep is not None:
                    source[part, cols] = out
                if layer < 2:
                    gain, bias = ((gain_1, bias_1), (gain_2, bias_2))[layer]
                    out = jnp.maximum(out * gain[:, cols] + bias[:, cols], 0.0)
                target[part, cols] = out.astype(jnp.bfloat16)
            if out_group is not None:
                out_group(number).start()
            return carry

        lax.fori_loop(0, groups, group, 0)

    def store(number, src, dst):
        copy = pltpu.make_async_copy(src, dst, store_sems.at[number])
        copy.start()
        return copy

    copies[0].wait()
    copies[1].wait()
    copies[4].start()
    copies[5].start()
    product(0, feat.at[0], weight_in.at[0], pre.at[0])
    copies[2].wait()
    copies[3].wait()
    product(1, feat.at[1], weight_in.at[1], pre.at[1])
    normalise(0, pre.at[0], act.at[0], 0, normed_1)
    out_n1 = store(0, pre.at[0], normed_1)
    out_x1 = store(1, act.at[0], act_1)
    copies[4].wait()
    product(2, act.at[0], weight.at[0], pre.at[2])
    copies[6].start()
    normalise(1, pre.at[1], act.at[1], 0, None)
    copies[5].wait()
    out_n1.wait()
    product(3, act.at[1], weight.at[1], pre.at[0])
    copies[7].start()
    out_x1.wait()
    normalise(2, pre.at[2], act.at[0], 1, normed_2)
    out_n2 = store(2, pre.at[2], normed_2)
    out_x2 = store(3, act.at[0], act_2)
    copies[6].wait()
    product(4, act.at[0], weight.at[0], pre.at[1])
    normalise(3, pre.at[0], act.at[1], 1, None)
    copies[7].wait()
    out_n2.wait()
    product(5, act.at[1], weight.at[1], pre.at[2])
    out_x2.wait()
    normalise(4, pre.at[1], act.at[0], 2, normed_z)
    out_z = store(4, pre.at[1], normed_z)
    out_a = store(5, act.at[0], emb_a)

    def last_group(number):
        cols = pl.ds(pl.multiple_of(number * COLS, COLS), COLS)
        return pltpu.make_async_copy(act.at[1, :, cols], emb_b.at[:, cols], store_sems.at[6 + number])

    normalise(5, pre.at[2], act.at[1], 2, None, last_group)
    for copy in [out_z, out_a] + [last_group(number) for number in range(groups)]:
        copy.wait()


def forward_pass(feat_a, feat_b, w_in, t_in, w_mid, t_mid, w_out, t_out, vectors, shards, row_count):
    rows, feat_dim = feat_a.shape
    width = w_mid.shape[0]
    groups = width // COLS
    vmem = pl.BlockSpec(memory_space=pltpu.VMEM)
    hbm = pl.BlockSpec(memory_space=pl.ANY)
    half_out = jax.ShapeDtypeStruct((rows, width), jnp.bfloat16)
    full_out = jax.ShapeDtypeStruct((rows, width), jnp.float32)
    return pl.pallas_call(
        functools.partial(forward_kernel, shards, row_count),
        out_shape=(half_out, half_out, full_out, full_out, full_out, half_out, half_out, jax.ShapeDtypeStruct((3, 8, COLS), jnp.float32)),
        in_specs=[hbm] * 8 + [vmem] * 4,
        out_specs=(hbm,) * 7 + (vmem,),
        scratch_shapes=[
            pltpu.VMEM((3, rows, width), jnp.float32),
            pltpu.VMEM((2, rows, width), jnp.bfloat16),
            pltpu.VMEM((2, rows, feat_dim), jnp.bfloat16),
            pltpu.VMEM((2, feat_dim, width), jnp.bfloat16),
            pltpu.VMEM((2, width, width), jnp.bfloat16),
            pltpu.VMEM((6, shards, 2 * groups, COLS), jnp.float32),
            pltpu.VMEM((6, 2 * groups, COLS), jnp.float32),
            pltpu.SemaphoreType.DMA((6, shards)),
            pltpu.SemaphoreType.DMA((6, shards)),
            pltpu.SemaphoreType.DMA((8,)),
            pltpu.SemaphoreType.DMA((6 + groups,)),
        ],
        compiler_params=pltpu.CompilerParams(collective_id=4, has_side_effects=True, vmem_limit_bytes=VMEM_LIMIT),
        cost_estimate=pl.CostEstimate(flops=4 * rows * width * (2 * width + feat_dim), bytes_accessed=24 * width * width, transcendentals=0),
        name="forward",
    )(feat_a, feat_b, w_in, t_in, w_mid, t_mid, w_out, t_out, *vectors)


PAIR, RS1, RS2, RS3, AG3, AG2, AG1, AGP, LOCAL = range(9)


PARTS = 2


def columns_of(unit, width):
    return pl.ds(pl.multiple_of(lax.rem(unit, PARTS) * width, UNIT), width)


class Exchange:
    def __init__(self, me, ring, halves, gathered, recv_pair, recv_1, recv_2, recv_3, total, send_sems, recv_sems, row_of, depth, send_total=False):
        self.depth, self.send_total = depth, send_total
        self.me, self.ring, self.halves, self.gathered = me, ring, halves, gathered
        self.recv_pair, self.recv_1, self.recv_2, self.recv_3, self.total = recv_pair, recv_1, recv_2, recv_3, total
        self.send_sems, self.recv_sems, self.row_of = send_sems, recv_sems, row_of

    def axes(self, unit):
        def mask(shift):
            axis = lax.rem(unit + shift, 3)
            return 2 + axis + axis * axis

        (p1, b1), (p2, b2), (p3, b3) = (flip(self.me, mask(shift)) for shift in range(3))
        return (p1, p2, p3), (b1, b2, b3)

    def copy(self, unit, kind):
        (p1, p2, p3), (b1, b2, b3) = self.axes(unit)
        partner, half = flip(self.me, 1)

        def rows(start, size):
            return pl.ds(pl.multiple_of(start, 16), size)

        slot = lax.rem(unit, self.depth)
        total = self.total.at[slot]
        row = self.row_of(unit, half)
        if kind == PAIR:
            src, dst, peer = self.halves.at[lax.rem(unit, self.ring)], self.recv_pair.at[slot], partner
        elif kind == RS1:
            src, dst, peer = total.at[rows((1 - b1) * 64, 64)], self.recv_1.at[lax.rem(unit, self.recv_1.shape[0])], p1
        elif kind == RS2:
            src, dst, peer = total.at[rows(b1 * 64 + (1 - b2) * 32, 32)], self.recv_2.at[lax.rem(unit, self.recv_2.shape[0])], p2
        elif kind == RS3:
            src, dst, peer = total.at[rows(b1 * 64 + b2 * 32 + (1 - b3) * 16, 16)], self.recv_3.at[lax.rem(unit, self.recv_3.shape[0])], p3
        else:
            start, size, peer = {
                AG3: (b1 * 64 + b2 * 32 + b3 * 16, 16, p3),
                AG2: (b1 * 64 + b2 * 32, 32, p2),
                AG1: (b1 * 64, 64, p1),
                AGP: (0, 128, partner),
            }[kind]
            src = dst = self.gathered.at[rows(row + start, size), columns_of(unit, total.shape[1])]
            if kind == AG3 and self.send_total:
                src = total.at[rows(start, size)]
        return pltpu.make_async_remote_copy(src_ref=src, dst_ref=dst, send_sem=self.send_sems.at[slot, kind], recv_sem=self.recv_sems.at[slot, kind], device_id=(peer,), device_id_type=MESH_ID)

    def reduce_step(self, unit, kind):
        _, (b1, b2, b3) = self.axes(unit)
        self.copy(unit, kind).wait()
        if kind == PAIR:
            start, size, landed = 0, 128, self.recv_pair
        elif kind == RS1:
            start, size, landed = b1 * 64, 64, self.recv_1
        else:
            start, size, landed = b1 * 64 + b2 * 32, 32, self.recv_2
        keep = pl.ds(pl.multiple_of(start, 16), size)
        slot = lax.rem(unit, self.depth)
        self.total[slot, keep] = self.total[slot, keep] + landed[lax.rem(unit, landed.shape[0])]
        self.copy(unit, kind + 1).start()

    def owned(self, unit):
        _, (b1, b2, b3) = self.axes(unit)
        return b1 * 64 + b2 * 32 + b3 * 16


def enter(me):
    barrier = pltpu.get_barrier_semaphore()
    for mask in (1, 2, 4, 8):
        pl.semaphore_signal(barrier, inc=1, device_id=(flip(me, mask)[0],), device_id_type=MESH_ID)
    pl.semaphore_wait(barrier, 4)


def pipeline(units, lags, stages):
    def step(now, carry):
        for lag, stage in reversed(list(zip(lags, stages))):
            unit = now - lag

            @pl.when((unit >= 0) & (unit < units))
            def _(unit=unit, stage=stage):
                stage(unit)

        return carry

    lax.fori_loop(0, units + max(lags), step, 0)


def product_unit(left_ref, right_ref, col_other, col_mine, halves, mine, ring, slot, unit, blocks):
    left = jnp.concatenate([left_ref[:, pl.ds(pl.multiple_of(col_other, UNIT), UNIT)], left_ref[:, pl.ds(pl.multiple_of(col_mine, UNIT), UNIT)]], axis=1)
    part = halves.shape[2]
    width = part // blocks
    for block in range(blocks):
        cols = pl.ds(block * width, width)
        source = pl.ds(pl.multiple_of(lax.rem(unit, PARTS) * part + block * width, UNIT), width)
        out = contract_rows(left, right_ref[:, source])
        halves[ring, :, cols] = out[:UNIT]
        mine[slot, :, cols] = out[UNIT:]


RING = 3
BACK_ROWS = 1024
CORR_LAGS = (0, 2, 5, 7, 10, 13, 16, 19, 21)


def corr_kernel(shards, row_count, off_ref, inv_ref, emb_a, emb_b, normed, emb_out, back_out, loss_ref, left_ref, right_ref, grad_ref, emb_grad, back, norm_in, loss_acc, wide, slots, halves, recv_pair, recv_1, recv_2, recv_3, total, send_sems, recv_sems, sum_send, sum_recv, norm_sems, store_sems, back_sems):
    me = lax.axis_index(DATA_AXIS)
    loads = [pltpu.make_async_copy(emb_b, right_ref, store_sems.at[0]), pltpu.make_async_copy(emb_a, left_ref, store_sems.at[1])]
    for copy in loads:
        copy.start()
    rows, width = right_ref.shape
    half_rows = width // 2
    units = half_rows // UNIT * PARTS
    part_width = width // PARTS
    groups = width // COLS
    _, half = flip(me, 1)
    enter_all(me, shards)
    ex = Exchange(me, RING, halves, grad_ref, recv_pair, recv_1, recv_2, recv_3, total, send_sems, recv_sems, lambda unit, h: h * half_rows + lax.div(unit, PARTS) * UNIT, units)
    sums = SumExchange(me, shards, slots, sum_send, sum_recv)
    loss_acc[...] = jnp.zeros_like(loss_acc)
    for copy in loads:
        copy.wait()

    def produce(unit):
        @pl.when(unit >= RING)
        def _():
            ex.copy(unit - RING, PAIR).wait_send()

        local = lax.div(unit, PARTS) * UNIT
        product_unit(left_ref, right_ref, (1 - half) * half_rows + local, half * half_rows + local, halves, total, lax.rem(unit, RING), unit, unit, 2)
        ex.copy(unit, PAIR).start()

    def pair_step(unit):
        ex.copy(unit, PAIR).wait_recv()
        total[unit] = total[unit] + recv_pair[unit]
        ex.copy(unit, RS1).start()

    def finish(unit):
        ex.copy(unit, RS3).wait()
        start = ex.owned(unit)
        keep = pl.ds(pl.multiple_of(start, 16), 16)
        corr = (total[unit, keep] + recv_3[unit]) * (1.0 / row_count)
        row = half * half_rows + lax.div(unit, PARTS) * UNIT + start
        shift = row - lax.rem(unit, PARTS) * part_width
        on_diag = lax.broadcasted_iota(jnp.int32, (16, part_width), 0) + shift == lax.broadcasted_iota(jnp.int32, (16, part_width), 1)
        off_weight = off_ref[0, 0]
        miss = 1.0 - corr
        terms = jnp.where(on_diag, miss * miss, off_weight * (corr * corr))
        loss_acc[...] += terms[:8] + terms[8:]
        grad = jnp.where(on_diag, -2.0 * miss, 2.0 * off_weight * corr).astype(jnp.bfloat16)
        grad_ref[pl.ds(pl.multiple_of(row, 16), 16), columns_of(unit, part_width)] = grad
        ex.copy(unit, AG3).start()

    def forward(kind):
        def stage(unit):
            ex.copy(unit, kind).wait()
            if kind != AGP:
                ex.copy(unit, kind + 1).start()

            if kind == AG1:

                @pl.when(lax.rem(unit, PARTS) == PARTS - 1)
                def _():
                    block = lax.div(unit, PARTS)
                    for side in range(2):
                        load_norm(row_of(block, side), lax.rem(block, 2), side).start()

        return stage

    for index in range(groups):
        wide[2:3, index * COLS : (index + 1) * COLS] = inv_ref[2, index : index + 1]

    def packed(which):
        piece = width // 8
        return [(4 * row + 2 * side + index, row, pl.ds(side * half_rows + (2 * which + index) * piece, piece)) for row in range(2) for side in range(2) for index in range(2)]

    def row_of(unit, side):
        return (half + side * (1 - 2 * half)) * half_rows + unit * UNIT

    def lanes(start):
        return pl.ds(pl.multiple_of(start, UNIT), UNIT)

    def load_norm(start, slot, side):
        return pltpu.make_async_copy(normed.at[:, lanes(start)], norm_in.at[slot, side], norm_sems.at[slot, side])

    def arrive(unit):
        ex.copy(unit, AGP).wait()

        @pl.when(lax.rem(unit, PARTS) == PARTS - 1)
        def _():
            embed(lax.div(unit, PARTS))

    def embed(unit):
        slot = lax.rem(unit, 2)
        starts = [row_of(unit, side) for side in range(2)]
        rhs = jnp.concatenate([grad_ref[lanes(start)] for start in starts], axis=0)
        for side in range(2):
            load_norm(starts[side], slot, side).wait()
        plain = [jnp.zeros((1, UNIT), jnp.float32)] * 2
        crossed = [jnp.zeros((1, UNIT), jnp.float32)] * 2
        for chunk in range(rows // ROWS):
            part = pl.ds(chunk * ROWS, ROWS)
            out = contract_cols(right_ref[part], rhs) * (1.0 / row_count)
            for side in range(2):
                piece = out[:, side * UNIT : (side + 1) * UNIT]
                emb_grad[part, lanes(starts[side])] = piece
                plain[side] = plain[side] + jnp.sum(piece, axis=0, keepdims=True)
                crossed[side] = crossed[side] + jnp.sum(piece * norm_in[slot, side, part], axis=0, keepdims=True)
        for side in range(2):
            wide[0:1, lanes(starts[side])] = plain[side]
            wide[1:2, lanes(starts[side])] = crossed[side]

        @pl.when(unit == half_rows // UNIT // 2 - 1)
        def _():
            for line, row, cols in packed(0):
                slots[0, me, line : line + 1, : width // 8] = wide[row : row + 1, cols]
            slots[0, me, :, width // 8 :] = jnp.zeros((8, UNIT), jnp.float32)
            sums.start(0)

    pipeline(units, CORR_LAGS, [produce, pair_step, lambda u: ex.reduce_step(u, RS1), lambda u: ex.reduce_step(u, RS2), finish, forward(AG3), forward(AG2), forward(AG1), arrive])
    for unit in range(units - RING, units):
        ex.copy(unit, PAIR).wait_send()
    folded = loss_acc[:, :UNIT]
    for index in range(1, part_width // UNIT):
        folded = folded + loss_acc[:, index * UNIT : (index + 1) * UNIT]
    for line, row, cols in packed(1):
        slots[1, me, line : line + 1, : width // 8] = wide[row : row + 1, cols]
    slots[1, me, :, width // 8 :] = folded
    sums.start(1)
    store_emb = pltpu.make_async_copy(emb_grad, emb_out, store_sems.at[0])
    store_emb.start()
    steps = width // (2 * UNIT)

    def block_at(position):
        place = lax.rem(position, steps // 2)
        return 2 * lax.div(position, steps // 2) + lax.rem(place, 2) + (steps // 2) * lax.div(place, 2)

    def load_block(position):
        return [load_norm((2 * block_at(position) + side) * UNIT, lax.rem(position, 2), side) for side in range(2)]

    def store_block(position):
        cols = pl.ds(pl.multiple_of(2 * block_at(position) * UNIT, 2 * UNIT), 2 * UNIT)
        return pltpu.make_async_copy(back.at[:, cols], back_out.at[:, cols], back_sems.at[position])

    for position in range(2):
        for copy in load_block(position):
            copy.start()

    def norm_back(position, carry):
        slot = lax.rem(position, 2)
        for side, copy in enumerate(load_block(position)):
            copy.wait()
            start = (2 * block_at(position) + side) * UNIT
            mean_g, mean_gn, inv = wide[0:1, lanes(start)], wide[1:2, lanes(start)], wide[2:3, lanes(start)]
            for chunk in range(rows // BACK_ROWS):
                part = pl.ds(chunk * BACK_ROWS, BACK_ROWS)
                back[part, lanes(start)] = ((emb_grad[part, lanes(start)] - mean_g - norm_in[slot, side, part] * mean_gn) * inv).astype(jnp.bfloat16)
        store_block(position).start()

        @pl.when(position + 2 < steps)
        def _():
            for copy in load_block(position + 2):
                copy.start()

        return carry

    for which in range(2):
        summed = sums.finish(which)
        if which == 1:
            loss_ref[0, 0] = jnp.sum(summed[:, width // 8 :])
        for line, row, cols in packed(which):
            wide[row : row + 1, cols] = summed[line : line + 1, : width // 8] / row_count
        lax.fori_loop(which * (steps // 2), (which + 1) * (steps // 2), norm_back, 0)
    for position in range(steps):
        store_block(position).wait()
    store_emb.wait()


def exchange_scratch(units, width):
    return [
        pltpu.VMEM((RING, UNIT, width), jnp.float32),
        pltpu.VMEM((units, UNIT, width), jnp.float32),
        pltpu.VMEM((units, 64, width), jnp.float32),
        pltpu.VMEM((units, 32, width), jnp.float32),
        pltpu.VMEM((units, 16, width), jnp.float32),
        pltpu.VMEM((units, UNIT, width), jnp.float32),
        pltpu.SemaphoreType.DMA((units, 9)),
        pltpu.SemaphoreType.DMA((units, 9)),
    ]


def corr_grad(emb_a, emb_b, normed, inv_std, off_weight, shards, row_count):
    rows, width = emb_a.shape
    vmem = pl.BlockSpec(memory_space=pltpu.VMEM)
    hbm = pl.BlockSpec(memory_space=pl.ANY)
    return pl.pallas_call(
        functools.partial(corr_kernel, shards, row_count),
        out_shape=(jax.ShapeDtypeStruct((rows, width), jnp.float32), jax.ShapeDtypeStruct((rows, width), jnp.bfloat16), jax.ShapeDtypeStruct((1, 1), jnp.float32)),
        in_specs=[pl.BlockSpec(memory_space=pltpu.SMEM), vmem, hbm, hbm, hbm],
        out_specs=(hbm, hbm, pl.BlockSpec(memory_space=pltpu.SMEM)),
        scratch_shapes=[
            pltpu.VMEM((rows, width), jnp.bfloat16),
            pltpu.VMEM((rows, width), jnp.bfloat16),
            pltpu.VMEM((width, width), jnp.bfloat16),
            pltpu.VMEM((rows, width), jnp.float32),
            pltpu.VMEM((rows, width), jnp.bfloat16),
            pltpu.VMEM((2, 2, rows, UNIT), jnp.float32),
            pltpu.VMEM((8, width // PARTS), jnp.float32),
            pltpu.VMEM((8, width), jnp.float32),
            pltpu.VMEM((2, shards, 8, width // 8 + UNIT), jnp.float32),
        ]
        + exchange_scratch(width // 2 // UNIT * PARTS, width // PARTS)
        + [pltpu.SemaphoreType.DMA((2, shards)), pltpu.SemaphoreType.DMA((2, shards)), pltpu.SemaphoreType.DMA((2, 2)), pltpu.SemaphoreType.DMA((2,)), pltpu.SemaphoreType.DMA((width // (2 * UNIT),))],
        compiler_params=pltpu.CompilerParams(collective_id=2, has_side_effects=True, vmem_limit_bytes=VMEM_LIMIT),
        cost_estimate=pl.CostEstimate(flops=4 * rows * width * width, bytes_accessed=8 * width * width, transcendentals=0),
        name="corr_grad",
    )(off_weight.reshape(1, 1), inv_std, emb_a, emb_b, normed)


DEPTH = 36
DEPTH_1, DEPTH_2, DEPTH_3 = 21, 12, 6
CHAIN = 11
PER_TICK = 1
CHAIN_START = 2
BLOCK = 256
NORM_SLOTS = 3
WEIGHT_SLOTS = 3
BACK_LAGS = (1, 4, 6, 8, 11, 14, 18, 21)


def backward_kernel(shards, row_count, left_2, grad_z, w_out, normed_2, left_1, w_mid, normed_1, feat, gain_1, bias_1, gain_2, bias_2, inv_ref, out_ref, stat_ref, vecs, left, feat_in, grad, weight, normed, deriv, halves, mine, total, recv_1, recv_2, recv_3, wide, slots, send_sems, recv_sems, load_sems, weight_sems, normed_sems, sum_send, sum_recv):
    me = lax.axis_index(DATA_AXIS)
    _, half = flip(me, 1)
    rows, width = left.shape
    groups = width // COLS
    blocks = width // BLOCK
    units_full = width // 2 // UNIT * PARTS
    units_last = feat_in.shape[1] // 2 // UNIT * PARTS
    part_width = width // PARTS
    units = 2 * units_full + units_last
    ticks = units + max(BACK_LAGS)

    load_left = pltpu.make_async_copy(left_2, left, load_sems.at[0])
    load_grad = pltpu.make_async_copy(grad_z, grad.at[0], load_sems.at[1])
    load_feat = pltpu.make_async_copy(feat, feat_in, load_sems.at[2])

    def block_of(index):
        return pl.ds(pl.multiple_of(index * BLOCK, BLOCK), BLOCK)

    def weight_copy(source, number):
        slot = lax.rem(number, WEIGHT_SLOTS)
        return pltpu.make_async_copy(source.at[block_of(lax.rem(number, blocks))], weight.at[slot], weight_sems.at[slot])

    def weight_start(number):
        @pl.when(number < blocks)
        def _():
            weight_copy(w_out, number).start()

        @pl.when((number >= blocks) & (number < 2 * blocks))
        def _():
            weight_copy(w_mid, number).start()

    def normed_copy(source, number):
        slot = lax.rem(number, NORM_SLOTS)
        return pltpu.make_async_copy(source.at[:, block_of(lax.rem(number, blocks))], normed.at[slot], normed_sems.at[slot])

    def normed_start(number):
        @pl.when(number < 2 * blocks)
        def _():
            normed_copy(normed_2, number).start()

        @pl.when((number >= 2 * blocks) & (number < 4 * blocks))
        def _():
            normed_copy(normed_1, number).start()

    load_left.start()
    load_grad.start()
    for layer, (gain, bias) in enumerate(((gain_2, bias_2), (gain_1, bias_1))):
        vecs[layer, 0:1] = gain[...]
        vecs[layer, 1:2] = bias[...]
        for index in range(groups):
            vecs[layer, 2:3, index * COLS : (index + 1) * COLS] = inv_ref[1 - layer, index : index + 1]
    enter_all(me, shards)

    def row_of(unit, h):
        layer = lax.div(unit, units_full)
        part = width // 2 - (width // 2 - feat_in.shape[1] // 2) * lax.div(layer, 2)
        return layer * width + h * part + lax.div(lax.rem(unit, units_full), PARTS) * UNIT

    ex = Exchange(me, 2, halves, out_ref, total, recv_1, recv_2, recv_3, total, send_sems, recv_sems, row_of, DEPTH, send_total=True)
    sums = SumExchange(me, shards, slots, sum_send, sum_recv)

    def produce(unit, source, part):
        @pl.when(unit >= 2)
        def _():
            ex.copy(unit - 2, PAIR).wait_send()

        which = lax.rem(lax.div(unit, units_full), 2)
        local = lax.div(lax.rem(unit, units_full), PARTS) * UNIT
        ring = lax.rem(unit, 2)
        product_unit(source, grad.at[which], (1 - half) * part + local, half * part + local, halves, mine, ring, ring, unit, 2)
        ex.copy(unit, PAIR).start()

    def pair_step(unit):
        slot = lax.rem(unit, DEPTH)
        ex.copy(unit, PAIR).wait_recv()
        total[slot] = total[slot] + mine[lax.rem(unit, 2)]
        ex.copy(unit, RS1).start()

    def to_out(unit):
        start = ex.owned(unit)
        slot = lax.rem(unit, DEPTH)
        return pltpu.make_async_copy(total.at[slot, pl.ds(pl.multiple_of(start, 16), 16)], out_ref.at[pl.ds(pl.multiple_of(row_of(unit, half) + start, 16), 16), columns_of(unit, part_width)], send_sems.at[slot, LOCAL])

    def finish(unit):
        ex.copy(unit, RS3).wait()
        slot = lax.rem(unit, DEPTH)
        keep = pl.ds(pl.multiple_of(ex.owned(unit), 16), 16)
        total[slot, keep] = total[slot, keep] + recv_3[lax.rem(unit, DEPTH_3)]
        to_out(unit).start()
        ex.copy(unit, AG3).start()

    def forward(kind):
        def stage(unit):
            if kind == AG3:
                to_out(unit).wait()
            ex.copy(unit, kind).wait()
            if kind != AGP:
                ex.copy(unit, kind + 1).start()

        return stage

    stages = [pair_step, lambda u: ex.reduce_step(u, RS1), lambda u: ex.reduce_step(u, RS2), finish, forward(AG3), forward(AG2), forward(AG1), forward(AGP)]

    def derivative(layer, index):
        number = layer * blocks + index
        stream = 2 * layer * blocks + index
        weight_copy(w_out, number).wait()
        normed_copy(normed_2, stream).wait()
        slot, weight_slot = lax.rem(stream, NORM_SLOTS), lax.rem(number, WEIGHT_SLOTS)
        cols = block_of(index)
        gain, bias = vecs[layer, 0:1, cols], vecs[layer, 1:2, cols]
        rhs = weight[weight_slot]
        sum_n = jnp.zeros((1, BLOCK), jnp.float32)
        sum_d = jnp.zeros((1, BLOCK), jnp.float32)
        for chunk in range(rows // BLOCK):
            part = pl.ds(chunk * BLOCK, BLOCK)
            n = normed[slot, part]
            d = jnp.where(n * gain + bias > 0.0, contract_cols(grad[layer, part], rhs), 0.0)
            deriv[part, cols] = d
            sum_n = sum_n + jnp.sum(d * n, axis=0, keepdims=True)
            sum_d = sum_d + jnp.sum(d, axis=0, keepdims=True)
        wide[0:1, cols] = sum_n
        wide[1:2, cols] = sum_d
        weight_start(number + WEIGHT_SLOTS)
        normed_start(stream + NORM_SLOTS)

    def send_sums(layer):
        for index in range(groups):
            cols = pl.ds(index * COLS, COLS)
            slots[layer, me, index : index + 1] = wide[0:1, cols]
            slots[layer, me, groups + index : groups + index + 1] = wide[1:2, cols]
        sums.start(layer)

    def next_grad(layer):
        summed = sums.finish(layer)
        for index in range(groups):
            cols = pl.ds(index * COLS, COLS)
            for row in range(2):
                line = summed[row * groups + index : row * groups + index + 1]
                stat_ref[layer, row : row + 1, cols] = line
                wide[2 + row : 3 + row, cols] = line / row_count

        def one(index, carry):
            stream = (2 * layer + 1) * blocks + index
            normed_copy(normed_2, stream).wait()
            slot = lax.rem(stream, NORM_SLOTS)
            cols = block_of(index)
            mean_n, mean_d = wide[2:3, cols], wide[3:4, cols]
            scale = vecs[layer, 0:1, cols] * vecs[layer, 2:3, cols]
            for chunk in range(rows // BLOCK):
                part = pl.ds(chunk * BLOCK, BLOCK)
                grad[1 - layer, part, cols] = ((deriv[part, cols] - mean_d - normed[slot, part] * mean_n) * scale).astype(jnp.bfloat16)
            normed_start(stream + NORM_SLOTS)
            return carry

        lax.fori_loop(0, blocks, one, 0)

    def tick(now, carry):
        for lag, stage in reversed(list(zip(BACK_LAGS, stages))):
            unit = now - lag

            @pl.when((unit >= 0) & (unit < units))
            def _(stage=stage, unit=unit):
                stage(unit)

        @pl.when(now < 2 * units_full)
        def _():
            @pl.when(lax.rem(now, units_full) == 0)
            def _():
                load_left.wait()

                @pl.when(now == 0)
                def _():
                    load_grad.wait()
                    for number in range(WEIGHT_SLOTS):
                        weight_copy(w_out, number).start()
                    for number in range(NORM_SLOTS):
                        normed_copy(normed_2, number).start()
                    load_feat.start()

            produce(now, left, width // 2)

            @pl.when(now == units_full - 1)
            def _():
                pltpu.make_async_copy(left_1, left, load_sems.at[0]).start()

        @pl.when((now >= 2 * units_full) & (now < units))
        def _():
            @pl.when(now == 2 * units_full)
            def _():
                load_feat.wait()

            produce(now, feat_in, feat_in.shape[1] // 2)

        layer, place = lax.div(now - CHAIN_START, CHAIN), lax.rem(now - CHAIN_START, CHAIN)
        steps = blocks // PER_TICK

        @pl.when((now >= CHAIN_START) & (layer < 2) & (place < steps))
        def _():
            def one(index, carry):
                derivative(layer, place * PER_TICK + index)
                return carry

            lax.fori_loop(0, PER_TICK, one, 0)

            @pl.when(place == steps - 1)
            def _():
                send_sums(layer)

        @pl.when((now >= CHAIN_START) & (layer < 2) & (place == CHAIN - 1))
        def _():
            next_grad(layer)

        return carry

    lax.fori_loop(0, ticks, tick, 0)
    for unit in (units - 2, units - 1):
        ex.copy(unit, PAIR).wait_send()


def backward(act_2, grad_z, w_out, normed_2, act_1, w_mid, normed_1, feat, vectors, inv_std, shards, row_count):
    rows, width = act_2.shape
    feat_dim = feat.shape[1]
    total_rows = 2 * width + feat_dim
    vmem = pl.BlockSpec(memory_space=pltpu.VMEM)
    hbm = pl.BlockSpec(memory_space=pl.ANY)
    return pl.pallas_call(
        functools.partial(backward_kernel, shards, row_count),
        out_shape=(jax.ShapeDtypeStruct((total_rows, width), jnp.float32), jax.ShapeDtypeStruct((2, 2, width), jnp.float32)),
        in_specs=[hbm] * 8 + [vmem] * 5,
        out_specs=(hbm, vmem),
        scratch_shapes=[
            pltpu.VMEM((2, 8, width), jnp.float32),
            pltpu.VMEM((rows, width), jnp.bfloat16),
            pltpu.VMEM((rows, feat_dim), jnp.bfloat16),
            pltpu.VMEM((2, rows, width), jnp.bfloat16),
            pltpu.VMEM((WEIGHT_SLOTS, BLOCK, width), jnp.bfloat16),
            pltpu.VMEM((NORM_SLOTS, rows, BLOCK), jnp.float32),
            pltpu.VMEM((rows, width), jnp.float32),
            pltpu.VMEM((2, UNIT, width // PARTS), jnp.float32),
            pltpu.VMEM((2, UNIT, width // PARTS), jnp.float32),
            pltpu.VMEM((DEPTH, UNIT, width // PARTS), jnp.float32),
            pltpu.VMEM((DEPTH_1, 64, width // PARTS), jnp.float32),
            pltpu.VMEM((DEPTH_2, 32, width // PARTS), jnp.float32),
            pltpu.VMEM((DEPTH_3, 16, width // PARTS), jnp.float32),
            pltpu.VMEM((8, width), jnp.float32),
            pltpu.VMEM((2, shards, 8, COLS), jnp.float32),
            pltpu.SemaphoreType.DMA((DEPTH, 9)),
            pltpu.SemaphoreType.DMA((DEPTH, 9)),
            pltpu.SemaphoreType.DMA((3,)),
            pltpu.SemaphoreType.DMA((WEIGHT_SLOTS,)),
            pltpu.SemaphoreType.DMA((NORM_SLOTS,)),
            pltpu.SemaphoreType.DMA((2, shards)),
            pltpu.SemaphoreType.DMA((2, shards)),
        ],
        compiler_params=pltpu.CompilerParams(collective_id=3, has_side_effects=True, vmem_limit_bytes=VMEM_LIMIT),
        cost_estimate=pl.CostEstimate(flops=2 * rows * width * (2 * width + total_rows), bytes_accessed=16 * width * width, transcendentals=0),
        name="backward",
    )(act_2, grad_z, w_out, normed_2, act_1, w_mid, normed_1, feat, *vectors, inv_std)


CHUNK = 128
FLIGHT = 12


def output_kernel(sums_ref, emb_ref, stat_ref, emb_out, in_out, mid_out, last_out, gain_1, bias_1, gain_2, bias_2, buffer, read_sems, write_sems):
    width = mid_out.shape[0]
    reads, writes = [], []
    for source, first, target in ((sums_ref, 0, last_out), (sums_ref, width, mid_out), (sums_ref, 2 * width, in_out), (emb_ref, 0, emb_out)):
        for start in range(0, target.shape[0], CHUNK):
            slot = len(reads) % FLIGHT
            reads.append(pltpu.make_async_copy(source.at[pl.ds(first + start, CHUNK)], buffer.at[slot], read_sems.at[slot]))
            writes.append(pltpu.make_async_copy(buffer.at[slot], target.at[pl.ds(start, CHUNK)], write_sems.at[slot]))
    for copy in reads[:FLIGHT]:
        copy.start()
    gain_1[...] = stat_ref[1, 0:1]
    bias_1[...] = stat_ref[1, 1:2]
    gain_2[...] = stat_ref[0, 0:1]
    bias_2[...] = stat_ref[0, 1:2]
    behind = FLIGHT // 2
    for index in range(len(reads) + behind):
        if index < len(reads):
            reads[index].wait()
            writes[index].start()
        if index >= behind:
            writes[index - behind].wait()
            if index - behind + FLIGHT < len(reads):
                reads[index - behind + FLIGHT].start()


def to_outputs(sums, emb_grad, stats, width):
    feat_dim = sums.shape[0] - 2 * width
    vmem = pl.BlockSpec(memory_space=pltpu.VMEM)
    hbm = pl.BlockSpec(memory_space=pl.ANY)
    row = jax.ShapeDtypeStruct((1, width), jnp.float32)
    return pl.pallas_call(
        output_kernel,
        out_shape=(jax.ShapeDtypeStruct(emb_grad.shape, jnp.float32), jax.ShapeDtypeStruct((feat_dim, width), jnp.float32), jax.ShapeDtypeStruct((width, width), jnp.float32), jax.ShapeDtypeStruct((width, width), jnp.float32)) + (row,) * 4,
        in_specs=[hbm, hbm, vmem],
        out_specs=(hbm,) * 4 + (vmem,) * 4,
        scratch_shapes=[pltpu.VMEM((FLIGHT, CHUNK, width), jnp.float32), pltpu.SemaphoreType.DMA((FLIGHT,)), pltpu.SemaphoreType.DMA((FLIGHT,))],
        compiler_params=pltpu.CompilerParams(vmem_limit_bytes=VMEM_LIMIT),
        name="to_outputs",
    )(sums, emb_grad, stats)


def solution(mesh):
    shards = mesh.shape[DATA_AXIS]
    row_part = P(DATA_AXIS, None)
    replicated = P()

    def local_step(feat_a, feat_b, w_in, w_mid, w_out, t_in, t_mid, t_out, gain_1, bias_1, gain_2, bias_2, off_weight):
        row_count = feat_a.shape[0] * shards

        vectors = [vector.reshape(1, -1) for vector in (gain_1, bias_1, gain_2, bias_2)]
        act_1, act_2, normed_1, normed_2, zh_a, emb_a, emb_b, inv_std = forward_pass(feat_a, feat_b, w_in, t_in, w_mid, t_mid, w_out, t_out, vectors, shards, row_count)
        width = w_mid.shape[0]
        grad_emb, grad_z, loss_sums = corr_grad(emb_a, emb_b, zh_a, inv_std, off_weight, shards, row_count)
        loss_value = loss_sums[0, 0]
        sums, stats = backward(act_2, grad_z, w_out, normed_2, act_1, w_mid, normed_1, feat_a, vectors, inv_std, shards, row_count)
        grad_emb, grad_in, grad_mid, grad_out, *vector_grads = to_outputs(sums, grad_emb, stats, width)
        return (loss_value, grad_emb, grad_in, grad_mid, grad_out, *[vector.reshape(-1) for vector in vector_grads])

    return jax.shard_map(local_step, mesh=mesh, in_specs=(row_part, row_part) + (replicated,) * 11, out_specs=(replicated, row_part) + (replicated,) * 7, check_vma=False)
```
